256 devices in a mesh: gx: 8 (over z), gy: 32 (over y, x, core).
Axes of the slice: x: 4, y: 4, z: 8, core: 2. Of those that a mesh axis runs over, the one named last changes fastest.
Arguments:
- right_side: float32 [1024, 8192], P('gx', 'gy'), may hold values from -1.2 to 1.2
- shift: float32 [1024, 8192], P('gx', 'gy'), may hold values from 0.0001 to 0.004
Outputs:
- solution: float32 [1024, 8192], P('gx', 'gy')
- residual: float32 [1024, 8192], P('gx', 'gy')
The draws below stay inside these ranges and needn't reach their ends.
All inputs are finite; a program needn't handle non-finite values.
Results may differ from the reference program's by a relative error of at most 0.0003.
Values sent between devices are 32-bit elements; how exact they have to be, the bound alone decides.
A program may use at most 128 MiB of HBM per device.

```python
import math
import jax
import jax.numpy as jnp

LEVELS = 4
COARSE_SWEEPS = 6
NX = 1024
NY = 8192


def draw_right_side(key, part):
    return jnp.clip(0.2 * jax.random.normal(key, (NX, NY), jnp.float32), -1.2, 1.2)


def steps_of(own_key, shape, shards, smallest, largest):
    def one(position, shards_of):
        draws = jax.random.uniform(jax.random.fold_in(jax.random.fold_in(own_key, 6), position), (shards_of,), jnp.float32, smallest / len(shards), largest / len(shards))
        return jnp.repeat(jnp.exp(draws), shape[position] // shards_of).reshape((-1,) + (1,) * (len(shape) - position - 1))

    factor_of = one(*shards[0])
    for cut in shards[1:]:
        factor_of = factor_of * one(*cut)
    return factor_of


def setup_inputs(seed: int = 0) -> dict:
    key_list = jax.random.split(jax.random.key(seed), 3)
    right_side = draw_right_side(jax.random.fold_in(key_list[2], 71), 0)
    shift = jnp.clip(jnp.exp(math.log(0.004) - 3.6888795 * jax.random.uniform(key_list[1], (NX, NY), jnp.float32) ** steps_of(key_list[1], (NX, NY), ((0, 8), (1, 32)), -0.2, 0.2)), 0.0001, 0.004)
    return dict(right_side=right_side, shift=shift)


damping = 0.8


def restrict(values):
    rows, columns = values.shape
    blocks = values.reshape(rows // 2, 2, columns // 2, 2)
    return 0.25 * (blocks[:, 0, :, 0] + blocks[:, 1, :, 0] + blocks[:, 0, :, 1] + blocks[:, 1, :, 1])


def prolong(values):
    rows, columns = values.shape
    copies = jnp.broadcast_to(values[:, None, :, None], (rows, 2, columns, 2))
    return copies.reshape(2 * rows, 2 * columns)


def operate_padded(padded, shifts, level):
    centre = padded[1:-1, 1:-1]
    beside = padded[2:, 1:-1] + padded[:-2, 1:-1] + padded[1:-1, 2:] + padded[1:-1, :-2]
    return 4.0 ** (-level) * (4.0 * centre - beside) + shifts * centre


def apply_operator(field, shifts, level):
    return operate_padded(jnp.pad(field, 1), shifts, level)


def sweeps(iterate, source, shifts, level, count):
    diagonal = 4.0 ** (1 - level) + shifts
    for turn in range(count):
        if iterate is None:
            iterate = damping * source / diagonal
        else:
            iterate = iterate + damping * (source - apply_operator(iterate, shifts, level)) / diagonal
    return iterate


def coarse_solve(iterate, source, shifts):
    unit_total = jnp.sum(apply_operator(jnp.ones_like(source), shifts, LEVELS))
    if iterate is None:
        left = jnp.sum(source)
        iterate = jnp.zeros_like(source) + left / unit_total
    else:
        left = jnp.sum(source - apply_operator(iterate, shifts, LEVELS))
        iterate = iterate + left / unit_total
    return sweeps(iterate, source, shifts, LEVELS, COARSE_SWEEPS)


def vcycle(level, iterate, source, shift_list):
    shifts = shift_list[level]
    if level == LEVELS:
        return coarse_solve(iterate, source, shifts)
    iterate = sweeps(iterate, source, shifts, level, 2)
    coarse_rhs = restrict(source - apply_operator(iterate, shifts, level))
    iterate = iterate + prolong(vcycle(level + 1, None, coarse_rhs, shift_list))
    return sweeps(iterate, source, shifts, level, 2)


def fcycle(level, source, shift_list):
    shifts = shift_list[level]
    if level == LEVELS:
        return coarse_solve(None, source, shifts)
    iterate = sweeps(None, source, shifts, level, 2)
    coarse_rhs = restrict(source - apply_operator(iterate, shifts, level))
    correction = fcycle(level + 1, coarse_rhs, shift_list)
    correction = vcycle(level + 1, correction, coarse_rhs, shift_list)
    iterate = iterate + prolong(correction)
    return sweeps(iterate, source, shifts, level, 2)


def reference(right_side, shift):
    shift_list = [shift]
    for level in range(LEVELS):
        shift_list.append(restrict(shift_list[-1]))
    solution = fcycle(0, right_side, shift_list)
    residual = right_side - apply_operator(solution, shift, 0)
    return solution, residual
```

```python
import jax
import jax.numpy as jnp
from jax import lax
from jax.experimental import pallas as pl
from jax.experimental.pallas import tpu as pltpu
from jax.sharding import PartitionSpec as P

MESH = pl.DeviceIdType.MESH
F32 = jnp.float32
BF16 = jnp.bfloat16
GX, GY = 8, 32
NX, NY = 1024, 8192
LV_Q = [4.0 ** (-l) for l in range(5)]
LV_D = [4.0 ** (1 - l) for l in range(5)]

AROUND = [(-1, 0), (1, 0), (0, -1), (0, 1), (-1, -1), (-1, 1), (1, -1), (1, 1)]
SIDE = [-1, 1, -2, 2]
LINE = [-1, 1, -2, 2, -3, 3]
GROUP_A = [(dz, dc) for dz in range(8) for dc in range(2) if dz or dc]
GROUP_B = [(dy, dx) for dy in range(4) for dx in range(4) if dy or dx]


def iota(shape, dim):
    return lax.broadcasted_iota(jnp.int32, shape, dim)


def beside(v):
    r, c = v.shape
    return (
        pltpu.roll(v, 1, axis=0)
        + pltpu.roll(v, r - 1, axis=0)
        + pltpu.roll(v, 1, axis=1)
        + pltpu.roll(v, c - 1, axis=1)
    )


def inside(shape, level, row0, col0):
    rows = iota(shape, 0) + row0
    cols = iota(shape, 1) + col0
    return (
        (rows >= 0) & (rows < (NX >> level)) & (cols >= 0) & (cols < (NY >> level))
    )


class Level:
    def __init__(self, level, shift, row0, col0, mask=None):
        self.level = level
        self.d = LV_D[level] + shift
        ok = inside(shift.shape, level, row0, col0)
        if mask is not None:
            ok = ok & mask
        self.ok = ok
        self.k = jnp.where(ok, 0.8 / self.d, 0.0)
        self.km = self.k * LV_Q[level]

    def cut(self, lo, hi):
        out = object.__new__(Level)
        out.level = self.level
        out.d, out.k, out.km, out.ok = (
            self.d[lo:hi],
            self.k[lo:hi],
            self.km[lo:hi],
            None,
        )
        return out

    def sweep0(self, v):
        return 0.2 * v + self.km * beside(v)

    def sweep(self, v, kg):
        return 0.2 * v + kg + self.km * beside(v)

    def residual(self, v, g):
        return g - self.d * v + LV_Q[self.level] * beside(v)

    def apply(self, v):
        return self.d * v - LV_Q[self.level] * beside(v)


def mm(x, w):
    m = x.shape[0]
    a = x.astype(BF16)
    r = x - a.astype(F32)
    b = r.astype(BF16)
    c = (r - b.astype(F32)).astype(BF16)
    y = jnp.dot(jnp.concatenate([a, b, c], axis=0), w, preferred_element_type=F32)
    return (y[2 * m :] + y[m : 2 * m]) + y[:m]


def total(x):
    return jnp.sum(jnp.sum(x, axis=0, keepdims=True), axis=1, keepdims=True)


def pick(row, at):
    lane = iota(row.shape, 1)
    return jnp.sum(jnp.where(lane == at, row, 0.0), axis=1, keepdims=True)


def kernel(
    rhs, shf, sol, res,
    xg, xs, kk, kg0, v0, wa, wb, tmp0,
    t1, t2, t3,
    rm, r23, r34, p43, p32, p21, r03,
    s_side, s_line, g_side, g_line, own3, own3g, ownb,
    x2s, x2g, x2h, own2s, own2g, own2h,
    x3a, x3b, own3a, own3b,
    ar_in, ar_a, ar_b,
    e0_ss, e0_rs, s_ss, s_rs, g_ss, g_rs, x2_ss, x2_rs, x3_ss, x3_rs, ar_ss, ar_rs,
):
    gx = lax.axis_index("gx")
    gy = lax.axis_index("gy")
    core = lax.rem(gy, 2)
    quad = lax.div(gy, 2)
    qy, qx = lax.div(quad, 4), lax.rem(quad, 4)

    def near(dz, dy):
        return (lax.rem(gx + (dz + GX), GX), lax.rem(gy + (dy + GY), GY))

    def in_a(dz, dc):
        return (lax.rem(gx + dz, GX), gy - core + lax.rem(core + dc, 2))

    def in_b(dy, dx):
        return (gx, (lax.rem(qy + dy, 4) * 4 + lax.rem(qx + dx, 4)) * 2 + core)

    barrier = pltpu.get_barrier_semaphore()
    partners = (
        [near(*o) for o in AROUND]
        + [in_a(*o) for o in GROUP_A]
        + [in_b(*o) for o in GROUP_B]
    )
    for p in partners:
        pl.semaphore_signal(barrier, inc=1, device_id=p, device_id_type=MESH)

    sent = []

    def send(src, dst, ss, rs, dev):
        cp = pltpu.make_async_remote_copy(
            src_ref=src, dst_ref=dst, send_sem=ss, recv_sem=rs,
            device_id=dev, device_id_type=MESH,
        )
        cp.start()
        sent.append(cp)
        return cp

    i, j = iota((256, 128), 0), iota((256, 128), 1)
    rm[...] = jnp.where((i >> 1) == j, 0.25, 0.0).astype(BF16)
    r03[...] = jnp.where((i >> 3) + 48 == j, 1.0 / 64, 0.0).astype(BF16)
    i, j = iota((128, 128), 0), iota((128, 128), 1)
    r34[...] = jnp.where((i >> 1) == j, 0.25, 0.0).astype(BF16)
    r23[...] = jnp.where((i >> 1) + 32 == j, 0.25, 0.0).astype(BF16)
    p43[...] = jnp.where(i == (j >> 1), 1.0, 0.0).astype(BF16)
    p32[...] = jnp.where(i == (j >> 1) + 32, 1.0, 0.0).astype(BF16)
    i, j = iota((128, 256), 0), iota((128, 256), 1)
    p21[...] = jnp.where(i == (j >> 1), 1.0, 0.0).astype(BF16)

    def pair_rows(ref, rows, lanes):
        return jnp.concatenate(
            [
                ref[t, pl.ds(0, rows // 2, 2), :] + ref[t, pl.ds(1, rows // 2, 2), :]
                for t in range(lanes // 128)
            ],
            axis=1,
        )

    def put(ref, x):
        for t in range(x.shape[1] // 128):
            ref[t, 0 : x.shape[0], :] = x[:, 128 * t : 128 * t + 128]

    def restrict(x, ref, w):
        put(ref, x)
        return mm(pair_rows(ref, x.shape[0], x.shape[1]), w[...])

    def prolong(e, ref, w):
        y = mm(e, w[...])
        m = y.shape[0]
        out = []
        for t in range(y.shape[1] // 128):
            yt = y[:, 128 * t : 128 * t + 128]
            ref[t, pl.ds(0, m, 2), :] = yt
            ref[t, pl.ds(1, m, 2), :] = yt
            out.append(ref[t, 0 : 2 * m, :])
        return jnp.concatenate(out, axis=1) if len(out) > 1 else out[0]

    s0 = shf[...]
    for t in range(2):
        tmp0[t, 0:128, :] = s0[:, 128 * t : 128 * t + 128]
    acc = pair_rows(tmp0, 128, 256)
    put(t1, acc)
    acc = pair_rows(t1, 64, 256)
    put(t2, acc)
    acc = pair_rows(t2, 32, 256)
    own3[...] = mm(acc, r03[...])
    put(t1, s0)
    s1own = mm(pair_rows(t1, 128, 256), rm[...])
    put(t2, s1own)
    s2own = mm(pair_rows(t2, 64, 128), r34[...])
    own2s[...] = pltpu.roll(s2own, 32, axis=1)

    pl.semaphore_wait(barrier, len(partners))

    ROWS = {-1: (0, 32, 160, 192), 1: (96, 128, 0, 32), 0: (0, 128, 32, 160)}
    COLS = {-1: (0, 128, 384, 512), 1: (128, 256, 0, 128), 0: (0, 256, 128, 384)}
    first = []

    def border(f):
        src, dst = (shf, xs) if f else (rhs, xg)
        for n, (dz, dy) in enumerate(AROUND):
            a, b, c, d = ROWS[dz]
            e, g, h, k = COLS[dy]
            first.append(
                send(
                    src.at[a:b, e:g], dst.at[8 + c : 8 + d, h:k],
                    e0_ss.at[f, n], e0_rs.at[f, n], near(dz, dy),
                )
            )

    def side_send(src, buf, ss, rs):
        return [
            send(src, buf.at[n], ss.at[n], rs.at[n], near(0, d))
            for n, d in enumerate(SIDE)
        ]

    def side_join(own, buf, cps):
        for cp in cps:
            cp.wait_recv()
        right1, left1, right2, left2 = (buf[n] for n in range(4))
        lane = iota((16, 128), 1)
        out = jnp.where(lane < 48, pltpu.roll(left1, 96, axis=1), own)
        out = jnp.where(lane < 16, pltpu.roll(left2, 64, axis=1), out)
        out = jnp.where(lane >= 80, pltpu.roll(right1, 32, axis=1), out)
        return jnp.where(lane >= 112, pltpu.roll(right2, 64, axis=1), out)

    def line_send(src, buf, ss, rs):
        return [
            send(
                src, buf.at[16 * (3 - d) : 16 * (4 - d)],
                ss.at[4 + n], rs.at[4 + n], near(d, 0),
            )
            for n, d in enumerate(LINE)
        ]

    SRC2 = {-1: (0, 16), 1: (16, 32), 0: (0, 32)}

    def send2(src, buf, k):
        cps = []
        for n, (dz, dy) in enumerate(AROUND):
            a, b = SRC2[dz]
            cps.append(
                send(
                    src.at[a:b], buf.at[n, 0 : b - a],
                    x2_ss.at[k, n], x2_rs.at[k, n], near(dz, dy),
                )
            )
        return cps

    def lanes3(left, mid, right, lo, hi, move):
        lane = iota(mid.shape, 1)
        out = jnp.where(lane < lo, pltpu.roll(left, 128 - move, axis=1), mid)
        return jnp.where(lane >= hi, pltpu.roll(right, move, axis=1), out)

    def join2(own, buf, cps):
        for cp in cps:
            cp.wait_recv()
        dn, up, rt, lf, dr, dl, ur, ul = range(8)
        return jnp.concatenate(
            [
                lanes3(buf[ul, 0:16], buf[up, 0:16], buf[ur, 0:16], 32, 96, 64),
                lanes3(buf[lf], own, buf[rt], 32, 96, 64),
                lanes3(buf[dl, 0:16], buf[dn, 0:16], buf[dr, 0:16], 32, 96, 64),
            ],
            axis=0,
        )

    SRC3 = {-1: (8, 32), 1: (0, 24), 0: (8, 24)}

    def send3(src, buf, k):
        cps = []
        for n, (dz, dy) in enumerate(AROUND):
            a, b = SRC3[dz]
            cps.append(
                send(
                    src.at[a:b], buf.at[n, 0 : b - a],
                    x3_ss.at[k, n], x3_rs.at[k, n], near(dz, dy),
                )
            )
        return cps

    def join3(own, buf, cps):
        for cp in cps:
            cp.wait_recv()
        dn, up, rt, lf, dr, dl, ur, ul = range(8)
        return jnp.concatenate(
            [
                lanes3(buf[ul], buf[up], buf[ur], 48, 80, 32),
                lanes3(buf[lf, 0:16], own, buf[rt, 0:16], 48, 80, 32),
                lanes3(buf[dl], buf[dn], buf[dr], 48, 80, 32),
            ],
            axis=0,
        )

    def sum_start(row, k):
        ar_in[k, 0] = row
        return [
            send(
                ar_in.at[k, 0], ar_a.at[k, n],
                ar_ss.at[k, 0, n], ar_rs.at[k, 0, n], in_a(*o),
            )
            for n, o in enumerate(GROUP_A)
        ]

    def sum_next(cps, k):
        for cp in cps:
            cp.wait_recv()
        part = ar_in[k, 0] + jnp.sum(ar_a[k], axis=0)
        ar_in[k, 1] = part
        return [
            send(
                ar_in.at[k, 1], ar_b.at[k, n],
                ar_ss.at[k, 1, n], ar_rs.at[k, 1, n], in_b(*o),
            )
            for n, o in enumerate(GROUP_B)
        ]

    def sum_end(cps, k):
        for cp in cps:
            cp.wait_recv()
        return ar_in[k, 1] + jnp.sum(ar_b[k], axis=0)

    side_s = side_send(own3, s_side, s_ss, s_rs)
    border(1)
    border(0)
    cps2s = send2(own2s, x2s, 0)
    xs[8 + 32 : 8 + 160, 128:384] = s0
    xg[8 + 32 : 8 + 160, 128:384] = rhs[...]
    zero8 = jnp.zeros((8, 512), F32)
    for ref in (kg0, v0, wa, wb):
        ref[0:8, :] = zero8
        ref[200:208, :] = zero8

    row0 = gx * 128 - 32
    col0 = gy * 256 - 128
    for cp in first[:8]:
        cp.wait_recv()
    STEP = 16

    def near4(ref, r, n=STEP):
        c = ref[8 + r : 8 + r + n, :]
        around = (
            ref[7 + r : 7 + r + n, :]
            + ref[9 + r : 9 + r + n, :]
            + pltpu.roll(c, 1, axis=1)
            + pltpu.roll(c, 511, axis=1)
        )
        return c, around

    for r in range(0, 192, STEP):
        w = slice(8 + r, 8 + r + STEP)
        ok = inside((STEP, 512), 0, row0 + r, col0)
        kk[w, :] = jnp.where(ok, 0.8 / (4.0 + xs[w, :]), 0.0)
    put(tmp0, xs[8:200, :])
    s1 = jnp.concatenate(
        [
            mm(tmp0_pair(tmp0, t, 192), rm[...])
            for t in range(2)
        ],
        axis=1,
    )
    l1 = Level(1, s1, gx * 64 - 16, gy * 128 - 64)
    s2 = restrict(s1, t1, rm)

    s_row = side_join(own3[...], s_side, side_s)
    ownb[0] = s_row
    line_s = line_send(ownb.at[0], s_line, s_ss, s_rs)
    s_line[48:64] = s_row

    for cp in first[8:]:
        cp.wait_recv()
    for r in range(0, 192, STEP):
        w = slice(8 + r, 8 + r + STEP)
        kg0[w, :] = kk[w, :] * xg[w, :]
    for r in range(0, 192, STEP):
        w = slice(8 + r, 8 + r + STEP)
        c, around = near4(kg0, r)
        v0[w, :] = 1.2 * c + kk[w, :] * around
    for r in range(0, 192, STEP):
        w = slice(8 + r, 8 + r + STEP)
        c, around = near4(v0, r)
        out = xg[w, :] - (4.0 + xs[w, :]) * c + around
        for t in range(4):
            tmp0[t, r : r + STEP, :] = out[:, 128 * t : 128 * t + 128]
    g1 = jnp.concatenate([mm(tmp0_pair(tmp0, t, 192), rm[...]) for t in range(2)], axis=1)

    kg1 = l1.k * g1
    v1 = l1.sweep(kg1, kg1)
    g2 = restrict(l1.residual(v1, g1), t1, rm)
    l2a = Level(2, s2, gx * 32 - 8, gy * 64 - 32)
    kg = l2a.k * g2
    r2 = l2a.residual(l2a.sweep(kg, kg), g2)
    own2g[...] = g2[8:40]
    g3 = restrict(r2, t2, r23)
    g3own = g3[4:20]
    own3g[...] = g3own
    side_g = side_send(own3g, g_side, g_ss, g_rs)
    cps2g = send2(own2g, x2g, 1)

    for cp in line_s:
        cp.wait_recv()
    l3 = Level(3, s_line[...], gx * 16 - 48, gy * 32 - 48)
    s4 = restrict(s_line[...], t3, r34)
    l4 = Level(4, s4, gx * 8 - 24, gy * 16 - 24, iota((56, 128), 1) < 64)

    g_row = side_join(g3own, g_side, side_g)
    ownb[1] = g_row
    line_g = line_send(ownb.at[1], g_line, g_ss, g_rs)
    g_line[48:64] = g_row

    one4 = jnp.where(l4.ok, 1.0, 0.0)
    one3 = jnp.where(l3.ok, 1.0, 0.0)
    w6 = one4
    for _ in range(6):
        w6 = l4.sweep0(w6)
    w12 = w6
    for _ in range(6):
        w12 = l4.sweep0(w12)
    y3 = l3.sweep0(l3.sweep0(one3))
    u = l3.sweep0(l3.sweep0(y3))
    q = 4.0 * restrict(jnp.where(l3.ok, l3.apply(u), 0.0), t3, r34)
    kq = l4.k * q
    z = kq
    for _ in range(11):
        z = l4.sweep(z, kq)
    f3 = l3.sweep0(l3.sweep0(u - 0.25 * prolong(z, t3, p43)))
    f2 = l3.sweep0(l3.sweep0(prolong(w6, t3, p43)))
    lane3 = (iota((16, 128), 1) >= 48) & (iota((16, 128), 1) < 80)
    lane4 = (iota((8, 128), 1) >= 24) & (iota((8, 128), 1) < 40)
    g3m = jnp.where(lane3, g3own, 0.0)

    def own4(x):
        return jnp.where(lane4, x[24:32], 0.0)

    parts = [
        0.25 * total(y3[48:64] * g3m),
        0.25 * total(f2[48:64] * g3m),
        total(f3[48:64] * g3m),
        total(own4(l4.apply(one4))),
        total(own4(l4.apply(w6))),
        total(own4(q * w12)),
        total(own4(q * w6)),
    ]
    lane = iota((1, 128), 1)
    row = jnp.zeros((1, 128), F32)
    for n, p in enumerate(parts):
        row = jnp.where(lane == n, p, row)
    sums1 = sum_start(row, 0)

    s2w = join2(own2s[...], x2s, cps2s)
    l2 = Level(2, s2w, gx * 32 - 16, gy * 64 - 32)
    y2 = l2.sweep0(l2.sweep0(prolong(y3[40:72], t2, p32)))
    f4 = l2.sweep0(l2.sweep0(y2))
    f5 = l1.sweep0(l1.sweep0(prolong(y2[8:56], t1, p21)))
    f5 = l1.sweep0(l1.sweep0(f5))

    sums1 = sum_next(sums1, 0)

    for cp in line_g:
        cp.wait_recv()
    G3 = g_line[...]
    kg3 = l3.k * G3
    v3 = l3.sweep(kg3, kg3)
    g4 = restrict(l3.residual(v3, G3), t3, r34)
    kg4 = l4.k * g4
    e4 = kg4
    for _ in range(11):
        e4 = l4.sweep(e4, kg4)
    g2w = join2(own2g[...], x2g, cps2g)
    kg2 = l2.k * g2w
    v2 = l2.sweep(kg2, kg2)

    tot = sum_end(sums1, 0)
    a1, a2, a3, ones_total, w6_total, qw12, qw6 = (pick(tot, n) for n in range(7))
    inv = 1.0 / ones_total
    c1 = a1 * inv
    c2 = (a2 - c1 * w6_total) * inv
    c3 = 0.25 * (a3 - c1 * qw12 - c2 * qw6) * inv
    e4 = e4 + c1 * w12 + c2 * w6
    x3 = v3 + prolong(e4, t3, p43)
    for _ in range(4):
        x3 = l3.sweep(x3, kg3)
    g4 = restrict(l3.residual(x3, G3), t3, r34)
    kg4 = l4.k * g4
    e4 = kg4
    for _ in range(5):
        e4 = l4.sweep(e4, kg4)
    e4 = e4 + c3 * w6
    x3 = x3 + prolong(e4, t3, p43)
    for _ in range(2):
        x3 = l3.sweep(x3, kg3)

    lane2 = (iota((32, 128), 1) >= 32) & (iota((32, 128), 1) < 96)
    x2 = v2 + prolong(x3[40:72], t2, p32)
    r2 = l2.residual(x2, g2w)
    part = total(jnp.where(lane2, f4[16:48] * r2[16:48], 0.0)) * (1.0 / 16)
    sums2 = sum_start(jnp.zeros((1, 128), F32) + part, 1)
    for _ in range(4):
        x2 = l2.sweep(x2, kg2)
    g3 = restrict(l2.residual(x2, g2w), t2, r23)
    own3a[...] = g3
    cps3 = send3(own3a, x3a, 0)
    l3b = l3.cut(24, 88)
    l4b = l4.cut(12, 44)
    w6b = w6[12:44]

    def coarse(g3_own, buf, cps, sums, k):
        G = join3(g3_own, buf, cps)
        kgc = l3b.k * G
        v = l3b.sweep(kgc, kgc)
        gc = restrict(l3b.residual(v, G), t3, r34)
        sums = sum_next(sums, k)
        kgd = l4b.k * gc
        e = kgd
        for _ in range(5):
            e = l4b.sweep(e, kgd)
        c = sum_end(sums, k)[:, 0:1] * inv
        x = v + prolong(e + c * w6b, t3, p43)
        for _ in range(2):
            x = l3b.sweep(x, kgc)
        return x[16:48]

    e3 = coarse(g3[8:24], x3a, cps3, sums2, 1)
    x2 = x2 + prolong(e3, t2, p32)
    for _ in range(2):
        x2 = l2.sweep(x2, kg2)

    x1 = v1 + prolong(x2[8:56], t1, p21)
    r1 = l1.residual(x1, g1)
    lane1 = (iota((64, 256), 1) >= 64) & (iota((64, 256), 1) < 192)
    part = total(jnp.where(lane1, f5[16:80] * r1[16:80], 0.0)) * (1.0 / 64)
    sums3 = sum_start(jnp.zeros((1, 128), F32) + part, 2)
    for _ in range(4):
        x1 = l1.sweep(x1, kg1)
    g2 = restrict(l1.residual(x1, g1), t1, rm)
    pad = jnp.zeros((8, 128), F32)
    g2 = jnp.concatenate([pad, g2, pad], axis=0)
    kg = l2.k * g2
    g3 = restrict(l2.residual(l2.sweep(kg, kg), g2), t2, r23)
    own3b[...] = g3
    cps3 = send3(own3b, x3b, 1)
    own2h[...] = g2[16:48]
    cps2h = send2(own2h, x2h, 2)
    e3 = coarse(g3[8:24], x3b, cps3, sums3, 2)
    g2 = join2(own2h[...], x2h, cps2h)
    kg2 = l2.k * g2
    x2 = l2.sweep(kg2, kg2) + prolong(e3, t2, p32)
    for _ in range(2):
        x2 = l2.sweep(x2, kg2)
    x1 = x1 + prolong(x2[8:56], t1, p21)
    for _ in range(2):
        x1 = l1.sweep(x1, kg1)

    for t in range(2):
        y = mm(x1[:, 128 * t : 128 * t + 128], p21[...])
        for h in range(2):
            tmp0[2 * t + h, pl.ds(0, 96, 2), :] = y[:, 128 * h : 128 * h + 128]
            tmp0[2 * t + h, pl.ds(1, 96, 2), :] = y[:, 128 * h : 128 * h + 128]
    for r in range(16, 176, STEP):
        w = slice(8 + r, 8 + r + STEP)
        e = jnp.concatenate([tmp0[t, r : r + STEP, :] for t in range(4)], axis=1)
        wa[w, :] = v0[w, :] + e
    for src, dst in ((wa, wb), (wb, wa)):
        for r in range(16, 176, STEP):
            w = slice(8 + r, 8 + r + STEP)
            c, around = near4(src, r)
            dst[w, :] = 0.2 * c + kg0[w, :] + kk[w, :] * around
    for r in range(32, 160, STEP):
        w = slice(8 + r, 8 + r + STEP)
        c, around = near4(wa, r)
        sol[r - 32 : r - 32 + STEP, :] = c[:, 128:384]
        out = rhs[r - 32 : r - 32 + STEP, :] + around[:, 128:384]
        out = out - (4.0 + shf[r - 32 : r - 32 + STEP, :]) * c[:, 128:384]
        res[r - 32 : r - 32 + STEP, :] = out
    for cp in sent:
        cp.wait_send()


def tmp0_pair(ref, t, rows):
    return jnp.concatenate(
        [
            ref[2 * t + h, pl.ds(0, rows // 2, 2), :] + ref[2 * t + h, pl.ds(1, rows // 2, 2), :]
            for h in range(2)
        ],
        axis=1,
    )


def body(right_side, shift):
    v = pltpu.VMEM
    dma = pltpu.SemaphoreType.DMA
    big = v((208, 512), F32)
    scratch = (
        [big] * 7
        + [v((4, 192, 128), F32)]
        + [v((2, 128, 128), F32), v((2, 128, 128), F32), v((1, 112, 128), F32)]
        + [v((256, 128), BF16)]
        + [v((128, 128), BF16)] * 4
        + [v((128, 256), BF16), v((256, 128), BF16)]
        + [v((4, 16, 128), F32), v((112, 128), F32)] * 2
        + [v((16, 128), F32)] * 2
        + [v((2, 16, 128), F32)]
        + [v((8, 32, 128), F32)] * 3
        + [v((32, 128), F32)] * 3
        + [v((8, 24, 128), F32)] * 2
        + [v((32, 128), F32)] * 2
        + [v((3, 2, 1, 128), F32), v((3, 15, 1, 128), F32), v((3, 15, 1, 128), F32)]
        + [dma((2, 8))] * 2
        + [dma((10,))] * 4
        + [dma((3, 8))] * 2
        + [dma((2, 8))] * 2
        + [dma((3, 2, 15))] * 2
    )
    shape = jax.ShapeDtypeStruct((128, 256), F32)
    vm = pl.BlockSpec(memory_space=pltpu.VMEM)
    return pl.pallas_call(
        kernel,
        out_shape=(shape, shape),
        in_specs=[vm, vm],
        out_specs=(vm, vm),
        scratch_shapes=scratch,
        compiler_params=pltpu.CompilerParams(
            collective_id=0, has_side_effects=True, vmem_limit_bytes=32 * 1024 * 1024
        ),
        name="fcycle",
    )(right_side, shift)


def solution(mesh):
    spec = P("gx", "gy")
    return jax.shard_map(
        body, mesh=mesh, in_specs=(spec, spec), out_specs=(spec, spec), check_vma=False
    )
```

```python
import jax
import jax.numpy as jnp
from jax import lax
from jax.experimental import pallas as pl
from jax.experimental.pallas import tpu as pltpu
from jax.sharding import PartitionSpec as P

MESH = pl.DeviceIdType.MESH
F32 = jnp.float32
BF16 = jnp.bfloat16
GX, GY = 8, 32
NX, NY = 1024, 8192
LV_Q = [4.0 ** (-l) for l in range(5)]
LV_D = [4.0 ** (1 - l) for l in range(5)]

AROUND = [(-1, 0), (1, 0), (0, -1), (0, 1), (-1, -1), (-1, 1), (1, -1), (1, 1)]
SIDE = [-1, 1, -2, 2]
LINE = [-1, 1, -2, 2, -3, 3]
GROUP_A = [(dz, dc) for dz in range(8) for dc in range(2) if dz or dc]
GROUP_B = [(dy, dx) for dy in range(4) for dx in range(4) if dy or dx]


def iota(shape, dim):
    return lax.broadcasted_iota(jnp.int32, shape, dim)


def beside(v):
    r, c = v.shape
    return (
        pltpu.roll(v, 1, axis=0)
        + pltpu.roll(v, r - 1, axis=0)
        + pltpu.roll(v, 1, axis=1)
        + pltpu.roll(v, c - 1, axis=1)
    )


def inside(shape, level, row0, col0):
    rows = iota(shape, 0) + row0
    cols = iota(shape, 1) + col0
    return (
        (rows >= 0) & (rows < (NX >> level)) & (cols >= 0) & (cols < (NY >> level))
    )


class Level:
    def __init__(self, level, shift, row0, col0, mask=None):
        self.level = level
        self.d = LV_D[level] + shift
        ok = inside(shift.shape, level, row0, col0)
        if mask is not None:
            ok = ok & mask
        self.ok = ok
        self.k = jnp.where(ok, 0.8 / self.d, 0.0)
        self.km = self.k * LV_Q[level]

    def cut(self, lo, hi):
        out = object.__new__(Level)
        out.level = self.level
        out.d, out.k, out.km, out.ok = (
            self.d[lo:hi],
            self.k[lo:hi],
            self.km[lo:hi],
            None,
        )
        return out

    def sweep0(self, v):
        return 0.2 * v + self.km * beside(v)

    def sweep(self, v, kg):
        return 0.2 * v + kg + self.km * beside(v)

    def residual(self, v, g):
        return g - self.d * v + LV_Q[self.level] * beside(v)

    def apply(self, v):
        return self.d * v - LV_Q[self.level] * beside(v)


def mm(x, w):
    m = x.shape[0]
    a = x.astype(BF16)
    r = x - a.astype(F32)
    b = r.astype(BF16)
    c = (r - b.astype(F32)).astype(BF16)
    y = jnp.dot(jnp.concatenate([a, b, c], axis=0), w, preferred_element_type=F32)
    return (y[2 * m :] + y[m : 2 * m]) + y[:m]


def total(x):
    return jnp.sum(jnp.sum(x, axis=0, keepdims=True), axis=1, keepdims=True)


def pick(row, at):
    lane = iota(row.shape, 1)
    return jnp.sum(jnp.where(lane == at, row, 0.0), axis=1, keepdims=True)


def kernel(
    rhs_in, shf_in, sol, res,
    xg, xs, kk, kg0, v0, wa, wb, tmp0,
    t1s, t2s, t3s,
    rm, r23, r34, p43, p32, p21, r03,
    s_side, s_line, g_side, g_line, own3, own3g, ownb,
    x2b, own2, x3b, own3n,
    ar_in, ar_a, ar_b,
    e0_ss, e0_rs, s_ss, s_rs, g_ss, g_rs, x2_ss, x2_rs, x3_ss, x3_rs, ar_ss, ar_rs, in_s,
):
    gx = lax.axis_index("gx")
    gy = lax.axis_index("gy")
    core = lax.rem(gy, 2)
    quad = lax.div(gy, 2)
    qy, qx = lax.div(quad, 4), lax.rem(quad, 4)

    def near(dz, dy):
        return (lax.rem(gx + (dz + GX), GX), lax.rem(gy + (dy + GY), GY))

    def in_a(dz, dc):
        return (lax.rem(gx + dz, GX), gy - core + lax.rem(core + dc, 2))

    def in_b(dy, dx):
        return (gx, (lax.rem(qy + dy, 4) * 4 + lax.rem(qx + dx, 4)) * 2 + core)

    barrier = pltpu.get_barrier_semaphore()
    partners = (
        [near(*o) for o in AROUND]
        + [in_a(*o) for o in GROUP_A]
        + [in_b(*o) for o in GROUP_B]
    )
    for p in partners:
        pl.semaphore_signal(barrier, inc=1, device_id=p, device_id_type=MESH)

    mid = (slice(40, 168), slice(128, 384))
    rhs, shf = xg.at[mid], xs.at[mid]
    in_shf = pltpu.make_async_copy(shf_in, shf, in_s.at[0])
    in_rhs = pltpu.make_async_copy(rhs_in, rhs, in_s.at[1])
    in_shf.start()
    in_rhs.start()

    sent = []
    turn = [0]

    def scratch(pool):
        turn[0] += 1
        return pool.at[turn[0] % pool.shape[0]]

    def send(src, dst, ss, rs, dev):
        cp = pltpu.make_async_remote_copy(
            src_ref=src, dst_ref=dst, send_sem=ss, recv_sem=rs,
            device_id=dev, device_id_type=MESH,
        )
        cp.start()
        sent.append(cp)
        return cp

    i, j = iota((256, 128), 0), iota((256, 128), 1)
    rm[...] = jnp.where((i >> 1) == j, 0.25, 0.0).astype(BF16)
    r03[...] = jnp.where((i >> 3) + 48 == j, 1.0 / 64, 0.0).astype(BF16)
    i, j = iota((128, 128), 0), iota((128, 128), 1)
    r34[...] = jnp.where((i >> 1) == j, 0.25, 0.0).astype(BF16)
    r23[...] = jnp.where((i >> 1) + 32 == j, 0.25, 0.0).astype(BF16)
    p43[...] = jnp.where(i == (j >> 1), 1.0, 0.0).astype(BF16)
    p32[...] = jnp.where(i == (j >> 1) + 32, 1.0, 0.0).astype(BF16)
    i, j = iota((128, 256), 0), iota((128, 256), 1)
    p21[...] = jnp.where(i == (j >> 1), 1.0, 0.0).astype(BF16)

    def pair_rows(ref, rows, lanes):
        return jnp.concatenate(
            [
                ref[t, pl.ds(0, rows // 2, 2), :] + ref[t, pl.ds(1, rows // 2, 2), :]
                for t in range(lanes // 128)
            ],
            axis=1,
        )

    def put(ref, x):
        for t in range(x.shape[1] // 128):
            ref[t, 0 : x.shape[0], :] = x[:, 128 * t : 128 * t + 128]

    def restrict(x, pool, w):
        ref = scratch(pool)
        put(ref, x)
        return mm(pair_rows(ref, x.shape[0], x.shape[1]), w[...])

    def prolong(e, pool, w):
        ref = scratch(pool)
        y = mm(e, w[...])
        m = y.shape[0]
        out = []
        for t in range(y.shape[1] // 128):
            yt = y[:, 128 * t : 128 * t + 128]
            ref[t, pl.ds(0, m, 2), :] = yt
            ref[t, pl.ds(1, m, 2), :] = yt
            out.append(ref[t, 0 : 2 * m, :])
        return jnp.concatenate(out, axis=1) if len(out) > 1 else out[0]

    zero8 = jnp.zeros((8, 512), F32)
    for ref in (kg0, v0, wa, wb):
        ref[0:8, :] = zero8
        ref[200:208, :] = zero8
    for ref in (xs, xg):
        ref[8:16, :] = zero8
        ref[192:200, :] = zero8

    in_shf.wait()
    s0 = shf[...]
    put(tmp0, s0)
    acc = pair_rows(tmp0, 128, 256)
    s1own = mm(acc, rm[...])
    ref1, ref2 = scratch(t1s), scratch(t2s)
    put(ref1, acc)
    acc = pair_rows(ref1, 64, 256)
    put(ref2, acc)
    own3[...] = mm(pair_rows(ref2, 32, 256), r03[...])
    own2[0] = pltpu.roll(restrict(s1own, t1s, r34), 32, axis=1)
    in_rhs.wait()

    pl.semaphore_wait(barrier, len(partners))

    ROWS = {-1: (0, 24, 160, 184), 1: (104, 128, 8, 32), 0: (0, 128, 32, 160)}
    COLS = {-1: (0, 128, 384, 512), 1: (128, 256, 0, 128), 0: (0, 256, 128, 384)}
    first = []

    def border(f):
        src, dst = (shf, xs) if f else (rhs, xg)
        for n, (dz, dy) in enumerate(AROUND):
            a, b, c, d = ROWS[dz]
            e, g, h, k = COLS[dy]
            first.append(
                send(
                    src.at[a:b, e:g], dst.at[8 + c : 8 + d, h:k],
                    e0_ss.at[f, n], e0_rs.at[f, n], near(dz, dy),
                )
            )

    def side_send(src, buf, ss, rs):
        return [
            send(src, buf.at[n], ss.at[n], rs.at[n], near(0, d))
            for n, d in enumerate(SIDE)
        ]

    def side_join(own, buf, cps):
        for cp in cps:
            cp.wait_recv()
        right1, left1, right2, left2 = (buf[n] for n in range(4))
        lane = iota((16, 128), 1)
        out = jnp.where(lane < 48, pltpu.roll(left1, 96, axis=1), own)
        out = jnp.where(lane < 16, pltpu.roll(left2, 64, axis=1), out)
        out = jnp.where(lane >= 80, pltpu.roll(right1, 32, axis=1), out)
        return jnp.where(lane >= 112, pltpu.roll(right2, 64, axis=1), out)

    def line_send(src, buf, ss, rs):
        return [
            send(
                src, buf.at[16 * (3 - d) : 16 * (4 - d)],
                ss.at[4 + n], rs.at[4 + n], near(d, 0),
            )
            for n, d in enumerate(LINE)
        ]

    SRC2 = {-1: (0, 16), 1: (16, 32), 0: (0, 32)}

    def send2(x, k):
        own2[k] = x
        src, buf = own2.at[k], x2b.at[k]
        cps = []
        for n, (dz, dy) in enumerate(AROUND):
            a, b = SRC2[dz]
            cps.append(
                send(
                    src.at[a:b], buf.at[n, 0 : b - a],
                    x2_ss.at[k, n], x2_rs.at[k, n], near(dz, dy),
                )
            )
        return cps

    def lanes3(left, mid, right, lo, hi, move):
        lane = iota(mid.shape, 1)
        out = jnp.where(lane < lo, pltpu.roll(left, 128 - move, axis=1), mid)
        return jnp.where(lane >= hi, pltpu.roll(right, move, axis=1), out)

    def join2(k, cps):
        for cp in cps:
            cp.wait_recv()
        own, buf = own2[k], x2b.at[k]
        dn, up, rt, lf, dr, dl, ur, ul = range(8)
        return jnp.concatenate(
            [
                lanes3(buf[ul, 0:16], buf[up, 0:16], buf[ur, 0:16], 32, 96, 64),
                lanes3(buf[lf], own, buf[rt], 32, 96, 64),
                lanes3(buf[dl, 0:16], buf[dn, 0:16], buf[dr, 0:16], 32, 96, 64),
            ],
            axis=0,
        )

    SRC3 = {-1: (8, 32), 1: (0, 24), 0: (8, 24)}

    def send3(x, k):
        own3n[k] = x
        src, buf = own3n.at[k], x3b.at[k]
        cps = []
        for n, (dz, dy) in enumerate(AROUND):
            a, b = SRC3[dz]
            cps.append(
                send(
                    src.at[a:b], buf.at[n, 0 : b - a],
                    x3_ss.at[k, n], x3_rs.at[k, n], near(dz, dy),
                )
            )
        return cps

    def join3(k, cps):
        for cp in cps:
            cp.wait_recv()
        own, buf = own3n[k, 8:24], x3b.at[k]
        dn, up, rt, lf, dr, dl, ur, ul = range(8)
        return jnp.concatenate(
            [
                lanes3(buf[ul], buf[up], buf[ur], 48, 80, 32),
                lanes3(buf[lf, 0:16], own, buf[rt, 0:16], 48, 80, 32),
                lanes3(buf[dl], buf[dn], buf[dr], 48, 80, 32),
            ],
            axis=0,
        )

    def sum_start(row, k):
        ar_in[k, 0] = row
        return [
            send(
                ar_in.at[k, 0], ar_a.at[k, n],
                ar_ss.at[k, 0, n], ar_rs.at[k, 0, n], in_a(*o),
            )
            for n, o in enumerate(GROUP_A)
        ]

    def sum_next(cps, k):
        for cp in cps:
            cp.wait_recv()
        part = ar_in[k, 0] + jnp.sum(ar_a[k], axis=0)
        ar_in[k, 1] = part
        return [
            send(
                ar_in.at[k, 1], ar_b.at[k, n],
                ar_ss.at[k, 1, n], ar_rs.at[k, 1, n], in_b(*o),
            )
            for n, o in enumerate(GROUP_B)
        ]

    def sum_end(cps, k):
        for cp in cps:
            cp.wait_recv()
        return ar_in[k, 1] + jnp.sum(ar_b[k], axis=0)

    side_s = side_send(own3, s_side, s_ss, s_rs)
    border(1)
    border(0)
    cps2s = send2(own2[0], 0)
    s_row = side_join(own3[...], s_side, side_s)
    ownb[0] = s_row
    line_s = line_send(ownb.at[0], s_line, s_ss, s_rs)
    s_line[48:64] = s_row

    row0 = gx * 128 - 32
    col0 = gy * 256 - 128
    for cp in first[:8]:
        cp.wait_recv()
    STEP = 16

    def near4(ref, r, n=STEP):
        c = ref[8 + r : 8 + r + n, :]
        around = (
            ref[7 + r : 7 + r + n, :]
            + ref[9 + r : 9 + r + n, :]
            + pltpu.roll(c, 1, axis=1)
            + pltpu.roll(c, 511, axis=1)
        )
        return c, around

    for r in range(0, 192, STEP):
        w = slice(8 + r, 8 + r + STEP)
        ok = inside((STEP, 512), 0, row0 + r, col0)
        kk[w, :] = jnp.where(ok, 0.8 / (4.0 + xs[w, :]), 0.0)
    put(tmp0, xs[8:200, :])
    s1 = jnp.concatenate(
        [
            mm(tmp0_pair(tmp0, t, 192), rm[...])
            for t in range(2)
        ],
        axis=1,
    )
    l1 = Level(1, s1, gx * 64 - 16, gy * 128 - 64)
    s2 = restrict(s1, t1s, rm)
    l2a = Level(2, s2, gx * 32 - 8, gy * 64 - 32)

    for cp in first[8:]:
        cp.wait_recv()
    for r in range(0, 192, STEP):
        w = slice(8 + r, 8 + r + STEP)
        kg0[w, :] = kk[w, :] * xg[w, :]
    for r in range(0, 192, STEP):
        w = slice(8 + r, 8 + r + STEP)
        c, around = near4(kg0, r)
        v0[w, :] = 1.2 * c + kk[w, :] * around
    for r in range(0, 192, STEP):
        w = slice(8 + r, 8 + r + STEP)
        c, around = near4(v0, r)
        out = xg[w, :] - (4.0 + xs[w, :]) * c + around
        for t in range(4):
            tmp0[t, r : r + STEP, :] = out[:, 128 * t : 128 * t + 128]
    g1 = jnp.concatenate([mm(tmp0_pair(tmp0, t, 192), rm[...]) for t in range(2)], axis=1)

    kg1 = l1.k * g1
    v1 = l1.sweep(kg1, kg1)
    g2 = restrict(l1.residual(v1, g1), t1s, rm)
    kg = l2a.k * g2
    r2 = l2a.residual(l2a.sweep(kg, kg), g2)
    g3 = restrict(r2, t2s, r23)
    g3own = g3[4:20]
    own3g[...] = g3own
    side_g = side_send(own3g, g_side, g_ss, g_rs)
    cps2g = send2(g2[8:40], 1)

    for cp in line_s:
        cp.wait_recv()
    l3 = Level(3, s_line[...], gx * 16 - 48, gy * 32 - 48)
    s4 = restrict(s_line[...], t3s, r34)
    l4 = Level(4, s4, gx * 8 - 24, gy * 16 - 24, iota((56, 128), 1) < 64)

    one4 = jnp.where(l4.ok, 1.0, 0.0)
    one3 = jnp.where(l3.ok, 1.0, 0.0)
    w6 = one4
    for _ in range(6):
        w6 = l4.sweep0(w6)
    w12 = w6
    for _ in range(6):
        w12 = l4.sweep0(w12)
    y3 = l3.sweep0(l3.sweep0(one3))
    u = l3.sweep0(l3.sweep0(y3))
    q = 4.0 * restrict(jnp.where(l3.ok, l3.apply(u), 0.0), t3s, r34)
    kq = l4.k * q
    z = kq
    for _ in range(11):
        z = l4.sweep(z, kq)
    f3 = l3.sweep0(l3.sweep0(u - 0.25 * prolong(z, t3s, p43)))
    f2 = l3.sweep0(l3.sweep0(prolong(w6, t3s, p43)))
    lane3 = (iota((16, 128), 1) >= 48) & (iota((16, 128), 1) < 80)
    lane4 = (iota((8, 128), 1) >= 24) & (iota((8, 128), 1) < 40)
    g3m = jnp.where(lane3, g3own, 0.0)

    def own4(x):
        return jnp.where(lane4, x[24:32], 0.0)

    parts = [
        0.25 * total(y3[48:64] * g3m),
        0.25 * total(f2[48:64] * g3m),
        total(f3[48:64] * g3m),
        total(own4(l4.apply(one4))),
        total(own4(l4.apply(w6))),
        total(own4(q * w12)),
        total(own4(q * w6)),
    ]
    lane = iota((1, 128), 1)
    row = jnp.zeros((1, 128), F32)
    for n, p in enumerate(parts):
        row = jnp.where(lane == n, p, row)
    sums1 = sum_start(row, 0)

    g_row = side_join(g3own, g_side, side_g)
    ownb[1] = g_row
    line_g = line_send(ownb.at[1], g_line, g_ss, g_rs)
    g_line[48:64] = g_row

    def down2(x):
        pad = jnp.zeros((8, 128), F32)
        g = jnp.concatenate([pad, x, pad], axis=0)
        kg = l2.k * g
        g3 = restrict(l2.residual(l2.sweep(kg, kg), g), t2s, r23)
        return g, g3

    s2w = join2(0, cps2s)
    l2 = Level(2, s2w, gx * 32 - 16, gy * 64 - 32)
    lane1 = (iota((64, 256), 1) >= 64) & (iota((64, 256), 1) < 192)
    lane2 = (iota((32, 128), 1) >= 32) & (iota((32, 128), 1) < 96)
    y2 = l2.sweep0(l2.sweep0(prolong(y3[40:72], t2s, p32)))
    z2 = l2.sweep0(l2.sweep0(prolong(f2[40:72], t2s, p32)))
    f4 = l2.sweep0(l2.sweep0(y2))
    f5 = l1.sweep0(l1.sweep0(prolong(y2[8:56], t1s, p21)))
    f5 = l1.sweep0(l1.sweep0(f5))
    z1 = prolong(z2[8:56], t1s, p21)
    p5r = total(jnp.where(lane1, f5[16:80] * l1.apply(z1)[16:80], 0.0)) * (-1.0 / 64)
    w1 = l1.sweep0(l1.sweep0(z1))
    d1 = l1.sweep0(l1.sweep0(w1))
    h2, h3 = down2(restrict(-l1.apply(d1), t1s, rm))
    cps3r = send3(h3, 2)
    cps2r = send2(h2[16:48], 3)

    sums1 = sum_next(sums1, 0)

    for cp in line_g:
        cp.wait_recv()
    G3 = g_line[...]
    kg3 = l3.k * G3
    v3 = l3.sweep(kg3, kg3)
    g4 = restrict(l3.residual(v3, G3), t3s, r34)
    kg4 = l4.k * g4
    e4 = kg4
    for _ in range(11):
        e4 = l4.sweep(e4, kg4)
    g2w = join2(1, cps2g)
    kg2 = l2.k * g2w
    v2 = l2.sweep(kg2, kg2)

    tot = sum_end(sums1, 0)
    a1, a2, a3, ones_total, w6_total, qw12, qw6 = (pick(tot, n) for n in range(7))
    inv = 1.0 / ones_total
    c1 = a1 * inv
    c2 = (a2 - c1 * w6_total) * inv
    c3 = 0.25 * (a3 - c1 * qw12 - c2 * qw6) * inv
    e4 = e4 + c1 * w12 + c2 * w6
    x3 = v3 + prolong(e4, t3s, p43)
    for _ in range(4):
        x3 = l3.sweep(x3, kg3)
    g4 = restrict(l3.residual(x3, G3), t3s, r34)
    kg4 = l4.k * g4
    e4 = kg4
    for _ in range(5):
        e4 = l4.sweep(e4, kg4)
    e4 = e4 + c3 * w6
    x3 = x3 + prolong(e4, t3s, p43)
    for _ in range(2):
        x3 = l3.sweep(x3, kg3)

    x2 = v2 + prolong(x3[40:72], t2s, p32)
    r2 = l2.residual(x2, g2w)
    p4 = total(jnp.where(lane2, f4[16:48] * r2[16:48], 0.0)) * (1.0 / 16)
    sums2 = sum_start(jnp.where(lane == 0, p4, jnp.where(lane == 1, p5r, 0.0)), 1)
    for _ in range(4):
        x2 = l2.sweep(x2, kg2)
    cps3 = send3(restrict(l2.residual(x2, g2w), t2s, r23), 0)
    l3b = l3.cut(24, 88)
    l4b = l4.cut(12, 44)

    def coarse(G):
        kgc = l3b.k * G
        v = l3b.sweep(kgc, kgc)
        kgd = l4b.k * restrict(l3b.residual(v, G), t3s, r34)
        e = kgd
        for _ in range(5):
            e = l4b.sweep(e, kgd)
        x = v + prolong(e, t3s, p43)
        for _ in range(2):
            x = l3b.sweep(x, kgc)
        return x[16:48]

    def up2(e3, g):
        kg = l2.k * g
        x = l2.sweep(kg, kg) + prolong(e3, t2s, p32)
        for _ in range(2):
            x = l2.sweep(x, kg)
        return x

    e3 = coarse(join3(2, cps3r))
    x2r = up2(e3, join2(3, cps2r))
    x1r = l1.sweep0(l1.sweep0(d1 + prolong(x2r[8:56], t1s, p21)))

    x2 = x2 + prolong(coarse(join3(0, cps3)), t2s, p32)
    for _ in range(2):
        x2 = l2.sweep(x2, kg2)

    x1 = v1 + prolong(x2[8:56], t1s, p21)
    r1 = l1.residual(x1, g1)
    p5 = total(jnp.where(lane1, f5[16:80] * r1[16:80], 0.0)) * (1.0 / 64)
    sums3 = sum_start(jnp.zeros((1, 128), F32) + p5, 2)
    for _ in range(4):
        x1 = l1.sweep(x1, kg1)
    g2, g3 = down2(restrict(l1.residual(x1, g1), t1s, rm))
    cps3 = send3(g3, 1)
    cps2h = send2(g2[16:48], 2)
    sums2 = sum_next(sums2, 1)
    sums3 = sum_next(sums3, 2)
    e3 = coarse(join3(1, cps3))
    x2 = up2(e3, join2(2, cps2h))
    x1 = x1 + prolong(x2[8:56], t1s, p21)
    for _ in range(2):
        x1 = l1.sweep(x1, kg1)
    tot2 = sum_end(sums2, 1)
    c4 = pick(tot2, 0) * inv
    p5r = pick(tot2, 1)
    x1 = x1 + c4 * x1r
    tot3 = sum_end(sums3, 2)
    c5 = (tot3[:, 0:1] + c4 * p5r) * inv
    x1 = x1 + c5 * w1

    for t in range(2):
        y = mm(x1[:, 128 * t : 128 * t + 128], p21[...])
        for h in range(2):
            tmp0[2 * t + h, pl.ds(0, 96, 2), :] = y[:, 128 * h : 128 * h + 128]
            tmp0[2 * t + h, pl.ds(1, 96, 2), :] = y[:, 128 * h : 128 * h + 128]
    for r in range(16, 176, STEP):
        w = slice(8 + r, 8 + r + STEP)
        e = jnp.concatenate([tmp0[t, r : r + STEP, :] for t in range(4)], axis=1)
        wa[w, :] = v0[w, :] + e
    for src, dst in ((wa, wb), (wb, wa)):
        for r in range(16, 176, STEP):
            w = slice(8 + r, 8 + r + STEP)
            c, around = near4(src, r)
            dst[w, :] = 0.2 * c + kg0[w, :] + kk[w, :] * around
    for r in range(32, 160, STEP):
        w = slice(8 + r, 8 + r + STEP)
        c, around = near4(wa, r)
        sol[r - 32 : r - 32 + STEP, :] = c[:, 128:384]
        out = rhs[r - 32 : r - 32 + STEP, :] + around[:, 128:384]
        out = out - (4.0 + shf[r - 32 : r - 32 + STEP, :]) * c[:, 128:384]
        res[r - 32 : r - 32 + STEP, :] = out
    for cp in sent:
        cp.wait_send()


def tmp0_pair(ref, t, rows):
    return jnp.concatenate(
        [
            ref[2 * t + h, pl.ds(0, rows // 2, 2), :] + ref[2 * t + h, pl.ds(1, rows // 2, 2), :]
            for h in range(2)
        ],
        axis=1,
    )


def body(right_side, shift):
    v = pltpu.VMEM
    dma = pltpu.SemaphoreType.DMA
    big = v((208, 512), F32)
    scratch = (
        [big] * 7
        + [v((4, 192, 128), F32)]
        + [v((4, 2, 128, 128), F32), v((4, 2, 128, 128), F32), v((4, 1, 112, 128), F32)]
        + [v((256, 128), BF16)]
        + [v((128, 128), BF16)] * 4
        + [v((128, 256), BF16), v((256, 128), BF16)]
        + [v((4, 16, 128), F32), v((112, 128), F32)] * 2
        + [v((16, 128), F32)] * 2
        + [v((2, 16, 128), F32)]
        + [v((4, 8, 32, 128), F32), v((4, 32, 128), F32)]
        + [v((3, 8, 24, 128), F32), v((3, 32, 128), F32)]
        + [v((3, 2, 1, 128), F32), v((3, 15, 1, 128), F32), v((3, 15, 1, 128), F32)]
        + [dma((2, 8))] * 2
        + [dma((10,))] * 4
        + [dma((4, 8))] * 2
        + [dma((3, 8))] * 2
        + [dma((3, 2, 15))] * 2
        + [dma((2,))]
    )
    shape = jax.ShapeDtypeStruct((128, 256), F32)
    vm = pl.BlockSpec(memory_space=pltpu.VMEM)
    return pl.pallas_call(
        kernel,
        out_shape=(shape, shape),
        in_specs=[pl.BlockSpec(memory_space=pl.ANY)] * 2,
        out_specs=(vm, vm),
        scratch_shapes=scratch,
        compiler_params=pltpu.CompilerParams(
            collective_id=0, has_side_effects=True, vmem_limit_bytes=40 * 1024 * 1024
        ),
        name="fcycle",
    )(right_side, shift)


def solution(mesh):
    spec = P("gx", "gy")
    return jax.shard_map(
        body, mesh=mesh, in_specs=(spec, spec), out_specs=(spec, spec), check_vma=False
    )
```

```python
import jax
import jax.numpy as jnp
from jax import lax
from jax.experimental import pallas as pl
from jax.experimental.pallas import tpu as pltpu
from jax.sharding import PartitionSpec as P

MESH = pl.DeviceIdType.MESH
F32 = jnp.float32
BF16 = jnp.bfloat16
GX, GY = 8, 32
NX, NY = 1024, 8192
LV_Q = [4.0 ** (-l) for l in range(5)]
LV_D = [4.0 ** (1 - l) for l in range(5)]

AROUND = [(-1, 0), (1, 0), (0, -1), (0, 1), (-1, -1), (-1, 1), (1, -1), (1, 1)]
SIDE = [-1, 1, -2, 2]
LINE = [-1, 1, -2, 2, -3, 3]
GROUP_A = [(dz, dc) for dz in range(8) for dc in range(2) if dz or dc]
GROUP_B = [(dy, dx) for dy in range(4) for dx in range(4) if dy or dx]


def iota(shape, dim):
    return lax.broadcasted_iota(jnp.int32, shape, dim)


def beside(v):
    r, c = v.shape
    return (
        pltpu.roll(v, 1, axis=0)
        + pltpu.roll(v, r - 1, axis=0)
        + pltpu.roll(v, 1, axis=1)
        + pltpu.roll(v, c - 1, axis=1)
    )


def inside(shape, level, row0, col0):
    rows = iota(shape, 0) + row0
    cols = iota(shape, 1) + col0
    return (
        (rows >= 0) & (rows < (NX >> level)) & (cols >= 0) & (cols < (NY >> level))
    )


class Level:
    def __init__(self, level, shift, row0, col0, mask=None):
        self.level = level
        self.d = LV_D[level] + shift
        ok = inside(shift.shape, level, row0, col0)
        if mask is not None:
            ok = ok & mask
        self.ok = ok
        self.k = jnp.where(ok, 0.8 / self.d, 0.0)
        self.km = self.k * LV_Q[level]

    def cut(self, lo, hi):
        out = object.__new__(Level)
        out.level = self.level
        out.d, out.k, out.km, out.ok = (
            self.d[lo:hi],
            self.k[lo:hi],
            self.km[lo:hi],
            None,
        )
        return out

    def sweep0(self, v):
        return 0.2 * v + self.km * beside(v)

    def sweep(self, v, kg):
        return 0.2 * v + kg + self.km * beside(v)

    def residual(self, v, g):
        return g - self.d * v + LV_Q[self.level] * beside(v)

    def apply(self, v):
        return self.d * v - LV_Q[self.level] * beside(v)


def mm(x, w):
    m = x.shape[0]
    a = x.astype(BF16)
    r = x - a.astype(F32)
    b = r.astype(BF16)
    c = (r - b.astype(F32)).astype(BF16)
    y = jnp.dot(jnp.concatenate([a, b, c], axis=0), w, preferred_element_type=F32)
    return (y[2 * m :] + y[m : 2 * m]) + y[:m]


def total(x):
    return jnp.sum(jnp.sum(x, axis=0, keepdims=True), axis=1, keepdims=True)


def pick(row, at):
    lane = iota(row.shape, 1)
    return jnp.sum(jnp.where(lane == at, row, 0.0), axis=1, keepdims=True)


def kernel(
    rhs_in, shf_in, sol, res,
    xg, xs, kk, kg0, v0, wa, wb, tmp0,
    t1s, t2s, t3s,
    rm, r23, r34, p43, p32, p21, r03,
    s_side, s_line, g_side, g_line, own3, own3g, ownb,
    x2b, own2, x3b, own3n, own3p,
    ar_in, ar_a, ar_b,
    e0_ss, e0_rs, s_ss, s_rs, g_ss, g_rs, x2_ss, x2_rs, x3_ss, x3_rs, ar_ss, ar_rs, in_s,
):
    gx = lax.axis_index("gx")
    gy = lax.axis_index("gy")
    core = lax.rem(gy, 2)
    quad = lax.div(gy, 2)
    qy, qx = lax.div(quad, 4), lax.rem(quad, 4)

    def near(dz, dy):
        return (lax.rem(gx + (dz + GX), GX), lax.rem(gy + (dy + GY), GY))

    def in_a(dz, dc):
        return (lax.rem(gx + dz, GX), gy - core + lax.rem(core + dc, 2))

    def in_b(dy, dx):
        return (gx, (lax.rem(qy + dy, 4) * 4 + lax.rem(qx + dx, 4)) * 2 + core)

    barrier = pltpu.get_barrier_semaphore()
    partners = (
        [near(*o) for o in AROUND]
        + [in_a(*o) for o in GROUP_A]
        + [in_b(*o) for o in GROUP_B]
    )
    for p in partners:
        pl.semaphore_signal(barrier, inc=1, device_id=p, device_id_type=MESH)

    mid = (slice(40, 168), slice(128, 384))
    rhs, shf = xg.at[mid], xs.at[mid]
    in_shf = pltpu.make_async_copy(shf_in, shf, in_s.at[0])
    in_rhs = pltpu.make_async_copy(rhs_in, rhs, in_s.at[1])
    in_shf.start()
    in_rhs.start()

    sent = []
    turn = [0]

    def scratch(pool):
        turn[0] += 1
        return pool.at[turn[0] % pool.shape[0]]

    def send(src, dst, ss, rs, dev):
        cp = pltpu.make_async_remote_copy(
            src_ref=src, dst_ref=dst, send_sem=ss, recv_sem=rs,
            device_id=dev, device_id_type=MESH,
        )
        cp.start()
        sent.append(cp)
        return cp

    i, j = iota((256, 128), 0), iota((256, 128), 1)
    rm[...] = jnp.where((i >> 1) == j, 0.25, 0.0).astype(BF16)
    r03[...] = jnp.where((i >> 3) + 48 == j, 1.0 / 64, 0.0).astype(BF16)
    i, j = iota((128, 128), 0), iota((128, 128), 1)
    r34[...] = jnp.where((i >> 1) == j, 0.25, 0.0).astype(BF16)
    r23[...] = jnp.where((i >> 1) + 32 == j, 0.25, 0.0).astype(BF16)
    p43[...] = jnp.where(i == (j >> 1), 1.0, 0.0).astype(BF16)
    p32[...] = jnp.where(i == (j >> 1) + 32, 1.0, 0.0).astype(BF16)
    i, j = iota((128, 256), 0), iota((128, 256), 1)
    p21[...] = jnp.where(i == (j >> 1), 1.0, 0.0).astype(BF16)

    def pair_rows(ref, rows, lanes):
        return jnp.concatenate(
            [
                ref[t, pl.ds(0, rows // 2, 2), :] + ref[t, pl.ds(1, rows // 2, 2), :]
                for t in range(lanes // 128)
            ],
            axis=1,
        )

    def put(ref, x):
        for t in range(x.shape[1] // 128):
            ref[t, 0 : x.shape[0], :] = x[:, 128 * t : 128 * t + 128]

    def restrict(x, pool, w):
        ref = scratch(pool)
        put(ref, x)
        return mm(pair_rows(ref, x.shape[0], x.shape[1]), w[...])

    def prolong(e, pool, w):
        ref = scratch(pool)
        y = mm(e, w[...])
        m = y.shape[0]
        out = []
        for t in range(y.shape[1] // 128):
            yt = y[:, 128 * t : 128 * t + 128]
            ref[t, pl.ds(0, m, 2), :] = yt
            ref[t, pl.ds(1, m, 2), :] = yt
            out.append(ref[t, 0 : 2 * m, :])
        return jnp.concatenate(out, axis=1) if len(out) > 1 else out[0]

    zero8 = jnp.zeros((8, 512), F32)
    for ref in (kg0, v0, wa, wb):
        ref[0:8, :] = zero8
        ref[200:208, :] = zero8
    for ref in (xs, xg):
        ref[8:16, :] = zero8
        ref[192:200, :] = zero8

    in_shf.wait()
    s0 = shf[...]
    put(tmp0, s0)
    acc = pair_rows(tmp0, 128, 256)
    s1own = mm(acc, rm[...])
    ref1, ref2 = scratch(t1s), scratch(t2s)
    put(ref1, acc)
    acc = pair_rows(ref1, 64, 256)
    put(ref2, acc)
    own3[...] = mm(pair_rows(ref2, 32, 256), r03[...])
    own2[0] = pltpu.roll(restrict(s1own, t1s, r34), 32, axis=1)
    in_rhs.wait()

    pl.semaphore_wait(barrier, len(partners))

    ROWS = {-1: (0, 24, 160, 184), 1: (104, 128, 8, 32), 0: (0, 128, 32, 160)}
    COLS = {-1: (0, 128, 384, 512), 1: (128, 256, 0, 128), 0: (0, 256, 128, 384)}
    first = []

    def border(f):
        src, dst = (shf, xs) if f else (rhs, xg)
        for n, (dz, dy) in enumerate(AROUND):
            a, b, c, d = ROWS[dz]
            e, g, h, k = COLS[dy]
            first.append(
                send(
                    src.at[a:b, e:g], dst.at[8 + c : 8 + d, h:k],
                    e0_ss.at[f, n], e0_rs.at[f, n], near(dz, dy),
                )
            )

    def side_send(src, buf, ss, rs):
        return [
            send(src, buf.at[n], ss.at[n], rs.at[n], near(0, d))
            for n, d in enumerate(SIDE)
        ]

    def side_join(own, buf, cps):
        for cp in cps:
            cp.wait_recv()
        right1, left1, right2, left2 = (buf[n] for n in range(4))
        lane = iota((16, 128), 1)
        out = jnp.where(lane < 48, pltpu.roll(left1, 96, axis=1), own)
        out = jnp.where(lane < 16, pltpu.roll(left2, 64, axis=1), out)
        out = jnp.where(lane >= 80, pltpu.roll(right1, 32, axis=1), out)
        return jnp.where(lane >= 112, pltpu.roll(right2, 64, axis=1), out)

    def line_send(src, buf, ss, rs):
        return [
            send(
                src, buf.at[16 * (3 - d) : 16 * (4 - d)],
                ss.at[4 + n], rs.at[4 + n], near(d, 0),
            )
            for n, d in enumerate(LINE)
        ]

    SRC2 = {-1: (0, 16), 1: (16, 32), 0: (0, 32)}

    def send2(x, k):
        own2[k] = x
        src, buf = own2.at[k], x2b.at[k]
        cps = []
        for n, (dz, dy) in enumerate(AROUND):
            a, b = SRC2[dz]
            cps.append(
                send(
                    src.at[a:b], buf.at[n, 0 : b - a],
                    x2_ss.at[k, n], x2_rs.at[k, n], near(dz, dy),
                )
            )
        return cps

    def lanes3(left, mid, right, lo, hi, move):
        lane = iota(mid.shape, 1)
        out = jnp.where(lane < lo, pltpu.roll(left, 128 - move, axis=1), mid)
        return jnp.where(lane >= hi, pltpu.roll(right, move, axis=1), out)

    def join2(k, cps):
        for cp in cps:
            cp.wait_recv()
        own, buf = own2[k], x2b.at[k]
        dn, up, rt, lf, dr, dl, ur, ul = range(8)
        return jnp.concatenate(
            [
                lanes3(buf[ul, 0:16], buf[up, 0:16], buf[ur, 0:16], 32, 96, 64),
                lanes3(buf[lf], own, buf[rt], 32, 96, 64),
                lanes3(buf[dl, 0:16], buf[dn, 0:16], buf[dr, 0:16], 32, 96, 64),
            ],
            axis=0,
        )

    def pack3(x, lo):
        lane = iota((8, 128), 1)
        a, b, c = (x[lo + 8 * n : lo + 8 * n + 8] for n in range(3))
        out = jnp.where(lane < 64, pltpu.roll(b, 112, axis=1), pltpu.roll(c, 16, axis=1))
        return jnp.where(lane < 32, pltpu.roll(a, 80, axis=1), out)

    def send3(x, k):
        own3n[k] = x
        own3p[k, 0] = pack3(x, 8)
        own3p[k, 1] = pack3(x, 0)
        return [
            send(
                own3p.at[k, 1 if dz == 1 else 0], x3b.at[k, n],
                x3_ss.at[k, n], x3_rs.at[k, n], near(dz, dy),
            )
            for n, (dz, dy) in enumerate(AROUND)
        ]

    def take3(k, cps):
        for cp in cps:
            cp.wait_recv()
        return [own3n[k, 8:24]] + [x3b[k, n] for n in range(8)]

    def join3(own, dn, up, rt, lf, dr, dl, ur, ul):
        lane = iota((8, 128), 1)

        def at(x, n, dest):
            move = (dest - 32 * n) % 128
            return pltpu.roll(x, move, axis=1) if move else x

        rows = []
        for left, centre, right, count in ((ul, up, ur, 3), (lf, None, rt, 2), (dl, dn, dr, 3)):
            for n in range(count):
                c = own[8 * n : 8 * n + 8] if centre is None else at(centre, n, 48)
                out = jnp.where(lane < 80, c, at(right, n, 80))
                rows.append(jnp.where(lane < 48, at(left, n, 16), out))
        return jnp.concatenate(rows, axis=0)

    def sum_start(row, k):
        ar_in[k, 0] = row
        return [
            send(
                ar_in.at[k, 0], ar_a.at[k, n],
                ar_ss.at[k, 0, n], ar_rs.at[k, 0, n], in_a(*o),
            )
            for n, o in enumerate(GROUP_A)
        ]

    def sum_next(cps, k):
        for cp in cps:
            cp.wait_recv()
        part = ar_in[k, 0] + jnp.sum(ar_a[k], axis=0)
        ar_in[k, 1] = part
        return [
            send(
                ar_in.at[k, 1], ar_b.at[k, n],
                ar_ss.at[k, 1, n], ar_rs.at[k, 1, n], in_b(*o),
            )
            for n, o in enumerate(GROUP_B)
        ]

    def sum_end(cps, k):
        for cp in cps:
            cp.wait_recv()
        return ar_in[k, 1] + jnp.sum(ar_b[k], axis=0)

    side_s = side_send(own3, s_side, s_ss, s_rs)
    border(1)
    border(0)
    cps2s = send2(own2[0], 0)
    s_row = side_join(own3[...], s_side, side_s)
    ownb[0] = s_row
    line_s = line_send(ownb.at[0], s_line, s_ss, s_rs)
    s_line[48:64] = s_row

    row0 = gx * 128 - 32
    col0 = gy * 256 - 128
    for cp in first[:8]:
        cp.wait_recv()
    STEP = 16

    def near4(ref, r, n=STEP):
        c = ref[8 + r : 8 + r + n, :]
        around = (
            ref[7 + r : 7 + r + n, :]
            + ref[9 + r : 9 + r + n, :]
            + pltpu.roll(c, 1, axis=1)
            + pltpu.roll(c, 511, axis=1)
        )
        return c, around

    for r in range(0, 192, STEP):
        w = slice(8 + r, 8 + r + STEP)
        ok = inside((STEP, 512), 0, row0 + r, col0)
        kk[w, :] = jnp.where(ok, 0.8 / (4.0 + xs[w, :]), 0.0)
    put(tmp0, xs[8:200, :])
    s1 = jnp.concatenate(
        [
            mm(tmp0_pair(tmp0, t, 192), rm[...])
            for t in range(2)
        ],
        axis=1,
    )
    l1 = Level(1, s1, gx * 64 - 16, gy * 128 - 64)
    s2 = restrict(s1, t1s, rm)
    l2a = Level(2, s2, gx * 32 - 8, gy * 64 - 32)

    for cp in first[8:]:
        cp.wait_recv()
    for r in range(0, 192, STEP):
        w = slice(8 + r, 8 + r + STEP)
        kg0[w, :] = kk[w, :] * xg[w, :]
    for r in range(0, 192, STEP):
        w = slice(8 + r, 8 + r + STEP)
        c, around = near4(kg0, r)
        v0[w, :] = 1.2 * c + kk[w, :] * around
    for r in range(0, 192, STEP):
        w = slice(8 + r, 8 + r + STEP)
        c, around = near4(v0, r)
        out = xg[w, :] - (4.0 + xs[w, :]) * c + around
        for t in range(4):
            tmp0[t, r : r + STEP, :] = out[:, 128 * t : 128 * t + 128]
    g1 = jnp.concatenate([mm(tmp0_pair(tmp0, t, 192), rm[...]) for t in range(2)], axis=1)

    kg1 = l1.k * g1
    v1 = l1.sweep(kg1, kg1)
    g2 = restrict(l1.residual(v1, g1), t1s, rm)
    kg = l2a.k * g2
    r2 = l2a.residual(l2a.sweep(kg, kg), g2)
    g3 = restrict(r2, t2s, r23)
    g3own = g3[4:20]
    own3g[...] = g3own
    side_g = side_send(own3g, g_side, g_ss, g_rs)
    cps2g = send2(g2[8:40], 1)

    for cp in line_s:
        cp.wait_recv()
    l3 = Level(3, s_line[...], gx * 16 - 48, gy * 32 - 48)
    s4 = restrict(s_line[...], t3s, r34)
    l4 = Level(4, s4, gx * 8 - 24, gy * 16 - 24, iota((56, 128), 1) < 64)

    one4 = jnp.where(l4.ok, 1.0, 0.0)
    one3 = jnp.where(l3.ok, 1.0, 0.0)
    w6 = one4
    for _ in range(6):
        w6 = l4.sweep0(w6)
    w12 = w6
    for _ in range(6):
        w12 = l4.sweep0(w12)
    y3 = l3.sweep0(l3.sweep0(one3))
    u = l3.sweep0(l3.sweep0(y3))
    q = 4.0 * restrict(jnp.where(l3.ok, l3.apply(u), 0.0), t3s, r34)
    kq = l4.k * q
    z = kq
    for _ in range(11):
        z = l4.sweep(z, kq)
    f3 = l3.sweep0(l3.sweep0(u - 0.25 * prolong(z, t3s, p43)))
    f2 = l3.sweep0(l3.sweep0(prolong(w6, t3s, p43)))
    lane3 = (iota((16, 128), 1) >= 48) & (iota((16, 128), 1) < 80)
    lane4 = (iota((8, 128), 1) >= 24) & (iota((8, 128), 1) < 40)
    g3m = jnp.where(lane3, g3own, 0.0)

    def own4(x):
        return jnp.where(lane4, x[24:32], 0.0)

    parts = [
        0.25 * total(y3[48:64] * g3m),
        0.25 * total(f2[48:64] * g3m),
        total(f3[48:64] * g3m),
        total(own4(l4.apply(one4))),
        total(own4(l4.apply(w6))),
        total(own4(q * w12)),
        total(own4(q * w6)),
    ]
    lane = iota((1, 128), 1)
    row = jnp.zeros((1, 128), F32)
    for n, p in enumerate(parts):
        row = jnp.where(lane == n, p, row)
    sums1 = sum_start(row, 0)

    g_row = side_join(g3own, g_side, side_g)
    ownb[1] = g_row
    line_g = line_send(ownb.at[1], g_line, g_ss, g_rs)
    g_line[48:64] = g_row

    def coarse(G):
        kgc = l3b.k * G
        v = l3b.sweep(kgc, kgc)
        kgd = l4b.k * restrict(l3b.residual(v, G), t3s, r34)
        e = kgd
        for _ in range(5):
            e = l4b.sweep(e, kgd)
        x = v + prolong(e, t3s, p43)
        for _ in range(2):
            x = l3b.sweep(x, kgc)
        return x[16:48]

    def down2(x):
        pad = jnp.zeros((8, 128), F32)
        g = jnp.concatenate([pad, x, pad], axis=0)
        kg = l2.k * g
        v = l2.sweep(kg, kg)
        r = l2.residual(v, g)
        return g, v, r, restrict(r, t2s, r23)

    def up2(e3, g):
        kg = l2.k * g
        x = l2.sweep(kg, kg) + prolong(e3, t2s, p32)
        for _ in range(2):
            x = l2.sweep(x, kg)
        return x

    l3b = l3.cut(24, 88)
    l4b = l4.cut(12, 44)
    lane1 = (iota((64, 256), 1) >= 64) & (iota((64, 256), 1) < 192)
    lane2 = (iota((32, 128), 1) >= 32) & (iota((32, 128), 1) < 96)

    def dot1(a, b):
        return total(jnp.where(lane1, a[16:80] * b[16:80], 0.0))

    def dot2(a, b):
        return total(jnp.where(lane2, a[16:48] * b[16:48], 0.0))

    def dot3(a, b):
        return total(jnp.where(lane3, a * b, 0.0))

    ra, rb = prolong(w12, t3s, p43), prolong(w6, t3s, p43)
    for _ in range(4):
        ra, rb = l3.sweep0(ra), l3.sweep0(rb)
    ka = l4.k * restrict(-l3.apply(ra), t3s, r34)
    kb = l4.k * restrict(-l3.apply(rb), t3s, r34)
    ea, eb = ka, kb
    for _ in range(5):
        ea, eb = l4.sweep(ea, ka), l4.sweep(eb, kb)
    ra, rb = ra + prolong(ea, t3s, p43), rb + prolong(eb, t3s, p43)
    for _ in range(2):
        ra, rb = l3.sweep0(ra), l3.sweep0(rb)

    s2w = join2(0, cps2s)
    l2 = Level(2, s2w, gx * 32 - 16, gy * 64 - 32)
    start2 = [prolong(r[40:72], t2s, p32) for r in (ra, rb, f2)]
    after2 = start2
    for _ in range(4):
        after2 = [l2.sweep0(x) for x in after2]
    h_of = [restrict(-l2.apply(x), t2s, r23) for x in after2]
    cps_of = [send3(h, 3 + n) for n, h in enumerate(h_of)]
    y2 = l2.sweep0(l2.sweep0(prolong(y3[40:72], t2s, p32)))
    f5 = l1.sweep0(l1.sweep0(prolong(y2[8:56], t1s, p21)))
    f5 = l1.sweep0(l1.sweep0(f5)) * (1.0 / 64)
    ga, va, ta, ha = down2(4.0 * restrict(l1.apply(f5), t1s, rm))
    ha = 4.0 * ha
    cpsa = send3(ha, 6)
    f4 = l2.sweep0(l2.sweep0(y2)) * (1.0 / 16)
    p4_of = [-dot2(f4, l2.apply(x)) for x in start2]
    p54 = -dot3(ha[8:24], f2[48:64])

    sums1 = sum_next(sums1, 0)

    g2w = join2(1, cps2g)
    kg2 = l2.k * g2w
    v2 = l2.sweep(kg2, kg2)
    pv = dot1(f5, l1.residual(v1, g1)) - dot2(va, g2w)
    for cp in line_g:
        cp.wait_recv()
    G3 = g_line[...]
    kg3 = l3.k * G3
    v3 = l3.sweep(kg3, kg3)
    kg4 = l4.k * restrict(l3.residual(v3, G3), t3s, r34)
    e4 = kg4
    for _ in range(11):
        e4 = l4.sweep(e4, kg4)
    x3 = v3 + prolong(e4, t3s, p43)
    for _ in range(4):
        x3 = l3.sweep(x3, kg3)
    kg4 = l4.k * restrict(l3.residual(x3, G3), t3s, r34)
    e4 = kg4
    for _ in range(5):
        e4 = l4.sweep(e4, kg4)
    x3 = x3 + prolong(e4, t3s, p43)
    for _ in range(2):
        x3 = l3.sweep(x3, kg3)

    x2 = v2 + prolong(x3[40:72], t2s, p32)
    p4 = dot2(f4, l2.residual(x2, g2w))
    for _ in range(4):
        x2 = l2.sweep(x2, kg2)
    g3 = restrict(l2.residual(x2, g2w), t2s, r23)
    cps3 = send3(g3, 0)
    ma = coarse(join3(*take3(6, cpsa)))[8:24]
    p5 = pv - dot2(ta, x2) - dot3(ma, g3[8:24])
    p5_of = [
        -dot2(ta, x) - dot3(ma, h[8:24]) for x, h in zip(after2, h_of)
    ]
    row = jnp.zeros((1, 128), F32)
    for n, p in enumerate([p4, *p4_of, p5, *p5_of, p54]):
        row = jnp.where(lane == n, p, row)
    sums2 = sum_start(row, 1)

    z2 = l2.sweep0(l2.sweep0(prolong(f2[40:72], t2s, p32)))
    z1 = prolong(z2[8:56], t1s, p21)
    w1 = l1.sweep0(l1.sweep0(z1))
    d1 = l1.sweep0(l1.sweep0(w1))
    h2, _, _, h3 = down2(restrict(-l1.apply(d1), t1s, rm))
    cps3r = send3(h3, 2)
    cps2r = send2(h2[16:48], 3)

    tot = sum_end(sums1, 0)
    a1, a2, a3, ones_total, w6_total, qw12, qw6 = (pick(tot, n) for n in range(7))
    inv = 1.0 / ones_total
    c1 = a1 * inv
    c2 = (a2 - c1 * w6_total) * inv
    c3 = 0.25 * (a3 - c1 * qw12 - c2 * qw6) * inv

    def with_constants(x, parts):
        return ((x + c1 * parts[0]) + c2 * parts[1]) + c3 * parts[2]

    x2 = with_constants(x2, after2)
    parts = [take3(3 + n, cps) for n, cps in enumerate(cps_of)]
    G = [with_constants(b, p) for b, p in zip(take3(0, cps3), zip(*parts))]
    x2 = x2 + prolong(coarse(join3(*G)), t2s, p32)
    for _ in range(2):
        x2 = l2.sweep(x2, kg2)

    x1 = v1 + prolong(x2[8:56], t1s, p21)
    for _ in range(4):
        x1 = l1.sweep(x1, kg1)
    g2, _, _, g3 = down2(restrict(l1.residual(x1, g1), t1s, rm))
    cps3 = send3(g3, 1)
    cps2h = send2(g2[16:48], 2)
    sums2 = sum_next(sums2, 1)
    e3 = coarse(join3(*take3(2, cps3r)))
    x2r = up2(e3, join2(3, cps2r))
    x1r = l1.sweep0(l1.sweep0(d1 + prolong(x2r[8:56], t1s, p21)))

    e3 = coarse(join3(*take3(1, cps3)))
    x2 = up2(e3, join2(2, cps2h))
    x1 = x1 + prolong(x2[8:56], t1s, p21)
    for _ in range(2):
        x1 = l1.sweep(x1, kg1)
    tot = sum_end(sums2, 1)
    b4, b41, b42, b43, b5, b51, b52, b53, b54 = (pick(tot, n) for n in range(9))
    c4 = with_constants(b4, (b41, b42, b43)) * inv
    c5 = (with_constants(b5, (b51, b52, b53)) + c4 * b54) * inv
    x1 = (x1 + c4 * x1r) + c5 * w1

    for t in range(2):
        y = mm(x1[:, 128 * t : 128 * t + 128], p21[...])
        for h in range(2):
            tmp0[2 * t + h, pl.ds(0, 96, 2), :] = y[:, 128 * h : 128 * h + 128]
            tmp0[2 * t + h, pl.ds(1, 96, 2), :] = y[:, 128 * h : 128 * h + 128]
    for r in range(16, 176, STEP):
        w = slice(8 + r, 8 + r + STEP)
        e = jnp.concatenate([tmp0[t, r : r + STEP, :] for t in range(4)], axis=1)
        wa[w, :] = v0[w, :] + e
    for src, dst in ((wa, wb), (wb, wa)):
        for r in range(16, 176, STEP):
            w = slice(8 + r, 8 + r + STEP)
            c, around = near4(src, r)
            dst[w, :] = 0.2 * c + kg0[w, :] + kk[w, :] * around
    for r in range(32, 160, STEP):
        w = slice(8 + r, 8 + r + STEP)
        c, around = near4(wa, r)
        sol[r - 32 : r - 32 + STEP, :] = c[:, 128:384]
        out = rhs[r - 32 : r - 32 + STEP, :] + around[:, 128:384]
        out = out - (4.0 + shf[r - 32 : r - 32 + STEP, :]) * c[:, 128:384]
        res[r - 32 : r - 32 + STEP, :] = out
    for cp in sent:
        cp.wait_send()


def tmp0_pair(ref, t, rows):
    return jnp.concatenate(
        [
            ref[2 * t + h, pl.ds(0, rows // 2, 2), :] + ref[2 * t + h, pl.ds(1, rows // 2, 2), :]
            for h in range(2)
        ],
        axis=1,
    )


def body(right_side, shift):
    v = pltpu.VMEM
    dma = pltpu.SemaphoreType.DMA
    big = v((208, 512), F32)
    scratch = (
        [big] * 7
        + [v((4, 192, 128), F32)]
        + [v((4, 2, 128, 128), F32), v((4, 2, 128, 128), F32), v((4, 1, 112, 128), F32)]
        + [v((256, 128), BF16)]
        + [v((128, 128), BF16)] * 4
        + [v((128, 256), BF16), v((256, 128), BF16)]
        + [v((4, 16, 128), F32), v((112, 128), F32)] * 2
        + [v((16, 128), F32)] * 2
        + [v((2, 16, 128), F32)]
        + [v((4, 8, 32, 128), F32), v((4, 32, 128), F32)]
        + [v((7, 8, 8, 128), F32), v((7, 32, 128), F32), v((7, 2, 8, 128), F32)]
        + [v((2, 2, 1, 128), F32), v((2, 15, 1, 128), F32), v((2, 15, 1, 128), F32)]
        + [dma((2, 8))] * 2
        + [dma((10,))] * 4
        + [dma((4, 8))] * 2
        + [dma((7, 8))] * 2
        + [dma((2, 2, 15))] * 2
        + [dma((2,))]
    )
    shape = jax.ShapeDtypeStruct((128, 256), F32)
    vm = pl.BlockSpec(memory_space=pltpu.VMEM)
    return pl.pallas_call(
        kernel,
        out_shape=(shape, shape),
        in_specs=[pl.BlockSpec(memory_space=pl.ANY)] * 2,
        out_specs=(vm, vm),
        scratch_shapes=scratch,
        compiler_params=pltpu.CompilerParams(
            collective_id=0, has_side_effects=True, vmem_limit_bytes=40 * 1024 * 1024
        ),
        name="fcycle",
    )(right_side, shift)


def solution(mesh):
    spec = P("gx", "gy")
    return jax.shard_map(
        body, mesh=mesh, in_specs=(spec, spec), out_specs=(spec, spec), check_vma=False
    )
```

```python
import jax
import jax.numpy as jnp
from jax import lax
from jax.experimental import pallas as pl
from jax.experimental.pallas import tpu as pltpu
from jax.sharding import PartitionSpec as P

MESH = pl.DeviceIdType.MESH
F32 = jnp.float32
BF16 = jnp.bfloat16
GX, GY = 8, 32
NX, NY = 1024, 8192
LV_Q = [4.0 ** (-l) for l in range(5)]
LV_D = [4.0 ** (1 - l) for l in range(5)]

AROUND = [(-1, 0), (1, 0), (0, -1), (0, 1), (-1, -1), (-1, 1), (1, -1), (1, 1)]
SIDE = [-1, 1, -2, 2]
LINE = [-1, 1, -2, 2, -3, 3]
GROUP_A = [(dz, dc) for dz in range(8) for dc in range(2) if dz or dc]
GROUP_B = [(dy, dx) for dy in range(4) for dx in range(4) if dy or dx]


def iota(shape, dim):
    return lax.broadcasted_iota(jnp.int32, shape, dim)


def beside(v):
    r, c = v.shape
    return (
        pltpu.roll(v, 1, axis=0)
        + pltpu.roll(v, r - 1, axis=0)
        + pltpu.roll(v, 1, axis=1)
        + pltpu.roll(v, c - 1, axis=1)
    )


def inside(shape, level, row0, col0):
    rows = iota(shape, 0) + row0
    cols = iota(shape, 1) + col0
    return (
        (rows >= 0) & (rows < (NX >> level)) & (cols >= 0) & (cols < (NY >> level))
    )


class Level:
    def __init__(self, level, shift, row0, col0, mask=None):
        self.level = level
        self.d = LV_D[level] + shift
        ok = inside(shift.shape, level, row0, col0)
        if mask is not None:
            ok = ok & mask
        self.ok = ok
        self.k = jnp.where(ok, 0.8 / self.d, 0.0)
        self.km = self.k * LV_Q[level]

    def cut(self, lo, hi):
        out = object.__new__(Level)
        out.level = self.level
        out.d, out.k, out.km, out.ok = (
            self.d[lo:hi],
            self.k[lo:hi],
            self.km[lo:hi],
            None,
        )
        return out

    def sweep0(self, v):
        return 0.2 * v + self.km * beside(v)

    def sweep(self, v, kg):
        return 0.2 * v + kg + self.km * beside(v)

    def residual(self, v, g):
        return g - self.d * v + LV_Q[self.level] * beside(v)

    def apply(self, v):
        return self.d * v - LV_Q[self.level] * beside(v)


def mm(x, w):
    m = x.shape[0]
    a = x.astype(BF16)
    r = x - a.astype(F32)
    b = r.astype(BF16)
    c = (r - b.astype(F32)).astype(BF16)
    y = jnp.dot(jnp.concatenate([a, b, c], axis=0), w, preferred_element_type=F32)
    return (y[2 * m :] + y[m : 2 * m]) + y[:m]


def total(x):
    return jnp.sum(jnp.sum(x, axis=0, keepdims=True), axis=1, keepdims=True)


def pick(row, at):
    lane = iota(row.shape, 1)
    return jnp.sum(jnp.where(lane == at, row, 0.0), axis=1, keepdims=True)


def kernel(
    rhs_in, shf_in, sol, res,
    xg, xs, kk, kg0, v0, wa, wb, tmp0,
    t1s, t2s, t3s,
    rm, r23, r34, p43, p32, p21, r03,
    s_side, s_line, g_side, g_line, own3, own3g, ownb,
    x2b, own2, x3b, own3n, own3p,
    ar_in, ar_a, ar_b,
    rows_of, all_sent, got_border, got_s, got_g, got_2, got_3, got_sum, in_s,
):
    gx = lax.axis_index("gx")
    gy = lax.axis_index("gy")
    core = lax.rem(gy, 2)
    quad = lax.div(gy, 2)
    qy, qx = lax.div(quad, 4), lax.rem(quad, 4)

    def near(dz, dy):
        return (lax.rem(gx + (dz + GX), GX), lax.rem(gy + (dy + GY), GY))

    def in_a(dz, dc):
        return (lax.rem(gx + dz, GX), gy - core + lax.rem(core + dc, 2))

    def in_b(dy, dx):
        return (gx, (lax.rem(qy + dy, 4) * 4 + lax.rem(qx + dx, 4)) * 2 + core)

    barrier = pltpu.get_barrier_semaphore()
    partners = (
        [near(*o) for o in AROUND]
        + [in_a(*o) for o in GROUP_A]
        + [in_b(*o) for o in GROUP_B]
    )
    for p in partners:
        pl.semaphore_signal(barrier, inc=1, device_id=p, device_id_type=MESH)

    mid = (slice(40, 168), slice(128, 384))
    rhs, shf = xg.at[mid], xs.at[mid]
    in_shf = pltpu.make_async_copy(shf_in, shf, in_s.at[0])
    in_rhs = pltpu.make_async_copy(rhs_in, rhs, in_s.at[1])
    in_shf.start()
    in_rhs.start()

    sent = [0]
    turn = [0]

    def got(sem, rows):
        ref = rows_of.at[0:rows]
        pltpu.make_async_copy(ref, ref, sem).wait()

    def scratch(pool):
        turn[0] += 1
        return pool.at[turn[0] % pool.shape[0]]

    def send(src, dst, sem, dev):
        pltpu.make_async_remote_copy(
            src_ref=src, dst_ref=dst, send_sem=all_sent.at[0], recv_sem=sem,
            device_id=dev, device_id_type=MESH,
        ).start()
        size = src.shape[0] * src.shape[1] // 128
        sent[0] += size
        return size

    i, j = iota((256, 128), 0), iota((256, 128), 1)
    rm[...] = jnp.where((i >> 1) == j, 0.25, 0.0).astype(BF16)
    r03[...] = jnp.where((i >> 3) + 48 == j, 1.0 / 64, 0.0).astype(BF16)
    i, j = iota((128, 128), 0), iota((128, 128), 1)
    r34[...] = jnp.where((i >> 1) == j, 0.25, 0.0).astype(BF16)
    r23[...] = jnp.where((i >> 1) + 32 == j, 0.25, 0.0).astype(BF16)
    p43[...] = jnp.where(i == (j >> 1), 1.0, 0.0).astype(BF16)
    p32[...] = jnp.where(i == (j >> 1) + 32, 1.0, 0.0).astype(BF16)
    i, j = iota((128, 256), 0), iota((128, 256), 1)
    p21[...] = jnp.where(i == (j >> 1), 1.0, 0.0).astype(BF16)

    def pair_rows(ref, rows, lanes):
        return jnp.concatenate(
            [
                ref[t, pl.ds(0, rows // 2, 2), :] + ref[t, pl.ds(1, rows // 2, 2), :]
                for t in range(lanes // 128)
            ],
            axis=1,
        )

    def put(ref, x):
        for t in range(x.shape[1] // 128):
            ref[t, 0 : x.shape[0], :] = x[:, 128 * t : 128 * t + 128]

    def restrict(x, pool, w):
        ref = scratch(pool)
        put(ref, x)
        return mm(pair_rows(ref, x.shape[0], x.shape[1]), w[...])

    def prolong(e, pool, w):
        ref = scratch(pool)
        y = mm(e, w[...])
        m = y.shape[0]
        out = []
        for t in range(y.shape[1] // 128):
            yt = y[:, 128 * t : 128 * t + 128]
            ref[t, pl.ds(0, m, 2), :] = yt
            ref[t, pl.ds(1, m, 2), :] = yt
            out.append(ref[t, 0 : 2 * m, :])
        return jnp.concatenate(out, axis=1) if len(out) > 1 else out[0]

    zero8 = jnp.zeros((8, 512), F32)
    for ref in (kg0, v0, wa, wb):
        ref[0:8, :] = zero8
        ref[200:208, :] = zero8
    for ref in (xs, xg):
        ref[8:16, :] = zero8
        ref[192:200, :] = zero8

    in_shf.wait()
    s0 = shf[...]
    put(tmp0, s0)
    acc = pair_rows(tmp0, 128, 256)
    s1own = mm(acc, rm[...])
    ref1, ref2 = scratch(t1s), scratch(t2s)
    put(ref1, acc)
    acc = pair_rows(ref1, 64, 256)
    put(ref2, acc)
    own3[...] = mm(pair_rows(ref2, 32, 256), r03[...])
    own2[0] = pltpu.roll(restrict(s1own, t1s, r34), 32, axis=1)
    in_rhs.wait()

    pl.semaphore_wait(barrier, len(partners))

    ROWS = {-1: (0, 24, 160, 184), 1: (104, 128, 8, 32), 0: (0, 128, 32, 160)}
    COLS = {-1: (0, 128, 384, 512), 1: (128, 256, 0, 128), 0: (0, 256, 128, 384)}

    def border(f):
        src, dst = (shf, xs) if f else (rhs, xg)
        rows = 0
        for dz, dy in AROUND:
            a, b, c, d = ROWS[dz]
            e, g, h, k = COLS[dy]
            rows += send(
                src.at[a:b, e:g], dst.at[8 + c : 8 + d, h:k], got_border.at[f], near(dz, dy)
            )
        return rows

    def side_send(src, buf, sem):
        for n, d in enumerate(SIDE):
            send(src, buf.at[n], sem.at[0], near(0, d))

    def side_join(own, buf, sem):
        got(sem.at[0], 64)
        right1, left1, right2, left2 = (buf[n] for n in range(4))
        lane = iota((16, 128), 1)
        out = jnp.where(lane < 48, pltpu.roll(left1, 96, axis=1), own)
        out = jnp.where(lane < 16, pltpu.roll(left2, 64, axis=1), out)
        out = jnp.where(lane >= 80, pltpu.roll(right1, 32, axis=1), out)
        return jnp.where(lane >= 112, pltpu.roll(right2, 64, axis=1), out)

    def line_send(src, buf, sem):
        for d in LINE:
            send(src, buf.at[16 * (3 - d) : 16 * (4 - d)], sem.at[1], near(d, 0))

    SRC2 = {-1: (0, 16), 1: (16, 32), 0: (0, 32)}

    def send2(x, k):
        own2[k] = x
        for n, (dz, dy) in enumerate(AROUND):
            a, b = SRC2[dz]
            send(own2.at[k, a:b], x2b.at[k, n, 0 : b - a], got_2.at[k], near(dz, dy))

    def lanes3(left, mid, right, lo, hi, move):
        lane = iota(mid.shape, 1)
        out = jnp.where(lane < lo, pltpu.roll(left, 128 - move, axis=1), mid)
        return jnp.where(lane >= hi, pltpu.roll(right, move, axis=1), out)

    def join2(k):
        got(got_2.at[k], 6 * 16 + 2 * 32)
        own, buf = own2[k], x2b.at[k]
        dn, up, rt, lf, dr, dl, ur, ul = range(8)
        return jnp.concatenate(
            [
                lanes3(buf[ul, 0:16], buf[up, 0:16], buf[ur, 0:16], 32, 96, 64),
                lanes3(buf[lf], own, buf[rt], 32, 96, 64),
                lanes3(buf[dl, 0:16], buf[dn, 0:16], buf[dr, 0:16], 32, 96, 64),
            ],
            axis=0,
        )

    def pack3(x, lo):
        lane = iota((8, 128), 1)
        a, b, c = (x[lo + 8 * n : lo + 8 * n + 8] for n in range(3))
        out = jnp.where(lane < 64, pltpu.roll(b, 112, axis=1), pltpu.roll(c, 16, axis=1))
        return jnp.where(lane < 32, pltpu.roll(a, 80, axis=1), out)

    def send3(x, k):
        own3n[k] = x
        own3p[k, 0] = pack3(x, 8)
        own3p[k, 1] = pack3(x, 0)
        for n, (dz, dy) in enumerate(AROUND):
            send(own3p.at[k, 1 if dz == 1 else 0], x3b.at[k, n], got_3.at[k], near(dz, dy))

    def take3(k):
        got(got_3.at[k], 64)
        return [own3n[k, 8:24]] + [x3b[k, n] for n in range(8)]

    def join3(own, dn, up, rt, lf, dr, dl, ur, ul):
        lane = iota((8, 128), 1)

        def at(x, n, dest):
            move = (dest - 32 * n) % 128
            return pltpu.roll(x, move, axis=1) if move else x

        rows = []
        for left, centre, right, count in ((ul, up, ur, 3), (lf, None, rt, 2), (dl, dn, dr, 3)):
            for n in range(count):
                c = own[8 * n : 8 * n + 8] if centre is None else at(centre, n, 48)
                out = jnp.where(lane < 80, c, at(right, n, 80))
                rows.append(jnp.where(lane < 48, at(left, n, 16), out))
        return jnp.concatenate(rows, axis=0)

    def sum_start(row, k):
        ar_in[k, 0] = row
        for n, o in enumerate(GROUP_A):
            send(ar_in.at[k, 0], ar_a.at[k, n], got_sum.at[k, 0], in_a(*o))

    def sum_next(k):
        got(got_sum.at[k, 0], 15)
        ar_in[k, 1] = ar_in[k, 0] + jnp.sum(ar_a[k], axis=0)
        for n, o in enumerate(GROUP_B):
            send(ar_in.at[k, 1], ar_b.at[k, n], got_sum.at[k, 1], in_b(*o))

    def sum_end(k):
        got(got_sum.at[k, 1], 15)
        return ar_in[k, 1] + jnp.sum(ar_b[k], axis=0)

    side_send(own3, s_side, got_s)
    border_rows = border(1)
    border(0)
    send2(own2[0], 0)
    s_row = side_join(own3[...], s_side, got_s)
    ownb[0] = s_row
    line_send(ownb.at[0], s_line, got_s)
    s_line[48:64] = s_row

    row0 = gx * 128 - 32
    col0 = gy * 256 - 128
    got(got_border.at[1], border_rows)
    STEP = 16

    def near4(ref, r, n=STEP):
        c = ref[8 + r : 8 + r + n, :]
        around = (
            ref[7 + r : 7 + r + n, :]
            + ref[9 + r : 9 + r + n, :]
            + pltpu.roll(c, 1, axis=1)
            + pltpu.roll(c, 511, axis=1)
        )
        return c, around

    for r in range(0, 192, STEP):
        w = slice(8 + r, 8 + r + STEP)
        ok = inside((STEP, 512), 0, row0 + r, col0)
        kk[w, :] = jnp.where(ok, 0.8 / (4.0 + xs[w, :]), 0.0)
    put(tmp0, xs[8:200, :])
    s1 = jnp.concatenate(
        [
            mm(tmp0_pair(tmp0, t, 192), rm[...])
            for t in range(2)
        ],
        axis=1,
    )
    l1 = Level(1, s1, gx * 64 - 16, gy * 128 - 64)
    s2 = restrict(s1, t1s, rm)
    l2a = Level(2, s2, gx * 32 - 8, gy * 64 - 32)

    got(got_border.at[0], border_rows)
    for r in range(0, 192, STEP):
        w = slice(8 + r, 8 + r + STEP)
        kg0[w, :] = kk[w, :] * xg[w, :]
    for r in range(0, 192, STEP):
        w = slice(8 + r, 8 + r + STEP)
        c, around = near4(kg0, r)
        v0[w, :] = 1.2 * c + kk[w, :] * around
    for r in range(0, 192, STEP):
        w = slice(8 + r, 8 + r + STEP)
        c, around = near4(v0, r)
        out = xg[w, :] - (4.0 + xs[w, :]) * c + around
        for t in range(4):
            tmp0[t, r : r + STEP, :] = out[:, 128 * t : 128 * t + 128]
    g1 = jnp.concatenate([mm(tmp0_pair(tmp0, t, 192), rm[...]) for t in range(2)], axis=1)

    kg1 = l1.k * g1
    v1 = l1.sweep(kg1, kg1)
    g2 = restrict(l1.residual(v1, g1), t1s, rm)
    kg = l2a.k * g2
    r2 = l2a.residual(l2a.sweep(kg, kg), g2)
    g3 = restrict(r2, t2s, r23)
    g3own = g3[4:20]
    own3g[...] = g3own
    side_send(own3g, g_side, got_g)
    send2(g2[8:40], 1)

    got(got_s.at[1], 96)
    l3 = Level(3, s_line[...], gx * 16 - 48, gy * 32 - 48)
    s4 = restrict(s_line[...], t3s, r34)
    l4 = Level(4, s4, gx * 8 - 24, gy * 16 - 24, iota((56, 128), 1) < 64)

    one4 = jnp.where(l4.ok, 1.0, 0.0)
    one3 = jnp.where(l3.ok, 1.0, 0.0)
    w6 = one4
    for _ in range(6):
        w6 = l4.sweep0(w6)
    w12 = w6
    for _ in range(6):
        w12 = l4.sweep0(w12)
    y3 = l3.sweep0(l3.sweep0(one3))
    u = l3.sweep0(l3.sweep0(y3))
    q = 4.0 * restrict(jnp.where(l3.ok, l3.apply(u), 0.0), t3s, r34)
    kq = l4.k * q
    z = kq
    for _ in range(11):
        z = l4.sweep(z, kq)
    f3 = l3.sweep0(l3.sweep0(u - 0.25 * prolong(z, t3s, p43)))
    f2 = l3.sweep0(l3.sweep0(prolong(w6, t3s, p43)))
    lane3 = (iota((16, 128), 1) >= 48) & (iota((16, 128), 1) < 80)
    lane4 = (iota((8, 128), 1) >= 24) & (iota((8, 128), 1) < 40)
    g3m = jnp.where(lane3, g3own, 0.0)

    def own4(x):
        return jnp.where(lane4, x[24:32], 0.0)

    parts = [
        0.25 * total(y3[48:64] * g3m),
        0.25 * total(f2[48:64] * g3m),
        total(f3[48:64] * g3m),
        total(own4(l4.apply(one4))),
        total(own4(l4.apply(w6))),
        total(own4(q * w12)),
        total(own4(q * w6)),
    ]
    lane = iota((1, 128), 1)
    row = jnp.zeros((1, 128), F32)
    for n, p in enumerate(parts):
        row = jnp.where(lane == n, p, row)
    sum_start(row, 0)

    g_row = side_join(g3own, g_side, got_g)
    ownb[1] = g_row
    line_send(ownb.at[1], g_line, got_g)
    g_line[48:64] = g_row

    def coarse(G):
        kgc = l3b.k * G
        v = l3b.sweep(kgc, kgc)
        kgd = l4b.k * restrict(l3b.residual(v, G), t3s, r34)
        e = kgd
        for _ in range(5):
            e = l4b.sweep(e, kgd)
        x = v + prolong(e, t3s, p43)
        for _ in range(2):
            x = l3b.sweep(x, kgc)
        return x[16:48]

    def down2(x):
        pad = jnp.zeros((8, 128), F32)
        g = jnp.concatenate([pad, x, pad], axis=0)
        kg = l2.k * g
        v = l2.sweep(kg, kg)
        r = l2.residual(v, g)
        return g, v, r, restrict(r, t2s, r23)

    def up2(e3, g):
        kg = l2.k * g
        x = l2.sweep(kg, kg) + prolong(e3, t2s, p32)
        for _ in range(2):
            x = l2.sweep(x, kg)
        return x

    l3b = l3.cut(24, 88)
    l4b = l4.cut(12, 44)
    lane1 = (iota((64, 256), 1) >= 64) & (iota((64, 256), 1) < 192)
    lane2 = (iota((32, 128), 1) >= 32) & (iota((32, 128), 1) < 96)

    def dot1(a, b):
        return total(jnp.where(lane1, a[16:80] * b[16:80], 0.0))

    def dot2(a, b):
        return total(jnp.where(lane2, a[16:48] * b[16:48], 0.0))

    def dot3(a, b):
        return total(jnp.where(lane3, a * b, 0.0))

    ra, rb = prolong(w12, t3s, p43), prolong(w6, t3s, p43)
    for _ in range(4):
        ra, rb = l3.sweep0(ra), l3.sweep0(rb)
    ka = l4.k * restrict(-l3.apply(ra), t3s, r34)
    kb = l4.k * restrict(-l3.apply(rb), t3s, r34)
    ea, eb = ka, kb
    for _ in range(5):
        ea, eb = l4.sweep(ea, ka), l4.sweep(eb, kb)
    ra, rb = ra + prolong(ea, t3s, p43), rb + prolong(eb, t3s, p43)
    for _ in range(2):
        ra, rb = l3.sweep0(ra), l3.sweep0(rb)

    s2w = join2(0)
    l2 = Level(2, s2w, gx * 32 - 16, gy * 64 - 32)
    start2 = [prolong(r[40:72], t2s, p32) for r in (ra, rb, f2)]
    after2 = start2
    for _ in range(4):
        after2 = [l2.sweep0(x) for x in after2]
    h_of = [restrict(-l2.apply(x), t2s, r23) for x in after2]
    for n, h in enumerate(h_of):
        send3(h, 3 + n)
    y2 = l2.sweep0(l2.sweep0(prolong(y3[40:72], t2s, p32)))
    f5 = l1.sweep0(l1.sweep0(prolong(y2[8:56], t1s, p21)))
    f5 = l1.sweep0(l1.sweep0(f5)) * (1.0 / 64)
    ga, va, ta, ha = down2(4.0 * restrict(l1.apply(f5), t1s, rm))
    ha = 4.0 * ha
    send3(ha, 6)
    f4 = l2.sweep0(l2.sweep0(y2)) * (1.0 / 16)
    p4_of = [-dot2(f4, l2.apply(x)) for x in start2]
    p54 = -dot3(ha[8:24], f2[48:64])

    sum_next(0)

    g2w = join2(1)
    kg2 = l2.k * g2w
    v2 = l2.sweep(kg2, kg2)
    pv = dot1(f5, l1.residual(v1, g1)) - dot2(va, g2w)
    got(got_g.at[1], 96)
    G3 = g_line[...]
    kg3 = l3.k * G3
    v3 = l3.sweep(kg3, kg3)
    kg4 = l4.k * restrict(l3.residual(v3, G3), t3s, r34)
    e4 = kg4
    for _ in range(11):
        e4 = l4.sweep(e4, kg4)
    x3 = v3 + prolong(e4, t3s, p43)
    for _ in range(4):
        x3 = l3.sweep(x3, kg3)
    kg4 = l4.k * restrict(l3.residual(x3, G3), t3s, r34)
    e4 = kg4
    for _ in range(5):
        e4 = l4.sweep(e4, kg4)
    x3 = x3 + prolong(e4, t3s, p43)
    for _ in range(2):
        x3 = l3.sweep(x3, kg3)

    x2 = v2 + prolong(x3[40:72], t2s, p32)
    p4 = dot2(f4, l2.residual(x2, g2w))
    for _ in range(4):
        x2 = l2.sweep(x2, kg2)
    g3 = restrict(l2.residual(x2, g2w), t2s, r23)
    send3(g3, 0)
    ma = coarse(join3(*take3(6)))[8:24]
    p5 = pv - dot2(ta, x2) - dot3(ma, g3[8:24])
    p5_of = [
        -dot2(ta, x) - dot3(ma, h[8:24]) for x, h in zip(after2, h_of)
    ]
    row = jnp.zeros((1, 128), F32)
    for n, p in enumerate([p4, *p4_of, p5, *p5_of, p54]):
        row = jnp.where(lane == n, p, row)
    sum_start(row, 1)
    tot = sum_end(0)

    z2 = l2.sweep0(l2.sweep0(prolong(f2[40:72], t2s, p32)))
    z1 = prolong(z2[8:56], t1s, p21)
    w1 = l1.sweep0(l1.sweep0(z1))
    d1 = l1.sweep0(l1.sweep0(w1))
    h2, _, _, h3 = down2(restrict(-l1.apply(d1), t1s, rm))
    send3(h3, 2)
    send2(h2[16:48], 3)

    a1, a2, a3, ones_total, w6_total, qw12, qw6 = (pick(tot, n) for n in range(7))
    inv = 1.0 / ones_total
    c1 = a1 * inv
    c2 = (a2 - c1 * w6_total) * inv
    c3 = 0.25 * (a3 - c1 * qw12 - c2 * qw6) * inv

    def with_constants(x, parts):
        return ((x + c1 * parts[0]) + c2 * parts[1]) + c3 * parts[2]

    x2 = with_constants(x2, after2)
    parts = [take3(3 + n) for n in range(3)]
    G = [with_constants(b, p) for b, p in zip(take3(0), zip(*parts))]
    x2 = x2 + prolong(coarse(join3(*G)), t2s, p32)
    for _ in range(2):
        x2 = l2.sweep(x2, kg2)

    x1 = v1 + prolong(x2[8:56], t1s, p21)
    for _ in range(4):
        x1 = l1.sweep(x1, kg1)
    g2, _, _, g3 = down2(restrict(l1.residual(x1, g1), t1s, rm))
    send3(g3, 1)
    send2(g2[16:48], 2)
    sum_next(1)
    e3 = coarse(join3(*take3(2)))
    x2r = up2(e3, join2(3))
    x1r = l1.sweep0(l1.sweep0(d1 + prolong(x2r[8:56], t1s, p21)))

    e3 = coarse(join3(*take3(1)))
    x2 = up2(e3, join2(2))
    x1 = x1 + prolong(x2[8:56], t1s, p21)
    for _ in range(2):
        x1 = l1.sweep(x1, kg1)
    tot = sum_end(1)
    b4, b41, b42, b43, b5, b51, b52, b53, b54 = (pick(tot, n) for n in range(9))
    c4 = with_constants(b4, (b41, b42, b43)) * inv
    c5 = (with_constants(b5, (b51, b52, b53)) + c4 * b54) * inv
    x1 = (x1 + c4 * x1r) + c5 * w1

    for t in range(2):
        y = mm(x1[:, 128 * t : 128 * t + 128], p21[...])
        for h in range(2):
            tmp0[2 * t + h, pl.ds(0, 96, 2), :] = y[:, 128 * h : 128 * h + 128]
            tmp0[2 * t + h, pl.ds(1, 96, 2), :] = y[:, 128 * h : 128 * h + 128]
    for r in range(16, 176, STEP):
        w = slice(8 + r, 8 + r + STEP)
        e = jnp.concatenate([tmp0[t, r : r + STEP, :] for t in range(4)], axis=1)
        wa[w, :] = v0[w, :] + e
    for src, dst in ((wa, wb), (wb, wa)):
        for r in range(16, 176, STEP):
            w = slice(8 + r, 8 + r + STEP)
            c, around = near4(src, r)
            dst[w, :] = 0.2 * c + kg0[w, :] + kk[w, :] * around
    for r in range(32, 160, STEP):
        w = slice(8 + r, 8 + r + STEP)
        c, around = near4(wa, r)
        sol[r - 32 : r - 32 + STEP, :] = c[:, 128:384]
        out = rhs[r - 32 : r - 32 + STEP, :] + around[:, 128:384]
        out = out - (4.0 + shf[r - 32 : r - 32 + STEP, :]) * c[:, 128:384]
        res[r - 32 : r - 32 + STEP, :] = out
    got(all_sent.at[0], sent[0])


def tmp0_pair(ref, t, rows):
    return jnp.concatenate(
        [
            ref[2 * t + h, pl.ds(0, rows // 2, 2), :] + ref[2 * t + h, pl.ds(1, rows // 2, 2), :]
            for h in range(2)
        ],
        axis=1,
    )


def body(right_side, shift):
    v = pltpu.VMEM
    dma = pltpu.SemaphoreType.DMA
    big = v((208, 512), F32)
    scratch = (
        [big] * 7
        + [v((4, 192, 128), F32)]
        + [v((4, 2, 128, 128), F32), v((4, 2, 128, 128), F32), v((4, 1, 112, 128), F32)]
        + [v((256, 128), BF16)]
        + [v((128, 128), BF16)] * 4
        + [v((128, 256), BF16), v((256, 128), BF16)]
        + [v((4, 16, 128), F32), v((112, 128), F32)] * 2
        + [v((16, 128), F32)] * 2
        + [v((2, 16, 128), F32)]
        + [v((4, 8, 32, 128), F32), v((4, 32, 128), F32)]
        + [v((7, 8, 8, 128), F32), v((7, 32, 128), F32), v((7, 2, 8, 128), F32)]
        + [v((2, 2, 1, 128), F32), v((2, 15, 1, 128), F32), v((2, 15, 1, 128), F32)]
        + [v((4096, 128), F32)]
        + [dma((1,)), dma((2,)), dma((2,)), dma((2,)), dma((4,)), dma((7,)), dma((2, 2)), dma((2,))]
    )
    shape = jax.ShapeDtypeStruct((128, 256), F32)
    vm = pl.BlockSpec(memory_space=pltpu.VMEM)
    return pl.pallas_call(
        kernel,
        out_shape=(shape, shape),
        in_specs=[pl.BlockSpec(memory_space=pl.ANY)] * 2,
        out_specs=(vm, vm),
        scratch_shapes=scratch,
        compiler_params=pltpu.CompilerParams(
            collective_id=0, has_side_effects=True, vmem_limit_bytes=40 * 1024 * 1024
        ),
        name="fcycle",
    )(right_side, shift)


def solution(mesh):
    spec = P("gx", "gy")
    return jax.shard_map(
        body, mesh=mesh, in_specs=(spec, spec), out_specs=(spec, spec), check_vma=False
    )
```

```python
import jax
import jax.numpy as jnp
from jax import lax
from jax.experimental import pallas as pl
from jax.experimental.pallas import tpu as pltpu
from jax.sharding import PartitionSpec as P

MESH = pl.DeviceIdType.MESH
F32 = jnp.float32
BF16 = jnp.bfloat16
GX, GY = 8, 32
NX, NY = 1024, 8192
LV_Q = [4.0 ** (-l) for l in range(5)]
LV_D = [4.0 ** (1 - l) for l in range(5)]

AROUND = [(-1, 0), (1, 0), (0, -1), (0, 1), (-1, -1), (-1, 1), (1, -1), (1, 1)]
MIRROR = [1, 0, 3, 2, 7, 6, 5, 4]
SIDE = [-1, 1, -2, 2]
LINE = [-1, 1, -2, 2, -3, 3]
P1, P2, P3, P4 = (1, 1), (2,), (2,), (2,)
PR, P3B, P4B = (1, 1), (2,), (3, 2)
GROUP_A = [(dz, dc) for dz in range(8) for dc in range(2) if dz or dc]
GROUP_B = [(dy, dx) for dy in range(4) for dx in range(4) if dy or dx]


def iota(shape, dim):
    return lax.broadcasted_iota(jnp.int32, shape, dim)


def shifted(v, by):
    by %= v.shape[1]
    return pltpu.roll(v, by, axis=1) if by else v


def updown(v):
    return pltpu.roll(v, 1, axis=0) + pltpu.roll(v, v.shape[0] - 1, axis=0)


def beside(v):
    return updown(v) + (shifted(v, 1) + shifted(v, -1))


class Moved:
    def __init__(self, x):
        self.at = {0: x}

    def __call__(self, by):
        if by not in self.at:
            self.at[by] = shifted(self.at[0], by)
        return self.at[by]


class MovedRows:
    def __init__(self, of, lo, hi):
        self.of, self.lo, self.hi = of, lo, hi

    def __call__(self, by):
        return self.of(by)[self.lo : self.hi]


def inside(shape, level, row0, col0):
    rows = iota(shape, 0) + row0
    cols = iota(shape, 1) + col0
    return (
        (rows >= 0) & (rows < (NX >> level)) & (cols >= 0) & (cols < (NY >> level))
    )


class Level:
    def __init__(self, level, shift, row0, col0, mask=None):
        self.level = level
        self.d = LV_D[level] + shift
        ok = inside(shift.shape, level, row0, col0)
        if mask is not None:
            ok = ok & mask
        self.ok = ok
        self.k = jnp.where(ok, 0.8 / self.d, 0.0)
        self.km = Moved(self.k * LV_Q[level])

    def cut(self, lo, hi):
        out = object.__new__(Level)
        out.level, out.ok = self.level, None
        out.d, out.k = self.d[lo:hi], self.k[lo:hi]
        out.km = MovedRows(self.km, lo, hi)
        return out

    def sweeps(self, v, kg, plan):
        for n in plan:
            v = self.several(v, kg, n)
        return v

    def several(self, v, kg, n):
        v = v if isinstance(v, Moved) else Moved(v)
        x = {s: v(s) for s in range(-n, n + 1)}
        for t in range(n - 1, -1, -1):
            x = {s: self.once(x, kg, s) for s in range(-t, t + 1)}
            if t == 0:
                return x[0]

    def once(self, x, kg, s):
        out = 0.2 * x[s] if kg is None else 0.2 * x[s] + kg(s)
        return out + self.km(s) * (updown(x[s]) + (x[s - 1] + x[s + 1]))

    def down(self, g):
        kg = Moved(self.k * g)
        x = {s: kg(s) for s in range(-2, 3)}
        x = {s: self.once(x, kg, s) for s in range(-1, 2)}
        v = x[0]
        r = g - self.d * v + LV_Q[self.level] * (updown(v) + (x[1] + x[-1]))
        return kg, v, r

    def residual(self, v, g):
        return g - self.d * v + LV_Q[self.level] * beside(v)

    def apply(self, v):
        return self.d * v - LV_Q[self.level] * beside(v)


def mm(x, w):
    m = x.shape[0]
    a = x.astype(BF16)
    r = x - a.astype(F32)
    b = r.astype(BF16)
    c = (r - b.astype(F32)).astype(BF16)
    y = jnp.dot(jnp.concatenate([a, b, c], axis=0), w, preferred_element_type=F32)
    return (y[2 * m :] + y[m : 2 * m]) + y[:m]


def total(x):
    return jnp.sum(jnp.sum(x, axis=0, keepdims=True), axis=1, keepdims=True)


def pick(row, at):
    lane = iota(row.shape, 1)
    return jnp.sum(jnp.where(lane == at, row, 0.0), axis=1, keepdims=True)


def kernel(
    rhs_in, shf_in, sol, res,
    xg, xs, kk, kg0, v0, wa, wb, tmp0,
    t1s, t2s, t3s,
    rm, r23, r34, p43, p32, p21, r03,
    s_side, s_line, g_side, g_line, own3, own3g, ownb,
    x2b, own2, x3b, own3n, own3p,
    ar_in, ar_a, ar_b,
    edge_out, edge_in, corner_out, corner_in, rows_of, all_sent, got_border, got_s, got_g, got_2, got_3, got_sum, in_s,
):
    gx = lax.axis_index("gx")
    gy = lax.axis_index("gy")
    core = lax.rem(gy, 2)
    quad = lax.div(gy, 2)
    qy, qx = lax.div(quad, 4), lax.rem(quad, 4)

    def past(at, by, size):
        if by > 0:
            return lax.div(at + by, size)
        return 1 - lax.div(at + (by + size), size) if by < 0 else 0 * at

    other_core = gy + 1 - 2 * core
    other_row = gx + 1 - 2 * lax.rem(gx, 2)

    def beyond(dz, dy):
        if not dy:
            out = past(gx, dz, GX)
            return (gx + (1 - out) * dz, gy + out * (other_core - gy)), out
        if not dz:
            out = past(gy, dy, GY)
            return (gx + out * (other_row - gx), gy + (1 - out) * dy), out
        zo, yo = past(gx, dz, GX), past(gy, dy, GY)
        high = lax.div(gx, 4)
        if dz > 0:
            ring = (1 - high) * other_row + high * (4 + lax.rem(gx, 3))
        else:
            ring = high * other_row + (1 - high) * (1 + lax.rem(gx, 3))
        to_z = zo * gx + (1 - zo) * (yo * ring + (1 - yo) * (gx + dz))
        to_y = zo * other_core + (1 - zo) * (yo * gy + (1 - yo) * (gy + dy))
        return (to_z, to_y), zo + (1 - zo) * yo

    def slot(n, mirror, out):
        return n + out * (mirror - n)

    def in_a(dz, dc):
        return (lax.rem(gx + dz, GX), gy - core + lax.rem(core + dc, 2))

    def in_b(dy, dx):
        return (gx, (lax.rem(qy + dy, 4) * 4 + lax.rem(qx + dx, 4)) * 2 + core)

    barrier = pltpu.get_barrier_semaphore()
    partners = (
        [beyond(*o)[0] for o in AROUND]
        + [in_a(*o) for o in GROUP_A]
        + [in_b(*o) for o in GROUP_B]
    )
    for p in partners:
        pl.semaphore_signal(barrier, inc=1, device_id=p, device_id_type=MESH)

    mid = (slice(40, 168), slice(128, 384))
    rhs, shf = xg.at[mid], xs.at[mid]
    in_shf = pltpu.make_async_copy(shf_in, shf, in_s.at[0])
    in_rhs = pltpu.make_async_copy(rhs_in, rhs, in_s.at[1])
    in_shf.start()
    in_rhs.start()

    sent = [0]
    turn = [0]

    def got(sem, rows):
        ref = rows_of.at[0:rows]
        pltpu.make_async_copy(ref, ref, sem).wait()

    def scratch(pool):
        turn[0] += 1
        return pool.at[turn[0] % pool.shape[0]]

    def send(src, dst, sem, dev):
        pltpu.make_async_remote_copy(
            src_ref=src, dst_ref=dst, send_sem=all_sent.at[0], recv_sem=sem,
            device_id=dev, device_id_type=MESH,
        ).start()
        size = src.shape[0] * src.shape[1] // 128
        sent[0] += size
        return size

    i, j = iota((256, 128), 0), iota((256, 128), 1)
    rm[...] = jnp.where((i >> 1) == j, 0.25, 0.0).astype(BF16)
    r03[...] = jnp.where((i >> 3) + 48 == j, 1.0 / 64, 0.0).astype(BF16)
    i, j = iota((128, 128), 0), iota((128, 128), 1)
    r34[...] = jnp.where((i >> 1) == j, 0.25, 0.0).astype(BF16)
    r23[...] = jnp.where((i >> 1) + 32 == j, 0.25, 0.0).astype(BF16)
    p43[...] = jnp.where(i == (j >> 1), 1.0, 0.0).astype(BF16)
    p32[...] = jnp.where(i == (j >> 1) + 32, 1.0, 0.0).astype(BF16)
    i, j = iota((128, 256), 0), iota((128, 256), 1)
    p21[...] = jnp.where(i == (j >> 1), 1.0, 0.0).astype(BF16)

    def pair_rows(ref, rows, lanes):
        return jnp.concatenate(
            [
                ref[t, pl.ds(0, rows // 2, 2), :] + ref[t, pl.ds(1, rows // 2, 2), :]
                for t in range(lanes // 128)
            ],
            axis=1,
        )

    def put(ref, x):
        for t in range(x.shape[1] // 128):
            ref[t, 0 : x.shape[0], :] = x[:, 128 * t : 128 * t + 128]

    def restrict(x, pool, w):
        ref = scratch(pool)
        put(ref, x)
        return mm(pair_rows(ref, x.shape[0], x.shape[1]), w[...])

    def prolong(e, pool, w):
        ref = scratch(pool)
        y = mm(e, w[...])
        m = y.shape[0]
        out = []
        for t in range(y.shape[1] // 128):
            yt = y[:, 128 * t : 128 * t + 128]
            ref[t, pl.ds(0, m, 2), :] = yt
            ref[t, pl.ds(1, m, 2), :] = yt
            out.append(ref[t, 0 : 2 * m, :])
        return jnp.concatenate(out, axis=1) if len(out) > 1 else out[0]

    zero8 = jnp.zeros((8, 512), F32)
    for ref in (kg0, v0, wa, wb):
        ref[0:8, :] = zero8
        ref[200:208, :] = zero8
    for ref in (xs, xg):
        ref[8:16, :] = zero8
        ref[192:200, :] = zero8

    in_shf.wait()
    s0 = shf[...]
    put(tmp0, s0)
    acc = pair_rows(tmp0, 128, 256)
    s1own = mm(acc, rm[...])
    ref1, ref2 = scratch(t1s), scratch(t2s)
    put(ref1, acc)
    acc = pair_rows(ref1, 64, 256)
    put(ref2, acc)
    own3[...] = mm(pair_rows(ref2, 32, 256), r03[...])
    own2[0] = pltpu.roll(restrict(s1own, t1s, r34), 32, axis=1)
    in_rhs.wait()

    def pack_border(f, x):
        for side in range(2):
            e = x[:, 128 * side : 128 * side + 128]
            at = 96 * side
            lane = iota((32, 128), 1)
            out = shifted(e[0:32], -at)
            for n in range(1, 4):
                out = jnp.where(lane < 32 * n, out, shifted(e[32 * n : 32 * n + 32], 32 * n - at))
            edge_out[f, side] = out
            lane = iota((8, 128), 1)
            for end in range(2):
                top = 104 * end
                out = shifted(e[top : top + 8], -at)
                for n in range(1, 3):
                    part = e[top + 8 * n : top + 8 * n + 8]
                    out = jnp.where(lane < 32 * n, out, shifted(part, 32 * n - at))
                corner_out[f, 2 * end + side] = out

    pack_border(1, s0)
    pack_border(0, rhs[...])

    pl.semaphore_wait(barrier, len(partners))

    def border(f):
        src, dst = (shf, xs) if f else (rhs, xg)
        sem = got_border.at[f]
        rows = 0
        for dz, lo, to, mirror in ((-1, 0, 168, 16), (1, 104, 16, 168)):
            dev, out = beyond(dz, 0)
            at = pl.ds(pl.multiple_of(slot(to, mirror, out), 8), 24)
            rows += send(src.at[lo : lo + 24, :], dst.at[at, 128:384], sem, dev)
        for side in range(2):
            dy = 2 * side - 1
            dev, out = beyond(0, dy)
            rows += send(edge_out.at[f, side], edge_in.at[f, slot(side, 1 - side, out)], sem, dev)
            for end in range(2):
                n = 2 * end + side
                dev, out = beyond(2 * end - 1, dy)
                rows += send(corner_out.at[f, n], corner_in.at[f, slot(n, 3 - n, out)], sem, dev)
        return rows

    def unpack_border(f):
        dst = xs if f else xg
        for side in range(2):
            lo = 0 if side else 384
            at = 96 * side
            lane = iota((32, 128), 1)
            keep = lane >= 96 if side else lane < 32
            p = edge_in[f, side]
            for n in range(4):
                dst[40 + 32 * n : 72 + 32 * n, lo : lo + 128] = jnp.where(
                    keep, shifted(p, at - 32 * n), 0.0
                )
            lane = iota((8, 128), 1)
            keep = lane >= 96 if side else lane < 32
            for end in range(2):
                top = 16 if end else 168
                p = corner_in[f, 2 * end + side]
                for n in range(3):
                    dst[top + 8 * n : top + 8 * n + 8, lo : lo + 128] = jnp.where(
                        keep, shifted(p, at - 32 * n), 0.0
                    )

    def side_send(src, buf, sem):
        for n, d in enumerate(SIDE):
            dev, out = beyond(0, d)
            send(src, buf.at[slot(n, n ^ 1, out)], sem.at[0], dev)

    def side_join(own, buf, sem):
        got(sem.at[0], 64)
        right1, left1, right2, left2 = (buf[n] for n in range(4))
        lane = iota((16, 128), 1)
        out = jnp.where(lane < 48, pltpu.roll(left1, 96, axis=1), own)
        out = jnp.where(lane < 16, pltpu.roll(left2, 64, axis=1), out)
        out = jnp.where(lane >= 80, pltpu.roll(right1, 32, axis=1), out)
        return jnp.where(lane >= 112, pltpu.roll(right2, 64, axis=1), out)

    def line_send(src, buf, sem):
        for d in LINE:
            dev, out = beyond(d, 0)
            at = pl.ds(pl.multiple_of(16 * slot(3 - d, 3 + d, out), 8), 16)
            send(src, buf.at[at], sem.at[1], dev)

    SRC2 = {-1: (0, 16), 1: (16, 32), 0: (0, 32)}

    def send2(x, k):
        own2[k] = x
        for n, (dz, dy) in enumerate(AROUND):
            a, b = SRC2[dz]
            dev, out = beyond(dz, dy)
            at = slot(n, MIRROR[n], out)
            send(own2.at[k, a:b], x2b.at[k, at, 0 : b - a], got_2.at[k], dev)

    def lanes3(left, mid, right, lo, hi, move):
        lane = iota(mid.shape, 1)
        out = jnp.where(lane < lo, pltpu.roll(left, 128 - move, axis=1), mid)
        return jnp.where(lane >= hi, pltpu.roll(right, move, axis=1), out)

    def join2(k):
        got(got_2.at[k], 6 * 16 + 2 * 32)
        own, buf = own2[k], x2b.at[k]
        dn, up, rt, lf, dr, dl, ur, ul = range(8)
        return jnp.concatenate(
            [
                lanes3(buf[ul, 0:16], buf[up, 0:16], buf[ur, 0:16], 32, 96, 64),
                lanes3(buf[lf], own, buf[rt], 32, 96, 64),
                lanes3(buf[dl, 0:16], buf[dn, 0:16], buf[dr, 0:16], 32, 96, 64),
            ],
            axis=0,
        )

    def pack3(x, lo):
        lane = iota((8, 128), 1)
        a, b, c = (x[lo + 8 * n : lo + 8 * n + 8] for n in range(3))
        out = jnp.where(lane < 64, pltpu.roll(b, 112, axis=1), pltpu.roll(c, 16, axis=1))
        return jnp.where(lane < 32, pltpu.roll(a, 80, axis=1), out)

    def send3(x, k):
        own3n[k] = x
        own3p[k, 0] = pack3(x, 8)
        own3p[k, 1] = pack3(x, 0)
        for n, (dz, dy) in enumerate(AROUND):
            dev, out = beyond(dz, dy)
            at = slot(n, MIRROR[n], out)
            send(own3p.at[k, 1 if dz == 1 else 0], x3b.at[k, at], got_3.at[k], dev)

    def take3(k):
        got(got_3.at[k], 64)
        return [own3n[k, 8:24]] + [x3b[k, n] for n in range(8)]

    def join3(own, dn, up, rt, lf, dr, dl, ur, ul):
        lane = iota((8, 128), 1)

        def at(x, n, dest):
            move = (dest - 32 * n) % 128
            return pltpu.roll(x, move, axis=1) if move else x

        rows = []
        for left, centre, right, count in ((ul, up, ur, 3), (lf, None, rt, 2), (dl, dn, dr, 3)):
            for n in range(count):
                c = own[8 * n : 8 * n + 8] if centre is None else at(centre, n, 48)
                out = jnp.where(lane < 80, c, at(right, n, 80))
                rows.append(jnp.where(lane < 48, at(left, n, 16), out))
        return jnp.concatenate(rows, axis=0)

    def sum_start(row, k):
        ar_in[k, 0] = row
        for n, o in enumerate(GROUP_A):
            send(ar_in.at[k, 0], ar_a.at[k, n], got_sum.at[k, 0], in_a(*o))

    def sum_next(k):
        got(got_sum.at[k, 0], 15)
        ar_in[k, 1] = ar_in[k, 0] + jnp.sum(ar_a[k], axis=0)
        for n, o in enumerate(GROUP_B):
            send(ar_in.at[k, 1], ar_b.at[k, n], got_sum.at[k, 1], in_b(*o))

    def sum_end(k):
        got(got_sum.at[k, 1], 15)
        return ar_in[k, 1] + jnp.sum(ar_b[k], axis=0)

    side_send(own3, s_side, got_s)
    border_rows = border(1)
    border(0)
    send2(own2[0], 0)
    s_row = side_join(own3[...], s_side, got_s)
    ownb[0] = s_row
    line_send(ownb.at[0], s_line, got_s)
    s_line[48:64] = s_row

    row0 = gx * 128 - 32
    col0 = gy * 256 - 128
    got(got_border.at[1], border_rows)
    unpack_border(1)
    STEP = 16

    def near4(ref, r, n=STEP):
        c = ref[8 + r : 8 + r + n, :]
        around = (
            ref[7 + r : 7 + r + n, :]
            + ref[9 + r : 9 + r + n, :]
            + pltpu.roll(c, 1, axis=1)
            + pltpu.roll(c, 511, axis=1)
        )
        return c, around

    for r in range(0, 192, STEP):
        w = slice(8 + r, 8 + r + STEP)
        ok = inside((STEP, 512), 0, row0 + r, col0)
        kk[w, :] = jnp.where(ok, 0.8 / (4.0 + xs[w, :]), 0.0)
    put(tmp0, xs[8:200, :])
    s1 = jnp.concatenate(
        [
            mm(tmp0_pair(tmp0, t, 192), rm[...])
            for t in range(2)
        ],
        axis=1,
    )
    l1 = Level(1, s1, gx * 64 - 16, gy * 128 - 64)
    s2 = restrict(s1, t1s, rm)
    l2a = Level(2, s2, gx * 32 - 8, gy * 64 - 32)

    got(got_border.at[0], border_rows)
    unpack_border(0)
    for r in range(0, 192, STEP):
        w = slice(8 + r, 8 + r + STEP)
        kg0[w, :] = kk[w, :] * xg[w, :]
    for r in range(0, 192, STEP):
        w = slice(8 + r, 8 + r + STEP)
        c, around = near4(kg0, r)
        v0[w, :] = 1.2 * c + kk[w, :] * around
    for r in range(0, 192, STEP):
        w = slice(8 + r, 8 + r + STEP)
        c, around = near4(v0, r)
        out = xg[w, :] - (4.0 + xs[w, :]) * c + around
        for t in range(4):
            tmp0[t, r : r + STEP, :] = out[:, 128 * t : 128 * t + 128]
    g1 = jnp.concatenate([mm(tmp0_pair(tmp0, t, 192), rm[...]) for t in range(2)], axis=1)

    kg1, v1, r1 = l1.down(g1)
    g2 = restrict(r1, t1s, rm)
    _, _, r2 = l2a.down(g2)
    g3 = restrict(r2, t2s, r23)
    g3own = g3[4:20]
    own3g[...] = g3own
    side_send(own3g, g_side, got_g)
    send2(g2[8:40], 1)

    got(got_s.at[1], 96)
    l3 = Level(3, s_line[...], gx * 16 - 48, gy * 32 - 48)
    s4 = restrict(s_line[...], t3s, r34)
    l4 = Level(4, s4, gx * 8 - 24, gy * 16 - 24, iota((56, 128), 1) < 64)

    one4 = jnp.where(l4.ok, 1.0, 0.0)
    one3 = jnp.where(l3.ok, 1.0, 0.0)
    w6 = l4.sweeps(one4, None, P4 * 3)
    w12 = l4.sweeps(w6, None, P4 * 3)
    y3 = l3.sweeps(one3, None, P3)
    u = l3.sweeps(y3, None, P3)
    q = 4.0 * restrict(jnp.where(l3.ok, l3.apply(u), 0.0), t3s, r34)
    kq = Moved(l4.k * q)
    z = l4.sweeps(kq, kq, P4 * 5 + (1,))
    f3 = l3.sweeps(u - 0.25 * prolong(z, t3s, p43), None, P3)
    f2 = l3.sweeps(prolong(w6, t3s, p43), None, P3)
    lane3 = (iota((16, 128), 1) >= 48) & (iota((16, 128), 1) < 80)
    lane4 = (iota((8, 128), 1) >= 24) & (iota((8, 128), 1) < 40)
    g3m = jnp.where(lane3, g3own, 0.0)

    def own4(x):
        return jnp.where(lane4, x[24:32], 0.0)

    parts = [
        0.25 * total(y3[48:64] * g3m),
        0.25 * total(f2[48:64] * g3m),
        total(f3[48:64] * g3m),
        total(own4(l4.apply(one4))),
        total(own4(l4.apply(w6))),
        total(own4(q * w12)),
        total(own4(q * w6)),
    ]
    lane = iota((1, 128), 1)
    row = jnp.zeros((1, 128), F32)
    for n, p in enumerate(parts):
        row = jnp.where(lane == n, p, row)
    sum_start(row, 0)

    def coarse(G):
        kgc, v, r = l3b.down(G)
        kgd = Moved(l4b.k * restrict(r, t3s, r34))
        e = l4b.sweeps(kgd, kgd, P4B)
        return l3b.sweeps(v + prolong(e, t3s, p43), kgc, P3B)[16:48]

    def down2(x):
        pad = jnp.zeros((8, 128), F32)
        g = jnp.concatenate([pad, x, pad], axis=0)
        kg, v, r = l2.down(g)
        return g, v, r, restrict(r, t2s, r23)

    def up2(e3, g):
        kg, v, _ = l2.down(g)
        return l2.sweeps(v + prolong(e3, t2s, p32), kg, P2)

    l3b = l3.cut(24, 88)
    l4b = l4.cut(12, 44)
    lane1 = (iota((64, 256), 1) >= 64) & (iota((64, 256), 1) < 192)
    lane2 = (iota((32, 128), 1) >= 32) & (iota((32, 128), 1) < 96)

    def dot1(a, b):
        return total(jnp.where(lane1, a[16:80] * b[16:80], 0.0))

    def dot2(a, b):
        return total(jnp.where(lane2, a[16:48] * b[16:48], 0.0))

    def dot3(a, b):
        return total(jnp.where(lane3, a * b, 0.0))

    s2w = join2(0)
    l2 = Level(2, s2w, gx * 32 - 16, gy * 64 - 32)
    y2 = l2.sweeps(prolong(y3[40:72], t2s, p32), None, P2)
    f5 = l1.sweeps(prolong(y2[8:56], t1s, p21), None, P1 * 2) * (1.0 / 64)
    ga, va, ta, ha = down2(4.0 * restrict(l1.apply(f5), t1s, rm))
    ha = 4.0 * ha
    send3(ha, 6)

    g_row = side_join(g3own, g_side, got_g)
    ownb[1] = g_row
    line_send(ownb.at[1], g_line, got_g)
    g_line[48:64] = g_row

    ra, rb = prolong(w12, t3s, p43), prolong(w6, t3s, p43)
    ra, rb = (l3.sweeps(x, None, PR * 2) for x in (ra, rb))
    ka, kb = (Moved(l4.k * restrict(-l3.apply(x), t3s, r34)) for x in (ra, rb))
    ea, eb = (l4.sweeps(x, x, P4 * 2 + (1,)) for x in (ka, kb))
    ra, rb = ra + prolong(ea, t3s, p43), rb + prolong(eb, t3s, p43)
    ra, rb = (l3.sweeps(x, None, PR) for x in (ra, rb))

    start2 = [prolong(r[40:72], t2s, p32) for r in (ra, rb, f2)]
    after2 = [l2.sweeps(x, None, P2 * 2) for x in start2]
    h_of = [restrict(-l2.apply(x), t2s, r23) for x in after2]
    for n, h in enumerate(h_of):
        send3(h, 3 + n)
    f4 = l2.sweeps(y2, None, P2) * (1.0 / 16)
    p4_of = [-dot2(f4, l2.apply(x)) for x in start2]
    p54 = -dot3(ha[8:24], f2[48:64])
    z2 = l2.sweeps(start2[2], None, P2)
    w1 = l1.sweeps(prolong(z2[8:56], t1s, p21), None, P1)
    d1 = l1.sweeps(w1, None, P1)
    h2, _, _, h3 = down2(restrict(-l1.apply(d1), t1s, rm))
    send3(h3, 2)
    send2(h2[16:48], 3)

    sum_next(0)

    g2w = join2(1)
    kg2, v2, _ = l2.down(g2w)
    pv = dot1(f5, l1.residual(v1, g1)) - dot2(va, g2w)
    got(got_g.at[1], 96)
    G3 = g_line[...]
    kg3, v3, r3 = l3.down(G3)
    kg4 = Moved(l4.k * restrict(r3, t3s, r34))
    e4 = l4.sweeps(kg4, kg4, P4 * 5 + (1,))
    x3 = l3.sweeps(v3 + prolong(e4, t3s, p43), kg3, P3 * 2)
    kg4 = Moved(l4.k * restrict(l3.residual(x3, G3), t3s, r34))
    e4 = l4.sweeps(kg4, kg4, P4 * 2 + (1,))
    x3 = l3.sweeps(x3 + prolong(e4, t3s, p43), kg3, P3)

    x2 = v2 + prolong(x3[40:72], t2s, p32)
    p4 = dot2(f4, l2.residual(x2, g2w))
    x2 = l2.sweeps(x2, kg2, P2 * 2)
    g3 = restrict(l2.residual(x2, g2w), t2s, r23)
    send3(g3, 0)
    ma = coarse(join3(*take3(6)))[8:24]
    p5 = pv - dot2(ta, x2) - dot3(ma, g3[8:24])
    p5_of = [
        -dot2(ta, x) - dot3(ma, h[8:24]) for x, h in zip(after2, h_of)
    ]
    row = jnp.zeros((1, 128), F32)
    for n, p in enumerate([p4, *p4_of, p5, *p5_of, p54]):
        row = jnp.where(lane == n, p, row)
    sum_start(row, 1)
    tot = sum_end(0)

    a1, a2, a3, ones_total, w6_total, qw12, qw6 = (pick(tot, n) for n in range(7))
    inv = 1.0 / ones_total
    c1 = a1 * inv
    c2 = (a2 - c1 * w6_total) * inv
    c3 = 0.25 * (a3 - c1 * qw12 - c2 * qw6) * inv

    def with_constants(x, parts):
        return ((x + c1 * parts[0]) + c2 * parts[1]) + c3 * parts[2]

    x2 = with_constants(x2, after2)
    parts = [take3(3 + n) for n in range(3)]
    G = [with_constants(b, p) for b, p in zip(take3(0), zip(*parts))]
    x2 = x2 + prolong(coarse(join3(*G)), t2s, p32)
    x2 = l2.sweeps(x2, kg2, P2)

    x1 = v1 + prolong(x2[8:56], t1s, p21)
    x1 = l1.sweeps(x1, kg1, P1 * 2)
    g2, _, _, g3 = down2(restrict(l1.residual(x1, g1), t1s, rm))
    send3(g3, 1)
    send2(g2[16:48], 2)
    sum_next(1)
    e3 = coarse(join3(*take3(2)))
    x2r = up2(e3, join2(3))
    x1r = l1.sweeps(d1 + prolong(x2r[8:56], t1s, p21), None, P1)

    e3 = coarse(join3(*take3(1)))
    x2 = up2(e3, join2(2))
    x1 = x1 + prolong(x2[8:56], t1s, p21)
    x1 = l1.sweeps(x1, kg1, P1)
    tot = sum_end(1)
    b4, b41, b42, b43, b5, b51, b52, b53, b54 = (pick(tot, n) for n in range(9))
    c4 = with_constants(b4, (b41, b42, b43)) * inv
    c5 = (with_constants(b5, (b51, b52, b53)) + c4 * b54) * inv
    x1 = (x1 + c4 * x1r) + c5 * w1

    for t in range(2):
        y = mm(x1[:, 128 * t : 128 * t + 128], p21[...])
        for h in range(2):
            tmp0[2 * t + h, pl.ds(0, 96, 2), :] = y[:, 128 * h : 128 * h + 128]
            tmp0[2 * t + h, pl.ds(1, 96, 2), :] = y[:, 128 * h : 128 * h + 128]
    for r in range(16, 176, STEP):
        w = slice(8 + r, 8 + r + STEP)
        e = jnp.concatenate([tmp0[t, r : r + STEP, :] for t in range(4)], axis=1)
        wa[w, :] = v0[w, :] + e
    for src, dst in ((wa, wb), (wb, wa)):
        for r in range(16, 176, STEP):
            w = slice(8 + r, 8 + r + STEP)
            c, around = near4(src, r)
            dst[w, :] = 0.2 * c + kg0[w, :] + kk[w, :] * around
    for r in range(32, 160, STEP):
        w = slice(8 + r, 8 + r + STEP)
        c, around = near4(wa, r)
        sol[r - 32 : r - 32 + STEP, :] = c[:, 128:384]
        out = rhs[r - 32 : r - 32 + STEP, :] + around[:, 128:384]
        out = out - (4.0 + shf[r - 32 : r - 32 + STEP, :]) * c[:, 128:384]
        res[r - 32 : r - 32 + STEP, :] = out
    got(all_sent.at[0], sent[0])


def tmp0_pair(ref, t, rows):
    return jnp.concatenate(
        [
            ref[2 * t + h, pl.ds(0, rows // 2, 2), :] + ref[2 * t + h, pl.ds(1, rows // 2, 2), :]
            for h in range(2)
        ],
        axis=1,
    )


def body(right_side, shift):
    v = pltpu.VMEM
    dma = pltpu.SemaphoreType.DMA
    big = v((208, 512), F32)
    scratch = (
        [big] * 7
        + [v((4, 192, 128), F32)]
        + [v((4, 2, 128, 128), F32), v((4, 2, 128, 128), F32), v((4, 1, 112, 128), F32)]
        + [v((256, 128), BF16)]
        + [v((128, 128), BF16)] * 4
        + [v((128, 256), BF16), v((256, 128), BF16)]
        + [v((4, 16, 128), F32), v((112, 128), F32)] * 2
        + [v((16, 128), F32)] * 2
        + [v((2, 16, 128), F32)]
        + [v((4, 8, 32, 128), F32), v((4, 32, 128), F32)]
        + [v((7, 8, 8, 128), F32), v((7, 32, 128), F32), v((7, 2, 8, 128), F32)]
        + [v((2, 2, 1, 128), F32), v((2, 15, 1, 128), F32), v((2, 15, 1, 128), F32)]
        + [v((2, 2, 32, 128), F32)] * 2
        + [v((2, 4, 8, 128), F32)] * 2
        + [v((4096, 128), F32)]
        + [dma((1,)), dma((2,)), dma((2,)), dma((2,)), dma((4,)), dma((7,)), dma((2, 2)), dma((2,))]
    )
    shape = jax.ShapeDtypeStruct((128, 256), F32)
    vm = pl.BlockSpec(memory_space=pltpu.VMEM)
    return pl.pallas_call(
        kernel,
        out_shape=(shape, shape),
        in_specs=[pl.BlockSpec(memory_space=pl.ANY)] * 2,
        out_specs=(vm, vm),
        scratch_shapes=scratch,
        compiler_params=pltpu.CompilerParams(
            collective_id=0, has_side_effects=True, vmem_limit_bytes=40 * 1024 * 1024
        ),
        name="fcycle",
    )(right_side, shift)


def solution(mesh):
    spec = P("gx", "gy")
    return jax.shard_map(
        body, mesh=mesh, in_specs=(spec, spec), out_specs=(spec, spec), check_vma=False
    )
```

```python
import jax
import jax.numpy as jnp
from jax import lax
from jax.experimental import pallas as pl
from jax.experimental.pallas import tpu as pltpu
from jax.sharding import PartitionSpec as P

MESH = pl.DeviceIdType.MESH
F32 = jnp.float32
BF16 = jnp.bfloat16
GX, GY = 8, 32
NX, NY = 1024, 8192
LV_Q = [4.0 ** (-l) for l in range(5)]
LV_D = [4.0 ** (1 - l) for l in range(5)]

AROUND = [(-1, 0), (1, 0), (0, -1), (0, 1), (-1, -1), (-1, 1), (1, -1), (1, 1)]
MIRROR = [1, 0, 3, 2, 7, 6, 5, 4]
SIDE = [-1, 1, -2, 2]
LINE = [-1, 1, -2, 2, -3, 3]
P1, P2, P3, P4 = (1, 1), (2,), (2,), (2,)
PR, P3B, P4B = (1, 1), (2,), (3, 2)
GROUP_A = [(dz, dc) for dz in range(8) for dc in range(2) if dz or dc]
GROUP_B = [(dy, dx) for dy in range(4) for dx in range(4) if dy or dx]


def iota(shape, dim):
    return lax.broadcasted_iota(jnp.int32, shape, dim)


def shifted(v, by):
    by %= v.shape[1]
    return pltpu.roll(v, by, axis=1) if by else v


def updown(v):
    return pltpu.roll(v, 1, axis=0) + pltpu.roll(v, v.shape[0] - 1, axis=0)


def beside(v):
    return updown(v) + (shifted(v, 1) + shifted(v, -1))


class Moved:
    def __init__(self, x):
        self.at = {0: x}

    def __call__(self, by):
        if by not in self.at:
            self.at[by] = shifted(self.at[0], by)
        return self.at[by]


class MovedRows:
    def __init__(self, of, lo, hi):
        self.of, self.lo, self.hi = of, lo, hi

    def __call__(self, by):
        return self.of(by)[self.lo : self.hi]


def inside(shape, level, row0, col0):
    rows = iota(shape, 0) + row0
    cols = iota(shape, 1) + col0
    return (
        (rows >= 0) & (rows < (NX >> level)) & (cols >= 0) & (cols < (NY >> level))
    )


class Level:
    def __init__(self, level, shift, row0, col0, mask=None):
        self.level = level
        self.d = LV_D[level] + shift
        ok = inside(shift.shape, level, row0, col0)
        if mask is not None:
            ok = ok & mask
        self.ok = ok
        self.k = jnp.where(ok, 0.8 / self.d, 0.0)
        self.km = Moved(self.k * LV_Q[level])

    def cut(self, lo, hi):
        out = object.__new__(Level)
        out.level, out.ok = self.level, None
        out.d, out.k = self.d[lo:hi], self.k[lo:hi]
        out.km = MovedRows(self.km, lo, hi)
        return out

    def sweeps(self, v, kg, plan):
        for n in plan:
            v = self.several(v, kg, n)
        return v

    def several(self, v, kg, n):
        v = v if isinstance(v, Moved) else Moved(v)
        x = {s: v(s) for s in range(-n, n + 1)}
        for t in range(n - 1, -1, -1):
            x = {s: self.once(x, kg, s) for s in range(-t, t + 1)}
            if t == 0:
                return x[0]

    def once(self, x, kg, s):
        out = 0.2 * x[s] if kg is None else 0.2 * x[s] + kg(s)
        return out + self.km(s) * (updown(x[s]) + (x[s - 1] + x[s + 1]))

    def down(self, g):
        kg = Moved(self.k * g)
        x = {s: kg(s) for s in range(-2, 3)}
        x = {s: self.once(x, kg, s) for s in range(-1, 2)}
        v = x[0]
        r = g - self.d * v + LV_Q[self.level] * (updown(v) + (x[1] + x[-1]))
        return kg, v, r

    def residual(self, v, g):
        return g - self.d * v + LV_Q[self.level] * beside(v)

    def apply(self, v):
        return self.d * v - LV_Q[self.level] * beside(v)


def mm(x, w):
    m = x.shape[0]
    a = x.astype(BF16)
    r = x - a.astype(F32)
    b = r.astype(BF16)
    c = (r - b.astype(F32)).astype(BF16)
    y = jnp.dot(jnp.concatenate([a, b, c], axis=0), w, preferred_element_type=F32)
    return (y[2 * m :] + y[m : 2 * m]) + y[:m]


def total(x):
    return jnp.sum(jnp.sum(x, axis=0, keepdims=True), axis=1, keepdims=True)


def pick(row, at):
    lane = iota(row.shape, 1)
    return jnp.sum(jnp.where(lane == at, row, 0.0), axis=1, keepdims=True)


def kernel(
    rhs_in, shf_in, sol, res,
    xg, xs, kk, kg0, v0, wa, wb, tmp0,
    t1s, t2s, t3s,
    rm, r23, r34, p43, p32, p21, r03,
    s_side, s_line, g_side, g_line, own3, own3g, ownb,
    x2b, own2, x3b, own3n, own3p,
    ar_in, ar_a, ar_b,
    edge_out, edge_in, corner_out, corner_in, rows_of, all_sent, got_border, got_s, got_g, got_2, got_3, got_sum, in_s,
):
    gx = lax.axis_index("gx")
    gy = lax.axis_index("gy")
    core = lax.rem(gy, 2)
    quad = lax.div(gy, 2)
    qy, qx = lax.div(quad, 4), lax.rem(quad, 4)

    def past(at, by, size):
        if by > 0:
            return lax.div(at + by, size)
        return 1 - lax.div(at + (by + size), size) if by < 0 else 0 * at

    other_core = gy + 1 - 2 * core
    other_row = gx + 1 - 2 * lax.rem(gx, 2)

    def beyond(dz, dy):
        if not dy:
            out = past(gx, dz, GX)
            return (gx + (1 - out) * dz, gy + out * (other_core - gy)), out
        if not dz:
            out = past(gy, dy, GY)
            return (gx + out * (other_row - gx), gy + (1 - out) * dy), out
        zo, yo = past(gx, dz, GX), past(gy, dy, GY)
        high = lax.div(gx, 4)
        if dz > 0:
            ring = (1 - high) * other_row + high * (4 + lax.rem(gx, 3))
        else:
            ring = high * other_row + (1 - high) * (1 + lax.rem(gx, 3))
        to_z = zo * gx + (1 - zo) * (yo * ring + (1 - yo) * (gx + dz))
        to_y = zo * other_core + (1 - zo) * (yo * gy + (1 - yo) * (gy + dy))
        return (to_z, to_y), zo + (1 - zo) * yo

    def slot(n, mirror, out):
        return n + out * (mirror - n)

    def in_a(dz, dc):
        return (lax.rem(gx + dz, GX), gy - core + lax.rem(core + dc, 2))

    def in_b(dy, dx):
        return (gx, (lax.rem(qy + dy, 4) * 4 + lax.rem(qx + dx, 4)) * 2 + core)

    barrier = pltpu.get_barrier_semaphore()
    partners = (
        [beyond(*o)[0] for o in AROUND]
        + [in_a(*o) for o in GROUP_A]
        + [in_b(*o) for o in GROUP_B]
    )
    for p in partners:
        pl.semaphore_signal(barrier, inc=1, device_id=p, device_id_type=MESH)

    mid = (slice(40, 168), slice(128, 384))
    rhs, shf = xg.at[mid], xs.at[mid]
    in_shf = pltpu.make_async_copy(shf_in, shf, in_s.at[0])
    in_rhs = pltpu.make_async_copy(rhs_in, rhs, in_s.at[1])
    in_shf.start()
    in_rhs.start()

    sent = [0]
    turn = [0]

    def got(sem, rows):
        ref = rows_of.at[0:rows]
        pltpu.make_async_copy(ref, ref, sem).wait()

    def scratch(pool):
        turn[0] += 1
        return pool.at[turn[0] % pool.shape[0]]

    def send(src, dst, sem, dev):
        pltpu.make_async_remote_copy(
            src_ref=src, dst_ref=dst, send_sem=all_sent.at[0], recv_sem=sem,
            device_id=dev, device_id_type=MESH,
        ).start()
        size = src.shape[0] * src.shape[1] // 128
        sent[0] += size
        return size

    i, j = iota((256, 128), 0), iota((256, 128), 1)
    rm[...] = jnp.where((i >> 1) == j, 0.25, 0.0).astype(BF16)
    r03[...] = jnp.where((i >> 3) + 48 == j, 1.0 / 64, 0.0).astype(BF16)
    i, j = iota((128, 128), 0), iota((128, 128), 1)
    r34[...] = jnp.where((i >> 1) == j, 0.25, 0.0).astype(BF16)
    r23[...] = jnp.where((i >> 1) + 32 == j, 0.25, 0.0).astype(BF16)
    p43[...] = jnp.where(i == (j >> 1), 1.0, 0.0).astype(BF16)
    p32[...] = jnp.where(i == (j >> 1) + 32, 1.0, 0.0).astype(BF16)
    i, j = iota((128, 256), 0), iota((128, 256), 1)
    p21[...] = jnp.where(i == (j >> 1), 1.0, 0.0).astype(BF16)

    def pair_rows(ref, rows, lanes):
        return jnp.concatenate(
            [
                ref[t, pl.ds(0, rows // 2, 2), :] + ref[t, pl.ds(1, rows // 2, 2), :]
                for t in range(lanes // 128)
            ],
            axis=1,
        )

    def put(ref, x):
        for t in range(x.shape[1] // 128):
            ref[t, 0 : x.shape[0], :] = x[:, 128 * t : 128 * t + 128]

    def restrict(x, pool, w):
        ref = scratch(pool)
        put(ref, x)
        return mm(pair_rows(ref, x.shape[0], x.shape[1]), w[...])

    def prolong(e, pool, w):
        ref = scratch(pool)
        y = mm(e, w[...])
        m = y.shape[0]
        out = []
        for t in range(y.shape[1] // 128):
            yt = y[:, 128 * t : 128 * t + 128]
            ref[t, pl.ds(0, m, 2), :] = yt
            ref[t, pl.ds(1, m, 2), :] = yt
            out.append(ref[t, 0 : 2 * m, :])
        return jnp.concatenate(out, axis=1) if len(out) > 1 else out[0]

    zero8 = jnp.zeros((8, 512), F32)
    for ref in (kg0, v0, wa, wb):
        ref[0:8, :] = zero8
        ref[200:208, :] = zero8
    for ref in (xs, xg):
        ref[8:16, :] = zero8
        ref[192:200, :] = zero8

    in_shf.wait()
    s0 = shf[...]
    put(tmp0, s0)
    acc = pair_rows(tmp0, 128, 256)
    s1own = mm(acc, rm[...])
    ref1, ref2 = scratch(t1s), scratch(t2s)
    put(ref1, acc)
    acc = pair_rows(ref1, 64, 256)
    put(ref2, acc)
    own3[...] = mm(pair_rows(ref2, 32, 256), r03[...])
    own2[0] = pltpu.roll(restrict(s1own, t1s, r34), 32, axis=1)
    in_rhs.wait()

    def pack_border(f, x):
        for side in range(2):
            e = x[:, 128 * side : 128 * side + 128]
            at = 96 * side
            lane = iota((32, 128), 1)
            out = shifted(e[0:32], -at)
            for n in range(1, 4):
                out = jnp.where(lane < 32 * n, out, shifted(e[32 * n : 32 * n + 32], 32 * n - at))
            edge_out[f, side] = out
            lane = iota((8, 128), 1)
            for end in range(2):
                top = 104 * end
                out = shifted(e[top : top + 8], -at)
                for n in range(1, 3):
                    part = e[top + 8 * n : top + 8 * n + 8]
                    out = jnp.where(lane < 32 * n, out, shifted(part, 32 * n - at))
                corner_out[f, 2 * end + side] = out

    pack_border(1, s0)
    pack_border(0, rhs[...])

    pl.semaphore_wait(barrier, len(partners))

    def border(f):
        src, dst = (shf, xs) if f else (rhs, xg)
        sem = got_border.at[f]
        rows = 0
        for dz, lo, to, mirror in ((-1, 0, 168, 16), (1, 104, 16, 168)):
            dev, out = beyond(dz, 0)
            at = pl.ds(pl.multiple_of(slot(to, mirror, out), 8), 24)
            rows += send(src.at[lo : lo + 24, :], dst.at[at, 128:384], sem, dev)
        for side in range(2):
            dy = 2 * side - 1
            dev, out = beyond(0, dy)
            rows += send(edge_out.at[f, side], edge_in.at[f, slot(side, 1 - side, out)], sem, dev)
            for end in range(2):
                n = 2 * end + side
                dev, out = beyond(2 * end - 1, dy)
                rows += send(corner_out.at[f, n], corner_in.at[f, slot(n, 3 - n, out)], sem, dev)
        return rows

    def unpack_border(f):
        dst = xs if f else xg
        for side in range(2):
            lo = 0 if side else 384
            at = 96 * side
            lane = iota((32, 128), 1)
            keep = lane >= 96 if side else lane < 32
            p = edge_in[f, side]
            for n in range(4):
                dst[40 + 32 * n : 72 + 32 * n, lo : lo + 128] = jnp.where(
                    keep, shifted(p, at - 32 * n), 0.0
                )
            lane = iota((8, 128), 1)
            keep = lane >= 96 if side else lane < 32
            for end in range(2):
                top = 16 if end else 168
                p = corner_in[f, 2 * end + side]
                for n in range(3):
                    dst[top + 8 * n : top + 8 * n + 8, lo : lo + 128] = jnp.where(
                        keep, shifted(p, at - 32 * n), 0.0
                    )

    def side_send(src, buf, sem):
        for n, d in enumerate(SIDE):
            dev, out = beyond(0, d)
            send(src, buf.at[slot(n, n ^ 1, out)], sem.at[0], dev)

    def side_join(own, buf, sem):
        got(sem.at[0], 64)
        right1, left1, right2, left2 = (buf[n] for n in range(4))
        lane = iota((16, 128), 1)
        out = jnp.where(lane < 48, pltpu.roll(left1, 96, axis=1), own)
        out = jnp.where(lane < 16, pltpu.roll(left2, 64, axis=1), out)
        out = jnp.where(lane >= 80, pltpu.roll(right1, 32, axis=1), out)
        return jnp.where(lane >= 112, pltpu.roll(right2, 64, axis=1), out)

    def line_send(src, buf, sem):
        for d in LINE:
            dev, out = beyond(d, 0)
            at = pl.ds(pl.multiple_of(16 * slot(3 - d, 3 + d, out), 8), 16)
            send(src, buf.at[at], sem.at[1], dev)

    SRC2 = {-1: (0, 16), 1: (16, 32), 0: (0, 32)}

    def send2(x, k):
        own2[k] = x
        for n, (dz, dy) in enumerate(AROUND):
            a, b = SRC2[dz]
            dev, out = beyond(dz, dy)
            at = slot(n, MIRROR[n], out)
            send(own2.at[k, a:b], x2b.at[k, at, 0 : b - a], got_2.at[k], dev)

    def lanes3(left, mid, right, lo, hi, move):
        lane = iota(mid.shape, 1)
        out = jnp.where(lane < lo, pltpu.roll(left, 128 - move, axis=1), mid)
        return jnp.where(lane >= hi, pltpu.roll(right, move, axis=1), out)

    def join2(k):
        got(got_2.at[k], 6 * 16 + 2 * 32)
        own, buf = own2[k], x2b.at[k]
        dn, up, rt, lf, dr, dl, ur, ul = range(8)
        return jnp.concatenate(
            [
                lanes3(buf[ul, 0:16], buf[up, 0:16], buf[ur, 0:16], 32, 96, 64),
                lanes3(buf[lf], own, buf[rt], 32, 96, 64),
                lanes3(buf[dl, 0:16], buf[dn, 0:16], buf[dr, 0:16], 32, 96, 64),
            ],
            axis=0,
        )

    def pack3(x, lo):
        lane = iota((8, 128), 1)
        a, b, c = (x[lo + 8 * n : lo + 8 * n + 8] for n in range(3))
        out = jnp.where(lane < 64, pltpu.roll(b, 112, axis=1), pltpu.roll(c, 16, axis=1))
        return jnp.where(lane < 32, pltpu.roll(a, 80, axis=1), out)

    def send3(x, k):
        own3n[k] = x
        own3p[k, 0] = pack3(x, 8)
        own3p[k, 1] = pack3(x, 0)
        for n, (dz, dy) in enumerate(AROUND):
            dev, out = beyond(dz, dy)
            at = slot(n, MIRROR[n], out)
            send(own3p.at[k, 1 if dz == 1 else 0], x3b.at[k, at], got_3.at[k], dev)

    def take3(k):
        got(got_3.at[k], 64)
        return [own3n[k, 8:24]] + [x3b[k, n] for n in range(8)]

    def join3(own, dn, up, rt, lf, dr, dl, ur, ul):
        lane = iota((8, 128), 1)

        def at(x, n, dest):
            move = (dest - 32 * n) % 128
            return pltpu.roll(x, move, axis=1) if move else x

        rows = []
        for left, centre, right, count in ((ul, up, ur, 3), (lf, None, rt, 2), (dl, dn, dr, 3)):
            for n in range(count):
                c = own[8 * n : 8 * n + 8] if centre is None else at(centre, n, 48)
                out = jnp.where(lane < 80, c, at(right, n, 80))
                rows.append(jnp.where(lane < 48, at(left, n, 16), out))
        return jnp.concatenate(rows, axis=0)

    def sum_start(row, k):
        ar_in[k, 0] = row
        for n, o in enumerate(GROUP_A):
            send(ar_in.at[k, 0], ar_a.at[k, n], got_sum.at[k, 0], in_a(*o))

    def sum_next(k):
        got(got_sum.at[k, 0], 15)
        ar_in[k, 1] = ar_in[k, 0] + jnp.sum(ar_a[k], axis=0)
        for n, o in enumerate(GROUP_B):
            send(ar_in.at[k, 1], ar_b.at[k, n], got_sum.at[k, 1], in_b(*o))

    def sum_end(k):
        got(got_sum.at[k, 1], 15)
        return ar_in[k, 1] + jnp.sum(ar_b[k], axis=0)

    side_send(own3, s_side, got_s)
    border_rows = border(1)
    border(0)
    send2(own2[0], 0)
    s_row = side_join(own3[...], s_side, got_s)
    ownb[0] = s_row
    line_send(ownb.at[0], s_line, got_s)
    s_line[48:64] = s_row

    row0 = gx * 128 - 32
    col0 = gy * 256 - 128
    got(got_border.at[1], border_rows)
    unpack_border(1)
    STEP = 16

    def near4(ref, r, n=STEP):
        c = ref[8 + r : 8 + r + n, :]
        around = (
            ref[7 + r : 7 + r + n, :]
            + ref[9 + r : 9 + r + n, :]
            + pltpu.roll(c, 1, axis=1)
            + pltpu.roll(c, 511, axis=1)
        )
        return c, around

    for r in range(0, 192, STEP):
        w = slice(8 + r, 8 + r + STEP)
        ok = inside((STEP, 512), 0, row0 + r, col0)
        kk[w, :] = jnp.where(ok, 0.8 / (4.0 + xs[w, :]), 0.0)
    put(tmp0, xs[8:200, :])
    s1 = jnp.concatenate(
        [
            mm(tmp0_pair(tmp0, t, 192), rm[...])
            for t in range(2)
        ],
        axis=1,
    )
    l1 = Level(1, s1, gx * 64 - 16, gy * 128 - 64)
    s2 = restrict(s1, t1s, rm)
    l2a = Level(2, s2, gx * 32 - 8, gy * 64 - 32)

    got(got_border.at[0], border_rows)
    unpack_border(0)
    for r in range(0, 192, STEP):
        w = slice(8 + r, 8 + r + STEP)
        kg0[w, :] = kk[w, :] * xg[w, :]
    for r in range(0, 192, STEP):
        w = slice(8 + r, 8 + r + STEP)
        c, around = near4(kg0, r)
        v0[w, :] = 1.2 * c + kk[w, :] * around
    for r in range(0, 192, STEP):
        w = slice(8 + r, 8 + r + STEP)
        c, around = near4(v0, r)
        out = xg[w, :] - (4.0 + xs[w, :]) * c + around
        for t in range(4):
            tmp0[t, r : r + STEP, :] = out[:, 128 * t : 128 * t + 128]
    g1 = jnp.concatenate([mm(tmp0_pair(tmp0, t, 192), rm[...]) for t in range(2)], axis=1)

    kg1, v1, r1 = l1.down(g1)
    g2 = restrict(r1, t1s, rm)
    _, _, r2 = l2a.down(g2)
    g3 = restrict(r2, t2s, r23)
    g3own = g3[4:20]
    own3g[...] = g3own
    side_send(own3g, g_side, got_g)
    send2(g2[8:40], 1)

    got(got_s.at[1], 96)
    l3 = Level(3, s_line[...], gx * 16 - 48, gy * 32 - 48)
    s4 = restrict(s_line[...], t3s, r34)
    l4 = Level(4, s4, gx * 8 - 24, gy * 16 - 24, iota((56, 128), 1) < 64)

    one4 = jnp.where(l4.ok, 1.0, 0.0)
    one3 = jnp.where(l3.ok, 1.0, 0.0)
    w6 = l4.sweeps(one4, None, P4 * 3)
    w12 = l4.sweeps(w6, None, P4 * 3)
    y3 = l3.sweeps(one3, None, P3)
    u = l3.sweeps(y3, None, P3)
    q = 4.0 * restrict(jnp.where(l3.ok, l3.apply(u), 0.0), t3s, r34)
    kq = Moved(l4.k * q)
    z = l4.sweeps(kq, kq, P4 * 5 + (1,))
    f3 = l3.sweeps(u - 0.25 * prolong(z, t3s, p43), None, P3)
    f2 = l3.sweeps(prolong(w6, t3s, p43), None, P3)
    lane3 = (iota((16, 128), 1) >= 48) & (iota((16, 128), 1) < 80)
    lane4 = (iota((8, 128), 1) >= 24) & (iota((8, 128), 1) < 40)
    g3m = jnp.where(lane3, g3own, 0.0)

    def own4(x):
        return jnp.where(lane4, x[24:32], 0.0)

    parts = [
        0.25 * total(y3[48:64] * g3m),
        0.25 * total(f2[48:64] * g3m),
        total(f3[48:64] * g3m),
        total(own4(l4.apply(one4))),
        total(own4(l4.apply(w6))),
        total(own4(q * w12)),
        total(own4(q * w6)),
    ]
    lane = iota((1, 128), 1)
    row = jnp.zeros((1, 128), F32)
    for n, p in enumerate(parts):
        row = jnp.where(lane == n, p, row)
    sum_start(row, 0)

    def coarse(G):
        kgc, v, r = l3b.down(G)
        kgd = Moved(l4b.k * restrict(r, t3s, r34))
        e = l4b.sweeps(kgd, kgd, P4B)
        return l3b.sweeps(v + prolong(e, t3s, p43), kgc, P3B)[16:48]

    def down2(x):
        pad = jnp.zeros((8, 128), F32)
        g = jnp.concatenate([pad, x, pad], axis=0)
        kg, v, r = l2.down(g)
        return g, v, r, restrict(r, t2s, r23)

    def up2(e3, g):
        kg, v, _ = l2.down(g)
        return l2.sweeps(v + prolong(e3, t2s, p32), kg, P2)

    l3b = l3.cut(24, 88)
    l4b = l4.cut(12, 44)
    lane1 = (iota((64, 256), 1) >= 64) & (iota((64, 256), 1) < 192)
    lane2 = (iota((32, 128), 1) >= 32) & (iota((32, 128), 1) < 96)

    def dot1(a, b):
        return total(jnp.where(lane1, a[16:80] * b[16:80], 0.0))

    def dot2(a, b):
        return total(jnp.where(lane2, a[16:48] * b[16:48], 0.0))

    def dot3(a, b):
        return total(jnp.where(lane3, a * b, 0.0))

    g_row = side_join(g3own, g_side, got_g)
    ownb[1] = g_row
    line_send(ownb.at[1], g_line, got_g)
    g_line[48:64] = g_row

    s2w = join2(0)
    l2 = Level(2, s2w, gx * 32 - 16, gy * 64 - 32)
    y2 = l2.sweeps(prolong(y3[40:72], t2s, p32), None, P2)
    f5 = l1.sweeps(prolong(y2[8:56], t1s, p21), None, P1 * 2) * (1.0 / 64)
    ga, va, ta, ha = down2(4.0 * restrict(l1.apply(f5), t1s, rm))
    ha = 4.0 * ha
    send3(ha, 6)

    ra, rb = prolong(w12, t3s, p43), prolong(w6, t3s, p43)
    ra, rb = (l3.sweeps(x, None, PR * 2) for x in (ra, rb))
    ka, kb = (Moved(l4.k * restrict(-l3.apply(x), t3s, r34)) for x in (ra, rb))
    ea, eb = (l4.sweeps(x, x, P4 * 2 + (1,)) for x in (ka, kb))
    ra, rb = ra + prolong(ea, t3s, p43), rb + prolong(eb, t3s, p43)
    ra, rb = (l3.sweeps(x, None, PR) for x in (ra, rb))

    start2 = [prolong(r[40:72], t2s, p32) for r in (ra, rb, f2)]
    after2 = [l2.sweeps(x, None, P2 * 2) for x in start2]
    h_of = [restrict(-l2.apply(x), t2s, r23) for x in after2]
    for n, h in enumerate(h_of):
        send3(h, 3 + n)
    f4 = l2.sweeps(y2, None, P2) * (1.0 / 16)
    p4_of = [-dot2(f4, l2.apply(x)) for x in start2]
    p54 = -dot3(ha[8:24], f2[48:64])
    sum_next(0)

    g2w = join2(1)
    kg2, v2, _ = l2.down(g2w)
    pv = dot1(f5, l1.residual(v1, g1)) - dot2(va, g2w)
    got(got_g.at[1], 96)
    G3 = g_line[...]
    kg3, v3, r3 = l3.down(G3)
    kg4 = Moved(l4.k * restrict(r3, t3s, r34))
    e4 = l4.sweeps(kg4, kg4, P4 * 5 + (1,))
    x3 = l3.sweeps(v3 + prolong(e4, t3s, p43), kg3, P3 * 2)
    kg4 = Moved(l4.k * restrict(l3.residual(x3, G3), t3s, r34))
    e4 = l4.sweeps(kg4, kg4, P4 * 2 + (1,))
    x3 = l3.sweeps(x3 + prolong(e4, t3s, p43), kg3, P3)

    x2 = v2 + prolong(x3[40:72], t2s, p32)
    p4 = dot2(f4, l2.residual(x2, g2w))
    x2 = l2.sweeps(x2, kg2, P2 * 2)
    g3 = restrict(l2.residual(x2, g2w), t2s, r23)
    send3(g3, 0)
    ma = coarse(join3(*take3(6)))[8:24]
    p5 = pv - dot2(ta, x2) - dot3(ma, g3[8:24])
    p5_of = [
        -dot2(ta, x) - dot3(ma, h[8:24]) for x, h in zip(after2, h_of)
    ]
    row = jnp.zeros((1, 128), F32)
    for n, p in enumerate([p4, *p4_of, p5, *p5_of, p54]):
        row = jnp.where(lane == n, p, row)
    sum_start(row, 1)
    tot = sum_end(0)

    z2 = l2.sweeps(start2[2], None, P2)
    w1 = l1.sweeps(prolong(z2[8:56], t1s, p21), None, P1)
    d1 = l1.sweeps(w1, None, P1)
    h2, _, _, h3 = down2(restrict(-l1.apply(d1), t1s, rm))
    send3(h3, 2)
    send2(h2[16:48], 3)

    a1, a2, a3, ones_total, w6_total, qw12, qw6 = (pick(tot, n) for n in range(7))
    inv = 1.0 / ones_total
    c1 = a1 * inv
    c2 = (a2 - c1 * w6_total) * inv
    c3 = 0.25 * (a3 - c1 * qw12 - c2 * qw6) * inv

    def with_constants(x, parts):
        return ((x + c1 * parts[0]) + c2 * parts[1]) + c3 * parts[2]

    x2 = with_constants(x2, after2)
    parts = [take3(3 + n) for n in range(3)]
    G = [with_constants(b, p) for b, p in zip(take3(0), zip(*parts))]
    x2 = x2 + prolong(coarse(join3(*G)), t2s, p32)
    x2 = l2.sweeps(x2, kg2, P2)

    x1 = v1 + prolong(x2[8:56], t1s, p21)
    x1 = l1.sweeps(x1, kg1, P1 * 2)
    g2, _, _, g3 = down2(restrict(l1.residual(x1, g1), t1s, rm))
    send3(g3, 1)
    send2(g2[16:48], 2)
    sum_next(1)
    e3 = coarse(join3(*take3(2)))
    x2r = up2(e3, join2(3))
    x1r = l1.sweeps(d1 + prolong(x2r[8:56], t1s, p21), None, P1)

    e3 = coarse(join3(*take3(1)))
    x2 = up2(e3, join2(2))
    x1 = x1 + prolong(x2[8:56], t1s, p21)
    x1 = l1.sweeps(x1, kg1, P1)
    tot = sum_end(1)
    b4, b41, b42, b43, b5, b51, b52, b53, b54 = (pick(tot, n) for n in range(9))
    c4 = with_constants(b4, (b41, b42, b43)) * inv
    c5 = (with_constants(b5, (b51, b52, b53)) + c4 * b54) * inv
    x1 = (x1 + c4 * x1r) + c5 * w1

    for t in range(2):
        y = mm(x1[:, 128 * t : 128 * t + 128], p21[...])
        for h in range(2):
            tmp0[2 * t + h, pl.ds(0, 96, 2), :] = y[:, 128 * h : 128 * h + 128]
            tmp0[2 * t + h, pl.ds(1, 96, 2), :] = y[:, 128 * h : 128 * h + 128]
    for r in range(16, 176, STEP):
        w = slice(8 + r, 8 + r + STEP)
        e = jnp.concatenate([tmp0[t, r : r + STEP, :] for t in range(4)], axis=1)
        wa[w, :] = v0[w, :] + e
    for src, dst in ((wa, wb), (wb, wa)):
        for r in range(16, 176, STEP):
            w = slice(8 + r, 8 + r + STEP)
            c, around = near4(src, r)
            dst[w, :] = 0.2 * c + kg0[w, :] + kk[w, :] * around
    for r in range(32, 160, STEP):
        w = slice(8 + r, 8 + r + STEP)
        c, around = near4(wa, r)
        sol[r - 32 : r - 32 + STEP, :] = c[:, 128:384]
        out = rhs[r - 32 : r - 32 + STEP, :] + around[:, 128:384]
        out = out - (4.0 + shf[r - 32 : r - 32 + STEP, :]) * c[:, 128:384]
        res[r - 32 : r - 32 + STEP, :] = out
    got(all_sent.at[0], sent[0])


def tmp0_pair(ref, t, rows):
    return jnp.concatenate(
        [
            ref[2 * t + h, pl.ds(0, rows // 2, 2), :] + ref[2 * t + h, pl.ds(1, rows // 2, 2), :]
            for h in range(2)
        ],
        axis=1,
    )


def store(a, b, out_a, out_b, sem):
    copies = [
        pltpu.make_async_copy(a, out_a, sem.at[0]),
        pltpu.make_async_copy(b, out_b, sem.at[1]),
    ]
    for cp in copies:
        cp.start()
    for cp in copies:
        cp.wait()


def body(right_side, shift):
    v = pltpu.VMEM
    dma = pltpu.SemaphoreType.DMA
    big = v((208, 512), F32)
    scratch = (
        [big] * 7
        + [v((4, 192, 128), F32)]
        + [v((4, 2, 128, 128), F32), v((4, 2, 128, 128), F32), v((4, 1, 112, 128), F32)]
        + [v((256, 128), BF16)]
        + [v((128, 128), BF16)] * 4
        + [v((128, 256), BF16), v((256, 128), BF16)]
        + [v((4, 16, 128), F32), v((112, 128), F32)] * 2
        + [v((16, 128), F32)] * 2
        + [v((2, 16, 128), F32)]
        + [v((4, 8, 32, 128), F32), v((4, 32, 128), F32)]
        + [v((7, 8, 8, 128), F32), v((7, 32, 128), F32), v((7, 2, 8, 128), F32)]
        + [v((2, 2, 1, 128), F32), v((2, 15, 1, 128), F32), v((2, 15, 1, 128), F32)]
        + [v((2, 2, 32, 128), F32)] * 2
        + [v((2, 4, 8, 128), F32)] * 2
        + [v((4096, 128), F32)]
        + [dma((1,)), dma((2,)), dma((2,)), dma((2,)), dma((4,)), dma((7,)), dma((2, 2)), dma((2,))]
    )
    shape = jax.ShapeDtypeStruct((128, 256), F32)
    vm = pl.BlockSpec(memory_space=pltpu.VMEM)
    solved = pl.pallas_call(
        kernel,
        out_shape=(v((128, 256), F32),) * 2,
        in_specs=[pl.BlockSpec(memory_space=pltpu.HBM)] * 2,
        out_specs=(vm, vm),
        scratch_shapes=scratch,
        compiler_params=pltpu.CompilerParams(
            collective_id=0, has_side_effects=True, vmem_limit_bytes=66428928
        ),
        name="fcycle",
    )(right_side, shift)
    out = pl.BlockSpec(memory_space=pl.ANY)
    return pl.pallas_call(
        store,
        out_shape=(shape, shape),
        in_specs=[vm, vm],
        out_specs=(out, out),
        scratch_shapes=[dma((2,))],
        compiler_params=pltpu.CompilerParams(vmem_limit_bytes=40 * 1024 * 1024),
        name="store",
    )(*solved)


def solution(mesh):
    spec = P("gx", "gy")
    return jax.shard_map(
        body, mesh=mesh, in_specs=(spec, spec), out_specs=(spec, spec), check_vma=False
    )
```

```python
import jax
import jax.numpy as jnp
from jax import lax
from jax.experimental import pallas as pl
from jax.experimental.pallas import tpu as pltpu
from jax.sharding import PartitionSpec as P

MESH = pl.DeviceIdType.MESH
F32 = jnp.float32
BF16 = jnp.bfloat16
GX, GY = 8, 32
NX, NY = 1024, 8192
LV_Q = [4.0 ** (-l) for l in range(5)]
LV_D = [4.0 ** (1 - l) for l in range(5)]

AROUND = [(-1, 0), (1, 0), (0, -1), (0, 1), (-1, -1), (-1, 1), (1, -1), (1, 1)]
MIRROR = [1, 0, 3, 2, 7, 6, 5, 4]
WINDOW = [(dz, dy) for dz in range(-3, 4) for dy in range(-2, 3) if dz or dy]
P1, P2, P3, P4 = (1, 1), (2,), (2,), (2,)
PR, P3B, P4B = (1, 1), (2,), (3, 2)
GROUP_A = [(dz, dc) for dz in range(8) for dc in range(2) if dz or dc]
GROUP_B = [(dy, dx) for dy in range(4) for dx in range(4) if dy or dx]


def iota(shape, dim):
    return lax.broadcasted_iota(jnp.int32, shape, dim)


def shifted(v, by):
    by %= v.shape[1]
    return pltpu.roll(v, by, axis=1) if by else v


def updown(v):
    return pltpu.roll(v, 1, axis=0) + pltpu.roll(v, v.shape[0] - 1, axis=0)


def beside(v):
    return updown(v) + (shifted(v, 1) + shifted(v, -1))


class Moved:
    def __init__(self, x):
        self.at = {0: x}

    def __call__(self, by):
        if by not in self.at:
            self.at[by] = shifted(self.at[0], by)
        return self.at[by]


class MovedRows:
    def __init__(self, of, lo, hi):
        self.of, self.lo, self.hi = of, lo, hi

    def __call__(self, by):
        return self.of(by)[self.lo : self.hi]


def inside(shape, level, row0, col0):
    rows = iota(shape, 0) + row0
    cols = iota(shape, 1) + col0
    return (
        (rows >= 0) & (rows < (NX >> level)) & (cols >= 0) & (cols < (NY >> level))
    )


class Level:
    def __init__(self, level, shift, row0, col0, mask=None):
        self.level = level
        self.d = LV_D[level] + shift
        ok = inside(shift.shape, level, row0, col0)
        if mask is not None:
            ok = ok & mask
        self.ok = ok
        self.k = jnp.where(ok, 0.8 / self.d, 0.0)
        self.km = Moved(self.k * LV_Q[level])

    def cut(self, lo, hi):
        out = object.__new__(Level)
        out.level, out.ok = self.level, None
        out.d, out.k = self.d[lo:hi], self.k[lo:hi]
        out.km = MovedRows(self.km, lo, hi)
        return out

    def sweeps(self, v, kg, plan):
        for n in plan:
            v = self.several(v, kg, n)
        return v

    def several(self, v, kg, n):
        v = v if isinstance(v, Moved) else Moved(v)
        x = {s: v(s) for s in range(-n, n + 1)}
        for t in range(n - 1, -1, -1):
            x = {s: self.once(x, kg, s) for s in range(-t, t + 1)}
            if t == 0:
                return x[0]

    def once(self, x, kg, s):
        out = 0.2 * x[s] if kg is None else 0.2 * x[s] + kg(s)
        return out + self.km(s) * (updown(x[s]) + (x[s - 1] + x[s + 1]))

    def down(self, g):
        kg = Moved(self.k * g)
        x = {s: kg(s) for s in range(-2, 3)}
        x = {s: self.once(x, kg, s) for s in range(-1, 2)}
        v = x[0]
        r = g - self.d * v + LV_Q[self.level] * (updown(v) + (x[1] + x[-1]))
        return kg, v, r

    def residual(self, v, g):
        return g - self.d * v + LV_Q[self.level] * beside(v)

    def apply(self, v):
        return self.d * v - LV_Q[self.level] * beside(v)


def mm(x, w):
    m = x.shape[0]
    a = x.astype(BF16)
    r = x - a.astype(F32)
    b = r.astype(BF16)
    c = (r - b.astype(F32)).astype(BF16)
    y = jnp.dot(jnp.concatenate([a, b, c], axis=0), w, preferred_element_type=F32)
    return (y[2 * m :] + y[m : 2 * m]) + y[:m]


def total(x):
    return jnp.sum(jnp.sum(x, axis=0, keepdims=True), axis=1, keepdims=True)


def pick(row, at):
    lane = iota(row.shape, 1)
    return jnp.sum(jnp.where(lane == at, row, 0.0), axis=1, keepdims=True)


def kernel(
    rhs_in, shf_in, sol, res,
    xg, xs, kk, kg0, v0, wa, wb, tmp0,
    t1s, t2s, t3s,
    rm, r23, r34, p43, p32, p21, r03,
    win_in, win_out, window, own3,
    x2b, own2, x3b, own3n, own3p,
    ar_in, ar_a, ar_b,
    edge_out, edge_in, corner_out, corner_in, rows_of, all_sent, got_border, got_window, got_2, got_3, got_sum, in_s,
):
    gx = lax.axis_index("gx")
    gy = lax.axis_index("gy")
    core = lax.rem(gy, 2)
    quad = lax.div(gy, 2)
    qy, qx = lax.div(quad, 4), lax.rem(quad, 4)

    def past(at, by, size):
        if by > 0:
            return lax.div(at + by, size)
        return 1 - lax.div(at + (by + size), size) if by < 0 else 0 * at

    other_core = gy + 1 - 2 * core
    other_row = gx + 1 - 2 * lax.rem(gx, 2)

    def beyond(dz, dy):
        if not dy:
            out = past(gx, dz, GX)
            return (gx + (1 - out) * dz, gy + out * (other_core - gy)), out
        if not dz:
            out = past(gy, dy, GY)
            return (gx + out * (other_row - gx), gy + (1 - out) * dy), out
        zo, yo = past(gx, dz, GX), past(gy, dy, GY)
        if dz % 2 == 0:
            ring = other_row
        elif dz > 0:
            first = 5 - dz
            high = lax.div(gx, first)
            ring = (1 - lax.min(high, 1)) * other_row + lax.min(high, 1) * (
                first + lax.rem(gx - first + 1 + 3 * 4, 3)
            )
        else:
            first = -dz
            high = lax.div(gx, first + 3)
            ring = high * other_row + (1 - high) * (first + lax.rem(gx - first + 1 + 3 * 4, 3))
        to_z = zo * gx + (1 - zo) * (yo * ring + (1 - yo) * (gx + dz))
        to_y = zo * other_core + (1 - zo) * (yo * gy + (1 - yo) * (gy + dy))
        return (to_z, to_y), zo + (1 - zo) * yo

    def slot(n, mirror, out):
        return n + out * (mirror - n)

    def in_a(dz, dc):
        return (lax.rem(gx + dz, GX), gy - core + lax.rem(core + dc, 2))

    def in_b(dy, dx):
        return (gx, (lax.rem(qy + dy, 4) * 4 + lax.rem(qx + dx, 4)) * 2 + core)

    barrier = pltpu.get_barrier_semaphore()
    partners = (
        [beyond(*o)[0] for o in WINDOW]
        + [in_a(*o) for o in GROUP_A]
        + [in_b(*o) for o in GROUP_B]
    )
    for p in partners:
        pl.semaphore_signal(barrier, inc=1, device_id=p, device_id_type=MESH)

    mid = (slice(40, 168), slice(128, 384))
    rhs, shf = xg.at[mid], xs.at[mid]
    in_shf = pltpu.make_async_copy(shf_in, shf, in_s.at[0])
    in_rhs = pltpu.make_async_copy(rhs_in, rhs, in_s.at[1])
    in_shf.start()
    in_rhs.start()

    sent = [0]
    turn = [0]

    def got(sem, rows):
        ref = rows_of.at[0:rows]
        pltpu.make_async_copy(ref, ref, sem).wait()

    def scratch(pool):
        turn[0] += 1
        return pool.at[turn[0] % pool.shape[0]]

    def send(src, dst, sem, dev):
        pltpu.make_async_remote_copy(
            src_ref=src, dst_ref=dst, send_sem=all_sent.at[0], recv_sem=sem,
            device_id=dev, device_id_type=MESH,
        ).start()
        size = src.shape[0] * src.shape[1] // 128
        sent[0] += size
        return size

    i, j = iota((256, 128), 0), iota((256, 128), 1)
    rm[...] = jnp.where((i >> 1) == j, 0.25, 0.0).astype(BF16)
    r03[...] = jnp.where((i >> 3) + 48 == j, 1.0 / 64, 0.0).astype(BF16)
    i, j = iota((128, 128), 0), iota((128, 128), 1)
    r34[...] = jnp.where((i >> 1) == j, 0.25, 0.0).astype(BF16)
    r23[...] = jnp.where((i >> 1) + 32 == j, 0.25, 0.0).astype(BF16)
    p43[...] = jnp.where(i == (j >> 1), 1.0, 0.0).astype(BF16)
    p32[...] = jnp.where(i == (j >> 1) + 32, 1.0, 0.0).astype(BF16)
    i, j = iota((128, 256), 0), iota((128, 256), 1)
    p21[...] = jnp.where(i == (j >> 1), 1.0, 0.0).astype(BF16)

    def pair_rows(ref, rows, lanes):
        return jnp.concatenate(
            [
                ref[t, pl.ds(0, rows // 2, 2), :] + ref[t, pl.ds(1, rows // 2, 2), :]
                for t in range(lanes // 128)
            ],
            axis=1,
        )

    def put(ref, x):
        for t in range(x.shape[1] // 128):
            ref[t, 0 : x.shape[0], :] = x[:, 128 * t : 128 * t + 128]

    def restrict(x, pool, w):
        ref = scratch(pool)
        put(ref, x)
        return mm(pair_rows(ref, x.shape[0], x.shape[1]), w[...])

    def prolong(e, pool, w):
        ref = scratch(pool)
        y = mm(e, w[...])
        m = y.shape[0]
        out = []
        for t in range(y.shape[1] // 128):
            yt = y[:, 128 * t : 128 * t + 128]
            ref[t, pl.ds(0, m, 2), :] = yt
            ref[t, pl.ds(1, m, 2), :] = yt
            out.append(ref[t, 0 : 2 * m, :])
        return jnp.concatenate(out, axis=1) if len(out) > 1 else out[0]

    zero8 = jnp.zeros((8, 512), F32)
    for ref in (kg0, v0, wa, wb):
        ref[0:8, :] = zero8
        ref[200:208, :] = zero8
    for ref in (xs, xg):
        ref[8:16, :] = zero8
        ref[192:200, :] = zero8

    in_shf.wait()
    s0 = shf[...]
    put(tmp0, s0)
    acc = pair_rows(tmp0, 128, 256)
    s1own = mm(acc, rm[...])
    ref1, ref2 = scratch(t1s), scratch(t2s)
    put(ref1, acc)
    acc = pair_rows(ref1, 64, 256)
    put(ref2, acc)
    own3[...] = mm(pair_rows(ref2, 32, 256), r03[...])
    own2[0] = pltpu.roll(restrict(s1own, t1s, r34), 32, axis=1)
    in_rhs.wait()

    def pack_border(f, x):
        for side in range(2):
            e = x[:, 128 * side : 128 * side + 128]
            at = 96 * side
            lane = iota((32, 128), 1)
            out = shifted(e[0:32], -at)
            for n in range(1, 4):
                out = jnp.where(lane < 32 * n, out, shifted(e[32 * n : 32 * n + 32], 32 * n - at))
            edge_out[f, side] = out
            lane = iota((8, 128), 1)
            for end in range(2):
                top = 104 * end
                out = shifted(e[top : top + 8], -at)
                for n in range(1, 3):
                    part = e[top + 8 * n : top + 8 * n + 8]
                    out = jnp.where(lane < 32 * n, out, shifted(part, 32 * n - at))
                corner_out[f, 2 * end + side] = out

    pack_border(1, s0)
    pack_border(0, rhs[...])

    pl.semaphore_wait(barrier, len(partners))

    def border(f):
        src, dst = (shf, xs) if f else (rhs, xg)
        sem = got_border.at[f]
        rows = 0
        for dz, lo, to, mirror in ((-1, 0, 168, 16), (1, 104, 16, 168)):
            dev, out = beyond(dz, 0)
            at = pl.ds(pl.multiple_of(slot(to, mirror, out), 8), 24)
            rows += send(src.at[lo : lo + 24, :], dst.at[at, 128:384], sem, dev)
        for side in range(2):
            dy = 2 * side - 1
            dev, out = beyond(0, dy)
            rows += send(edge_out.at[f, side], edge_in.at[f, slot(side, 1 - side, out)], sem, dev)
            for end in range(2):
                n = 2 * end + side
                dev, out = beyond(2 * end - 1, dy)
                rows += send(corner_out.at[f, n], corner_in.at[f, slot(n, 3 - n, out)], sem, dev)
        return rows

    def unpack_border(f):
        dst = xs if f else xg
        for side in range(2):
            lo = 0 if side else 384
            at = 96 * side
            lane = iota((32, 128), 1)
            keep = lane >= 96 if side else lane < 32
            p = edge_in[f, side]
            for n in range(4):
                dst[40 + 32 * n : 72 + 32 * n, lo : lo + 128] = jnp.where(
                    keep, shifted(p, at - 32 * n), 0.0
                )
            lane = iota((8, 128), 1)
            keep = lane >= 96 if side else lane < 32
            for end in range(2):
                top = 16 if end else 168
                p = corner_in[f, 2 * end + side]
                for n in range(3):
                    dst[top + 8 * n : top + 8 * n + 8, lo : lo + 128] = jnp.where(
                        keep, shifted(p, at - 32 * n), 0.0
                    )

    def pack_window(x):
        a, b = x[0:8], x[8:16]
        lane = iota((8, 128), 1)
        out = jnp.where(
            lane < 96, shifted(b, 16), shifted(pltpu.roll(b, 4, axis=0), 48)
        )
        out = jnp.where(lane < 64, shifted(pltpu.roll(a, 4, axis=0), -16), out)
        return jnp.where(lane < 32, shifted(a, -48), out)[0:4]

    def spread(k, x):
        p = pack_window(x)
        win_out[k] = p
        win_in[k, 3, 2] = p
        for dz, dy in WINDOW:
            dev, out = beyond(dz, dy)
            at = win_in.at[k, 3 - dz + 2 * dz * out, 2 - dy + 2 * dy * out]
            send(win_out.at[k], at, got_window.at[k], dev)

    def collect(k):
        got(got_window.at[k], 4 * len(WINDOW))
        lane = iota((4, 128), 1)
        for r in range(7):
            for q in range(4):
                out = shifted(win_in[k, r, 0], -16 - 32 * q)
                for c in range(1, 5):
                    at = 32 * c - 16
                    out = jnp.where(lane < at, out, shifted(win_in[k, r, c], at - 32 * q))
                window[k, 16 * r + 4 * q : 16 * r + 4 * q + 4, :] = out
        return window[k]

    SRC2 = {-1: (0, 16), 1: (16, 32), 0: (0, 32)}

    def send2(x, k):
        own2[k] = x
        for n, (dz, dy) in enumerate(AROUND):
            a, b = SRC2[dz]
            dev, out = beyond(dz, dy)
            at = slot(n, MIRROR[n], out)
            send(own2.at[k, a:b], x2b.at[k, at, 0 : b - a], got_2.at[k], dev)

    def lanes3(left, mid, right, lo, hi, move):
        lane = iota(mid.shape, 1)
        out = jnp.where(lane < lo, pltpu.roll(left, 128 - move, axis=1), mid)
        return jnp.where(lane >= hi, pltpu.roll(right, move, axis=1), out)

    def join2(k):
        got(got_2.at[k], 6 * 16 + 2 * 32)
        own, buf = own2[k], x2b.at[k]
        dn, up, rt, lf, dr, dl, ur, ul = range(8)
        return jnp.concatenate(
            [
                lanes3(buf[ul, 0:16], buf[up, 0:16], buf[ur, 0:16], 32, 96, 64),
                lanes3(buf[lf], own, buf[rt], 32, 96, 64),
                lanes3(buf[dl, 0:16], buf[dn, 0:16], buf[dr, 0:16], 32, 96, 64),
            ],
            axis=0,
        )

    def pack3(x, lo):
        lane = iota((8, 128), 1)
        a, b, c = (x[lo + 8 * n : lo + 8 * n + 8] for n in range(3))
        out = jnp.where(lane < 64, pltpu.roll(b, 112, axis=1), pltpu.roll(c, 16, axis=1))
        return jnp.where(lane < 32, pltpu.roll(a, 80, axis=1), out)

    def send3(x, k):
        own3n[k] = x
        own3p[k, 0] = pack3(x, 8)
        own3p[k, 1] = pack3(x, 0)
        for n, (dz, dy) in enumerate(AROUND):
            dev, out = beyond(dz, dy)
            at = slot(n, MIRROR[n], out)
            send(own3p.at[k, 1 if dz == 1 else 0], x3b.at[k, at], got_3.at[k], dev)

    def take3(k):
        got(got_3.at[k], 64)
        return [own3n[k, 8:24]] + [x3b[k, n] for n in range(8)]

    def join3(own, dn, up, rt, lf, dr, dl, ur, ul):
        lane = iota((8, 128), 1)

        def at(x, n, dest):
            move = (dest - 32 * n) % 128
            return pltpu.roll(x, move, axis=1) if move else x

        rows = []
        for left, centre, right, count in ((ul, up, ur, 3), (lf, None, rt, 2), (dl, dn, dr, 3)):
            for n in range(count):
                c = own[8 * n : 8 * n + 8] if centre is None else at(centre, n, 48)
                out = jnp.where(lane < 80, c, at(right, n, 80))
                rows.append(jnp.where(lane < 48, at(left, n, 16), out))
        return jnp.concatenate(rows, axis=0)

    def sum_start(row, k):
        ar_in[k, 0] = row
        for n, o in enumerate(GROUP_A):
            send(ar_in.at[k, 0], ar_a.at[k, n], got_sum.at[k, 0], in_a(*o))

    def sum_next(k):
        got(got_sum.at[k, 0], 15)
        ar_in[k, 1] = ar_in[k, 0] + jnp.sum(ar_a[k], axis=0)
        for n, o in enumerate(GROUP_B):
            send(ar_in.at[k, 1], ar_b.at[k, n], got_sum.at[k, 1], in_b(*o))

    def sum_end(k):
        got(got_sum.at[k, 1], 15)
        return ar_in[k, 1] + jnp.sum(ar_b[k], axis=0)

    border_rows = border(1)
    border(0)
    spread(0, own3[...])
    send2(own2[0], 0)

    row0 = gx * 128 - 32
    col0 = gy * 256 - 128
    got(got_border.at[1], border_rows)
    unpack_border(1)
    STEP = 16

    def near4(ref, r, n=STEP):
        c = ref[8 + r : 8 + r + n, :]
        around = (
            ref[7 + r : 7 + r + n, :]
            + ref[9 + r : 9 + r + n, :]
            + pltpu.roll(c, 1, axis=1)
            + pltpu.roll(c, 511, axis=1)
        )
        return c, around

    for r in range(0, 192, STEP):
        w = slice(8 + r, 8 + r + STEP)
        ok = inside((STEP, 512), 0, row0 + r, col0)
        kk[w, :] = jnp.where(ok, 0.8 / (4.0 + xs[w, :]), 0.0)
    put(tmp0, xs[8:200, :])
    s1 = jnp.concatenate(
        [
            mm(tmp0_pair(tmp0, t, 192), rm[...])
            for t in range(2)
        ],
        axis=1,
    )
    l1 = Level(1, s1, gx * 64 - 16, gy * 128 - 64)
    s2 = restrict(s1, t1s, rm)
    l2a = Level(2, s2, gx * 32 - 8, gy * 64 - 32)

    got(got_border.at[0], border_rows)
    unpack_border(0)
    for r in range(0, 192, STEP):
        w = slice(8 + r, 8 + r + STEP)
        kg0[w, :] = kk[w, :] * xg[w, :]
    for r in range(0, 192, STEP):
        w = slice(8 + r, 8 + r + STEP)
        c, around = near4(kg0, r)
        v0[w, :] = 1.2 * c + kk[w, :] * around
    for r in range(0, 192, STEP):
        w = slice(8 + r, 8 + r + STEP)
        c, around = near4(v0, r)
        out = xg[w, :] - (4.0 + xs[w, :]) * c + around
        for t in range(4):
            tmp0[t, r : r + STEP, :] = out[:, 128 * t : 128 * t + 128]
    g1 = jnp.concatenate([mm(tmp0_pair(tmp0, t, 192), rm[...]) for t in range(2)], axis=1)

    kg1, v1, r1 = l1.down(g1)
    g2 = restrict(r1, t1s, rm)
    _, _, r2 = l2a.down(g2)
    g3 = restrict(r2, t2s, r23)
    g3own = g3[4:20]
    spread(1, g3own)
    send2(g2[8:40], 1)

    s_window = collect(0)
    l3 = Level(3, s_window, gx * 16 - 48, gy * 32 - 48)
    s4 = restrict(s_window, t3s, r34)
    l4 = Level(4, s4, gx * 8 - 24, gy * 16 - 24, iota((56, 128), 1) < 64)

    one4 = jnp.where(l4.ok, 1.0, 0.0)
    one3 = jnp.where(l3.ok, 1.0, 0.0)
    w6 = l4.sweeps(one4, None, P4 * 3)
    w12 = l4.sweeps(w6, None, P4 * 3)
    y3 = l3.sweeps(one3, None, P3)
    u = l3.sweeps(y3, None, P3)
    q = 4.0 * restrict(jnp.where(l3.ok, l3.apply(u), 0.0), t3s, r34)
    kq = Moved(l4.k * q)
    z = l4.sweeps(kq, kq, P4 * 5 + (1,))
    f3 = l3.sweeps(u - 0.25 * prolong(z, t3s, p43), None, P3)
    f2 = l3.sweeps(prolong(w6, t3s, p43), None, P3)
    lane3 = (iota((16, 128), 1) >= 48) & (iota((16, 128), 1) < 80)
    lane4 = (iota((8, 128), 1) >= 24) & (iota((8, 128), 1) < 40)
    g3m = jnp.where(lane3, g3own, 0.0)

    def own4(x):
        return jnp.where(lane4, x[24:32], 0.0)

    parts = [
        0.25 * total(y3[48:64] * g3m),
        0.25 * total(f2[48:64] * g3m),
        total(f3[48:64] * g3m),
        total(own4(l4.apply(one4))),
        total(own4(l4.apply(w6))),
        total(own4(q * w12)),
        total(own4(q * w6)),
    ]
    lane = iota((1, 128), 1)
    row = jnp.zeros((1, 128), F32)
    for n, p in enumerate(parts):
        row = jnp.where(lane == n, p, row)
    sum_start(row, 0)

    def coarse(G):
        kgc, v, r = l3b.down(G)
        kgd = Moved(l4b.k * restrict(r, t3s, r34))
        e = l4b.sweeps(kgd, kgd, P4B)
        return l3b.sweeps(v + prolong(e, t3s, p43), kgc, P3B)[16:48]

    def down2(x):
        pad = jnp.zeros((8, 128), F32)
        g = jnp.concatenate([pad, x, pad], axis=0)
        kg, v, r = l2.down(g)
        return g, v, r, restrict(r, t2s, r23)

    def up2(e3, g):
        kg, v, _ = l2.down(g)
        return l2.sweeps(v + prolong(e3, t2s, p32), kg, P2)

    l3b = l3.cut(24, 88)
    l4b = l4.cut(12, 44)
    lane1 = (iota((64, 256), 1) >= 64) & (iota((64, 256), 1) < 192)
    lane2 = (iota((32, 128), 1) >= 32) & (iota((32, 128), 1) < 96)

    def dot1(a, b):
        return total(jnp.where(lane1, a[16:80] * b[16:80], 0.0))

    def dot2(a, b):
        return total(jnp.where(lane2, a[16:48] * b[16:48], 0.0))

    def dot3(a, b):
        return total(jnp.where(lane3, a * b, 0.0))

    s2w = join2(0)
    l2 = Level(2, s2w, gx * 32 - 16, gy * 64 - 32)
    y2 = l2.sweeps(prolong(y3[40:72], t2s, p32), None, P2)
    f5 = l1.sweeps(prolong(y2[8:56], t1s, p21), None, P1 * 2) * (1.0 / 64)
    ga, va, ta, ha = down2(4.0 * restrict(l1.apply(f5), t1s, rm))
    ha = 4.0 * ha
    send3(ha, 6)

    ra, rb = prolong(w12, t3s, p43), prolong(w6, t3s, p43)
    ra, rb = (l3.sweeps(x, None, PR * 2) for x in (ra, rb))
    ka, kb = (Moved(l4.k * restrict(-l3.apply(x), t3s, r34)) for x in (ra, rb))
    ea, eb = (l4.sweeps(x, x, P4 * 2 + (1,)) for x in (ka, kb))
    ra, rb = ra + prolong(ea, t3s, p43), rb + prolong(eb, t3s, p43)
    ra, rb = (l3.sweeps(x, None, PR) for x in (ra, rb))

    start2 = [prolong(r[40:72], t2s, p32) for r in (ra, rb, f2)]
    after2 = [l2.sweeps(x, None, P2 * 2) for x in start2]
    h_of = [restrict(-l2.apply(x), t2s, r23) for x in after2]
    for n, h in enumerate(h_of):
        send3(h, 3 + n)
    f4 = l2.sweeps(y2, None, P2) * (1.0 / 16)
    p4_of = [-dot2(f4, l2.apply(x)) for x in start2]
    p54 = -dot3(ha[8:24], f2[48:64])

    g2w = join2(1)
    kg2, v2, _ = l2.down(g2w)
    pv = dot1(f5, l1.residual(v1, g1)) - dot2(va, g2w)
    G3 = collect(1)
    kg3, v3, r3 = l3.down(G3)
    kg4 = Moved(l4.k * restrict(r3, t3s, r34))
    e4 = l4.sweeps(kg4, kg4, P4 * 5 + (1,))
    sum_next(0)
    x3 = l3.sweeps(v3 + prolong(e4, t3s, p43), kg3, P3 * 2)
    kg4 = Moved(l4.k * restrict(l3.residual(x3, G3), t3s, r34))
    e4 = l4.sweeps(kg4, kg4, P4 * 2 + (1,))
    x3 = l3.sweeps(x3 + prolong(e4, t3s, p43), kg3, P3)

    x2 = v2 + prolong(x3[40:72], t2s, p32)
    p4 = dot2(f4, l2.residual(x2, g2w))
    x2 = l2.sweeps(x2, kg2, P2 * 2)
    g3 = restrict(l2.residual(x2, g2w), t2s, r23)
    send3(g3, 0)
    ma = coarse(join3(*take3(6)))[8:24]
    p5 = pv - dot2(ta, x2) - dot3(ma, g3[8:24])
    p5_of = [
        -dot2(ta, x) - dot3(ma, h[8:24]) for x, h in zip(after2, h_of)
    ]
    row = jnp.zeros((1, 128), F32)
    for n, p in enumerate([p4, *p4_of, p5, *p5_of, p54]):
        row = jnp.where(lane == n, p, row)
    sum_start(row, 1)
    parts = [take3(3 + n) for n in range(3)]

    z2 = l2.sweeps(start2[2], None, P2)
    w1 = l1.sweeps(prolong(z2[8:56], t1s, p21), None, P1)
    d1 = l1.sweeps(w1, None, P1)
    h2, _, _, h3 = down2(restrict(-l1.apply(d1), t1s, rm))
    send3(h3, 2)
    send2(h2[16:48], 3)

    tot = sum_end(0)
    a1, a2, a3, ones_total, w6_total, qw12, qw6 = (pick(tot, n) for n in range(7))
    inv = 1.0 / ones_total
    c1 = a1 * inv
    c2 = (a2 - c1 * w6_total) * inv
    c3 = 0.25 * (a3 - c1 * qw12 - c2 * qw6) * inv

    def with_constants(x, parts):
        return ((x + c1 * parts[0]) + c2 * parts[1]) + c3 * parts[2]

    x2 = with_constants(x2, after2)
    G = [with_constants(b, p) for b, p in zip(take3(0), zip(*parts))]
    x2 = x2 + prolong(coarse(join3(*G)), t2s, p32)
    x2 = l2.sweeps(x2, kg2, P2)

    x1 = v1 + prolong(x2[8:56], t1s, p21)
    x1 = l1.sweeps(x1, kg1, P1 * 2)
    g2, _, _, g3 = down2(restrict(l1.residual(x1, g1), t1s, rm))
    send3(g3, 1)
    send2(g2[16:48], 2)
    sum_next(1)
    e3 = coarse(join3(*take3(2)))
    x2r = up2(e3, join2(3))
    x1r = l1.sweeps(d1 + prolong(x2r[8:56], t1s, p21), None, P1)

    e3 = coarse(join3(*take3(1)))
    x2 = up2(e3, join2(2))
    x1 = x1 + prolong(x2[8:56], t1s, p21)
    x1 = l1.sweeps(x1, kg1, P1)
    tot = sum_end(1)
    b4, b41, b42, b43, b5, b51, b52, b53, b54 = (pick(tot, n) for n in range(9))
    c4 = with_constants(b4, (b41, b42, b43)) * inv
    c5 = (with_constants(b5, (b51, b52, b53)) + c4 * b54) * inv
    x1 = (x1 + c4 * x1r) + c5 * w1

    for t in range(2):
        y = mm(x1[:, 128 * t : 128 * t + 128], p21[...])
        for h in range(2):
            tmp0[2 * t + h, pl.ds(0, 96, 2), :] = y[:, 128 * h : 128 * h + 128]
            tmp0[2 * t + h, pl.ds(1, 96, 2), :] = y[:, 128 * h : 128 * h + 128]
    for r in range(16, 176, STEP):
        w = slice(8 + r, 8 + r + STEP)
        e = jnp.concatenate([tmp0[t, r : r + STEP, :] for t in range(4)], axis=1)
        wa[w, :] = v0[w, :] + e
    for src, dst in ((wa, wb), (wb, wa)):
        for r in range(16, 176, STEP):
            w = slice(8 + r, 8 + r + STEP)
            c, around = near4(src, r)
            dst[w, :] = 0.2 * c + kg0[w, :] + kk[w, :] * around
    for r in range(32, 160, STEP):
        w = slice(8 + r, 8 + r + STEP)
        c, around = near4(wa, r)
        sol[r - 32 : r - 32 + STEP, :] = c[:, 128:384]
        out = rhs[r - 32 : r - 32 + STEP, :] + around[:, 128:384]
        out = out - (4.0 + shf[r - 32 : r - 32 + STEP, :]) * c[:, 128:384]
        res[r - 32 : r - 32 + STEP, :] = out
    got(all_sent.at[0], sent[0])


def tmp0_pair(ref, t, rows):
    return jnp.concatenate(
        [
            ref[2 * t + h, pl.ds(0, rows // 2, 2), :] + ref[2 * t + h, pl.ds(1, rows // 2, 2), :]
            for h in range(2)
        ],
        axis=1,
    )


def store(a, b, out_a, out_b, sem):
    copies = [
        pltpu.make_async_copy(a, out_a, sem.at[0]),
        pltpu.make_async_copy(b, out_b, sem.at[1]),
    ]
    for cp in copies:
        cp.start()
    for cp in copies:
        cp.wait()


def body(right_side, shift):
    v = pltpu.VMEM
    dma = pltpu.SemaphoreType.DMA
    big = v((208, 512), F32)
    scratch = (
        [big] * 7
        + [v((4, 192, 128), F32)]
        + [v((4, 2, 128, 128), F32), v((4, 2, 128, 128), F32), v((4, 1, 112, 128), F32)]
        + [v((256, 128), BF16)]
        + [v((128, 128), BF16)] * 4
        + [v((128, 256), BF16), v((256, 128), BF16)]
        + [v((2, 7, 5, 4, 128), F32), v((2, 4, 128), F32), v((2, 112, 128), F32)]
        + [v((16, 128), F32)]
        + [v((4, 8, 32, 128), F32), v((4, 32, 128), F32)]
        + [v((7, 8, 8, 128), F32), v((7, 32, 128), F32), v((7, 2, 8, 128), F32)]
        + [v((2, 2, 1, 128), F32), v((2, 15, 1, 128), F32), v((2, 15, 1, 128), F32)]
        + [v((2, 2, 32, 128), F32)] * 2
        + [v((2, 4, 8, 128), F32)] * 2
        + [v((4096, 128), F32)]
        + [dma((1,)), dma((2,)), dma((2,)), dma((4,)), dma((7,)), dma((2, 2)), dma((2,))]
    )
    shape = jax.ShapeDtypeStruct((128, 256), F32)
    vm = pl.BlockSpec(memory_space=pltpu.VMEM)
    solved = pl.pallas_call(
        kernel,
        out_shape=(v((128, 256), F32),) * 2,
        in_specs=[pl.BlockSpec(memory_space=pltpu.HBM)] * 2,
        out_specs=(vm, vm),
        scratch_shapes=scratch,
        compiler_params=pltpu.CompilerParams(
            collective_id=0, has_side_effects=True, vmem_limit_bytes=66428928
        ),
        name="fcycle",
    )(right_side, shift)
    out = pl.BlockSpec(memory_space=pl.ANY)
    return pl.pallas_call(
        store,
        out_shape=(shape, shape),
        in_specs=[vm, vm],
        out_specs=(out, out),
        scratch_shapes=[dma((2,))],
        compiler_params=pltpu.CompilerParams(vmem_limit_bytes=40 * 1024 * 1024),
        name="store",
    )(*solved)


def solution(mesh):
    spec = P("gx", "gy")
    return jax.shard_map(
        body, mesh=mesh, in_specs=(spec, spec), out_specs=(spec, spec), check_vma=False
    )
```
